128 devices in a mesh: row: 8 (over z, x_lo), col: 16 (over y, x_hi, core).
Axes of the slice: x: 4 (x_hi: 2, x_lo: 2; x = x_hi * 2 + x_lo), y: 4, z: 4, core: 2. Of those that a mesh axis runs over, the one named last changes fastest.
Arguments:
- cell_index: int32 [2, 3, 262144], P(None, None, ('row', 'col')), may hold values from 0 to 255, as said below
- fraction: float32 [2, 3, 262144], P(None, None, ('row', 'col')), may hold values from 0 to 1
- charge: float32 [2, 262144], P(None, ('row', 'col')), may hold values from -4 to 4
- atom_count: int32 [2, 128], P(None, ('row', 'col')), may hold values from 1024 to 2048, as said below
- influence: float32 [256, 256, 256], P('row', 'col'), as said below
Outputs:
- forces: float32 [2, 3, 262144], P(None, None, ('row', 'col'))
The draws below stay inside these ranges and needn't reach their ends.
Inputs may be any that keep to these rules, and one draw needn't show every extreme that they name: `cell_index`: slot a belongs to pencil p = a // 2048; with P = 16, its first cell index lies in [(p // P) * 32, (p // P + 1) * 32) and its second in [(p % P) * 16, (p % P + 1) * 16). `atom_count`: in every frame some pencil has all 2048 slots live. Even: influence[a, b, c] equals influence[(-a) mod 256, (-b) mod 256, (-c) mod 256]; it is 0 at the root and positive elsewhere.
All inputs are finite; a program needn't handle non-finite values.
Results may differ from the reference program's by a relative error of at most 0.0003.
Values sent between devices are 32-bit elements; how exact they have to be, the bound alone decides.
A program may use at most 128 MiB of HBM per device.

```python
import math
import jax
import jax.numpy as jnp

K = 256
ATOM_DEV = 2048
STEPS = 2
XB = 32
YB = 16
PENCILS = 128
ATOMS = 262144


def draw_cell_index(key, part):
    per_row = K // YB
    slot_ids = jnp.arange(ATOMS, dtype=jnp.int32)
    pencil = slot_ids // ATOM_DEV
    first_base = pencil // per_row * XB
    second_base = pencil % per_row * YB
    subkeys = jax.random.split(key, 3)
    first_index = first_base[None, :] + jax.random.randint(subkeys[0], (STEPS, ATOMS), 0, XB)
    second_index = second_base[None, :] + jax.random.randint(subkeys[1], (STEPS, ATOMS), 0, YB)
    third_index = jax.random.randint(subkeys[2], (STEPS, ATOMS), 0, K)
    return jnp.stack([first_index, second_index, third_index], axis=1).astype(jnp.int32)


def draw_atom_count(key, part):
    subkeys = jax.random.split(key, 2)
    counts = jax.random.randint(subkeys[0], (STEPS, PENCILS), ATOM_DEV // 2, ATOM_DEV + 1)
    chosen = jax.random.randint(subkeys[1], (STEPS, 1), 0, PENCILS)
    column = jnp.arange(PENCILS, dtype=jnp.int32)
    return jnp.where(column[None, :] == chosen, ATOM_DEV, counts).astype(jnp.int32)


def draw_influence(key, part):
    wave_index = jnp.arange(K, dtype=jnp.int32)
    roughness = jnp.exp(jax.random.uniform(key, (K, K, K), jnp.float32, math.log(2.0), math.log(40.0)))
    mirror = jnp.roll(jnp.flip(roughness, (0, 1, 2)), 1, axis=(0, 1, 2))
    symmetric = 0.5 * (roughness + mirror)
    root = (wave_index[:, None, None] == 0) & (wave_index[None, :, None] == 0) & (wave_index[None, None, :] == 0)
    return jnp.where(root, 0.0, symmetric).astype(jnp.float32)


def steps_of(key, shape, cuts, smallest, high):
    factor_of, own = 1.0, jax.random.fold_in(key, 6)
    for position, blocks in cuts:
        steps = jnp.exp(jax.random.uniform(jax.random.fold_in(own, position), (blocks,), jnp.float32, smallest / len(cuts), high / len(cuts)))
        factor_of = factor_of * jnp.repeat(steps, shape[position] // blocks).reshape([-1 if axis == position else 1 for axis in range(len(shape))])
    return factor_of


def scatter_about(rng, extent, spread, limit, pieces=(), kind=jnp.bfloat16):
    values = jax.random.normal(rng, extent, jnp.float32) * spread
    if len(pieces) > 0:
        values = steps_of(rng, extent, pieces, -0.22, 0.18) * values
    return jnp.clip(values, min=-limit, max=limit).astype(kind)


def setup_inputs(seed: int = 0) -> dict:
    splits = jax.random.split(jax.random.key(seed), 6)
    return {
        "cell_index": draw_cell_index(jax.random.fold_in(splits[5], 71), 0),
        "fraction": jnp.clip(1.0 * jax.random.uniform(splits[1], (STEPS, 3, ATOMS), jnp.float32) ** steps_of(splits[1], (STEPS, 3, ATOMS), ((2, 128),), -0.2, 0.2), 0.0, 1.0),
        "charge": scatter_about(splits[2], (STEPS, ATOMS), 1.0, 4.0, ((1, 128),), jnp.float32),
        "atom_count": draw_atom_count(jax.random.fold_in(splits[5], 71), 0),
        "influence": draw_influence(jax.random.fold_in(splits[5], 71), 0),
    }


def spline_values(fraction):
    nothing = jnp.zeros_like(fraction)
    levels = [fraction, 1.0 - fraction]
    slopes = levels
    for degree in range(3, 7):
        padded = levels + [nothing]
        following = []
        for offset in range(degree):
            beneath = padded[offset - 1] if offset > 0 else nothing
            following.append(((fraction + offset) * padded[offset] + (degree - fraction - offset) * beneath) / (degree - 1))
        if degree == 6:
            slopes = [padded[offset] - (padded[offset - 1] if offset > 0 else nothing) for offset in range(6)]
        levels = following
    return jnp.stack(levels), jnp.stack(slopes)


def reference(cell_index, fraction, charge, atom_count, influence):
    slot_ids = jnp.arange(ATOMS, dtype=jnp.int32)
    pencil = slot_ids // ATOM_DEV
    green_table = jnp.transpose(influence, (2, 0, 1))
    offsets = jnp.arange(6, dtype=jnp.int32)
    results = []
    for step in range(STEPS):
        living = (slot_ids % ATOM_DEV) < atom_count[step][pencil]
        charges = jnp.where(living, charge[step], 0.0)
        values = []
        slopes = []
        corners = []
        for dimension in range(3):
            weight, gradient = spline_values(fraction[step, dimension])
            values.append(weight)
            slopes.append(gradient)
            corners.append(((cell_index[step, dimension][None, :] - offsets[:, None]) % K).astype(jnp.int32))
        index_inner = corners[1][:, None, :] * K + corners[2][None, :, :]
        weight_inner = values[1][:, None, :] * values[2][None, :, :]
        charge_mesh = jnp.zeros((K * K * K,), jnp.float32)
        for offset in range(6):
            target = corners[0][offset][None, None, :] * (K * K) + index_inner
            amount = charges[None, None, :] * values[0][offset][None, None, :] * weight_inner
            charge_mesh = charge_mesh.at[target.reshape(-1)].add(amount.reshape(-1))
        spectrum = jnp.fft.fftn(charge_mesh.reshape(K, K, K))
        potential = jnp.real(jnp.fft.ifftn(green_table * spectrum)).reshape(-1)
        first_total = jnp.zeros_like(charges)
        second_total = jnp.zeros_like(charges)
        third_total = jnp.zeros_like(charges)
        for offset in range(6):
            target = corners[0][offset][None, None, :] * (K * K) + index_inner
            sampled = potential[target]
            first_total = first_total + slopes[0][offset] * jnp.sum(sampled * weight_inner, axis=(0, 1))
            second_total = second_total + values[0][offset] * jnp.sum(sampled * slopes[1][:, None, :] * values[2][None, :, :], axis=(0, 1))
            third_total = third_total + values[0][offset] * jnp.sum(sampled * values[1][:, None, :] * slopes[2][None, :, :], axis=(0, 1))
        results.append(-charges[None, :] * jnp.stack([first_total, second_total, third_total]))
    return jnp.stack(results)
```

```python
import functools

import jax
import jax.numpy as jnp
import numpy as np
from jax import lax
from jax.experimental import pallas as pl
from jax.experimental.pallas import tpu as pltpu
from jax.sharding import PartitionSpec as P

F32 = jnp.float32
BF16 = jnp.bfloat16
MESH = pl.DeviceIdType.MESH

K = 256
ROWS = 8
COLS = 16
DEVS = ROWS * COLS
ATOMS = 2048
CHUNK = 512
CHUNKS = ATOMS // CHUNK
GCHUNK = 256
GCHUNKS = ATOMS // GCHUNK

YH, XH, CH = 160, 80, 48
HALO = YH + XH + CH


def halves(x):
    top = x.astype(BF16)
    return top, (x - top.astype(F32)).astype(BF16)


def np_halves(x):
    x = np.asarray(x, np.float32)
    top = x.astype(jnp.bfloat16)
    return [top, (x - top.astype(np.float32)).astype(jnp.bfloat16)]


def tables():
    d = np.arange(DEVS)
    waves = np.concatenate([16 * (d % COLS) + 2 * (d // COLS) + p for p in range(2)])
    turn = 2.0 * np.pi / K
    angle = (waves[:, None] * np.arange(K)[None, :] % K) * turn
    out = np_halves(np.cos(angle)) + np_halves(np.sin(angle))
    k1 = np.arange(256)
    k1x, k1y = k1 // 16, k1 % 16
    src = np.arange(256)
    xh, rc = src // DEVS, src % DEVS
    rx, cc = 2 * (rc // COLS) + xh, rc % COLS
    angle = ((k1x[:, None] * rx[None, :] + k1y[:, None] * cc[None, :]) % 16) * (16 * turn)
    out += np_halves(np.cos(angle)) + np_halves(np.sin(angle))
    out += np_halves(np.cos(angle.T)) + np_halves(np.sin(angle.T))
    spot = np.arange(256)
    xl, yl = spot // 16, spot % 16
    k2 = np.arange(256)
    k2y, k2x = k2 // 16, k2 % 16
    angle = ((xl[:, None] * k2x[None, :] + yl[:, None] * k2y[None, :]) % 16) * (16 * turn)
    out += np_halves(np.cos(angle)) + np_halves(np.sin(angle))
    angle = ((k1x[:, None] * xl[None, :] + k1y[:, None] * yl[None, :]) % K) * turn
    out += [np.cos(angle).astype(np.float32), np.sin(angle).astype(np.float32)]
    return out


def spline_values(f):
    nothing = jnp.zeros_like(f)
    levels = [f, 1.0 - f]
    slopes = levels
    for degree in range(3, 7):
        padded = levels + [nothing]
        following = []
        for o in range(degree):
            value = (f + float(o)) * padded[o]
            if o > 0:
                value = value + (float(degree - o) - f) * padded[o - 1]
            following.append(value * (1.0 / (degree - 1)))
        if degree == 6:
            slopes = [padded[0]] + [padded[o] - padded[o - 1] for o in range(1, 6)]
        levels = following
    return levels, slopes


def dot_nn(a, b):
    return lax.dot_general(a, b, (((1,), (0,)), ((), ())), preferred_element_type=F32)


def dot_nt(a, b):
    return lax.dot_general(a, b, (((1,), (1,)), ((), ())), preferred_element_type=F32)


def triple(dot, a, b):
    return dot(a[0], b[0]) + dot(a[0], b[1]) + dot(a[1], b[0])


def dense(gap, rows):
    total = jnp.where(gap == 0, rows[0], 0.0)
    for j in range(1, 6):
        total = jnp.where(gap == j, rows[j], total)
    return total


def kernel(
    cell, frac, charge, count, infl,
    zc0, zc1, zs0, zs1, fc0, fc1, fs0, fs1, gc0, gc1, gs0, gs1, lc0, lc1, ls0, ls1, twc, tws,
    forces,
    w_scr, x_scr, y_scr, yq_scr, z_hi, z_lo, sx_scr, sy_scr, sz_hi, sz_lo,
    p_hi, p_lo, hal, yr, xr, cr, mesh, gsend, grecv, green,
    sbuf, rbuf, tbuf, qbuf, pot, ys, yb, xb, cb, fint, fhal,
    sems,
):
    row = lax.axis_index("row")
    col = lax.axis_index("col")
    me = row * COLS + col
    up_r, dn_r = lax.rem(row + 1, ROWS), lax.rem(row + ROWS - 1, ROWS)
    up_c, dn_c = lax.rem(col + 1, COLS), lax.rem(col + COLS - 1, COLS)

    barrier = pltpu.get_barrier_semaphore()

    def greet(k, carry):
        dr = lax.rem(row + k // COLS, ROWS)
        dc = lax.rem(col + lax.rem(k, COLS), COLS)
        pl.semaphore_signal(barrier, inc=1, device_id=(dr, dc), device_id_type=MESH)
        return carry

    lax.fori_loop(1, DEVS, greet, 0)

    for k in range(16):
        gsend[k // 2, k % 2] = infl[:, k, :]

    slot = lax.broadcasted_iota(jnp.int32, (1, ATOMS), 1)
    for s in range(2):
        values, slopes = spline_values(frac[s])
        for j in range(6):
            w_scr[s, 0, j] = values[j]
            w_scr[s, 1, j] = slopes[j]
        yq_scr[s, 24:25] = jnp.where(slot < count[s : s + 1, 0:1], charge[s : s + 1], 0.0)

    def spans(i):
        s = i // CHUNKS
        return s, pl.ds(pl.multiple_of(lax.rem(i, CHUNKS) * CHUNK, CHUNK), CHUNK)

    def positions(n, near):
        spot = lax.broadcasted_iota(jnp.int32, (n, CHUNK), 0)
        return jnp.where(spot < near, spot, spot - n)

    def rows_of(s, kind, dim, lanes):
        return [w_scr[s, kind, j, dim : dim + 1, lanes] for j in range(6)]

    def build(i, carry):
        s, lanes = spans(i)
        gap = (cell[s, 0:1, lanes] - row * 32) - positions(40, 32)
        x_scr[s, :, lanes] = dense(gap, rows_of(s, 0, 0, lanes))
        gap = (cell[s, 1:2, lanes] - col * 16) - positions(24, 16)
        y = dense(gap, rows_of(s, 0, 1, lanes))
        y_scr[s, :, lanes] = y
        yq_scr[s, 0:24, lanes] = y * yq_scr[s, 24:25, lanes]
        gap = (cell[s, 2:3, lanes] - positions(256, 256)) & 255
        top, rest = halves(dense(gap, rows_of(s, 0, 2, lanes)))
        z_hi[s, :, lanes] = top
        z_lo[s, :, lanes] = rest
        return carry

    def build_slopes(i, carry):
        s, lanes = spans(i)
        gap = (cell[s, 0:1, lanes] - row * 32) - positions(40, 32)
        sx_scr[s, :, lanes] = dense(gap, rows_of(s, 1, 0, lanes))
        gap = (cell[s, 1:2, lanes] - col * 16) - positions(24, 16)
        sy_scr[s, :, lanes] = dense(gap, rows_of(s, 1, 1, lanes))
        gap = (cell[s, 2:3, lanes] - positions(256, 256)) & 255
        top, rest = halves(dense(gap, rows_of(s, 1, 2, lanes)))
        sz_hi[s, :, lanes] = top
        sz_lo[s, :, lanes] = rest
        return carry

    lax.fori_loop(0, 2 * CHUNKS, build, 0)

    def put(at, value):
        top, rest = halves(value)
        p_hi[at : at + value.shape[0], :] = top
        p_lo[at : at + value.shape[0], :] = rest

    def accumulate(ref, s, lanes, n):
        a = p_hi[0:n, :], p_lo[0:n, :]
        b = z_hi[s, :, lanes], z_lo[s, :, lanes]
        ref[s] += triple(dot_nt, a, b)

    def halo_chunk(i, carry):
        s, lanes = spans(i)
        for k in range(5):
            put(32 * k, x_scr[s, 0:32, lanes] * yq_scr[s, 19 + k : 20 + k, lanes])
        for k in range(5):
            put(YH + 16 * k, yq_scr[s, 0:16, lanes] * x_scr[s, 35 + k : 36 + k, lanes])
        edge = yq_scr[s, 16:24, lanes]
        for k in range(3):
            first = edge * x_scr[s, 35 + 2 * k : 36 + 2 * k, lanes]
            if k < 2:
                second = edge * x_scr[s, 36 + 2 * k : 37 + 2 * k, lanes]
            else:
                second = jnp.zeros_like(first)
            put(YH + XH + 16 * k, jnp.concatenate([first, second], axis=0))
        accumulate(hal, s, lanes, HALO)
        return carry

    hal[...] = jnp.zeros_like(hal)
    lax.fori_loop(0, 2 * CHUNKS, halo_chunk, 0)

    pl.semaphore_wait(barrier, DEVS - 1)

    def remote(src, dst, pair, dr, dc):
        return pltpu.make_async_remote_copy(
            src_ref=src, dst_ref=dst, send_sem=sems.at[2 * pair], recv_sem=sems.at[2 * pair + 1],
            device_id=(dr, dc), device_id_type=MESH,
        )

    out_halo = [
        remote(hal.at[:, 0:YH], yr, 0, row, dn_c),
        remote(hal.at[:, YH : YH + XH], xr, 1, dn_r, col),
        remote(hal.at[:, YH + XH : HALO], cr, 2, dn_r, dn_c),
    ]
    for copy in out_halo:
        copy.start()

    def send_green(k, carry):
        there = lax.rem(row + k, ROWS)
        remote(gsend.at[there], grecv.at[row], 3, there, col).start()
        return carry

    lax.fori_loop(1, ROWS, send_green, 0)
    grecv[row] = gsend[row]

    def inner_chunk(i, carry):
        s, lanes = spans(i)
        for x in range(32):
            put(16 * x, yq_scr[s, 0:16, lanes] * x_scr[s, x : x + 1, lanes])
        accumulate(mesh, s, lanes, 512)
        return carry

    mesh[...] = jnp.zeros_like(mesh)
    lax.fori_loop(0, 2 * CHUNKS, inner_chunk, 0)

    for copy in out_halo:
        copy.wait()
    for s in range(2):
        view = mesh.at[s].reshape(32, 16, 256)
        for k in range(5):
            view[:, 11 + k, :] += yr[s, 32 * k : 32 * k + 32]
        for k in range(5):
            view[27 + k] += xr[s, 16 * k : 16 * k + 16]
            view[27 + k, 8:16] += cr[s, 8 * k : 8 * k + 8]

    zc, zs = (zc0[...], zc1[...]), (zs0[...], zs1[...])
    for xh in range(2):
        lo = slice(256 * xh, 256 * xh + 256)
        m0, m1 = halves(mesh[0, lo, :]), halves(mesh[1, lo, :])
        re = triple(dot_nt, zc, m0) + triple(dot_nt, zs, m1)
        im = triple(dot_nt, zc, m1) - triple(dot_nt, zs, m0)
        for par in range(2):
            sbuf[:, 4 * par + xh, :] = re[128 * par : 128 * par + 128]
            sbuf[:, 4 * par + 2 + xh, :] = im[128 * par : 128 * par + 128]

    def exchange(src, dst, pair):
        def send(k, carry):
            dr = lax.rem(row + k // COLS, ROWS)
            dc = lax.rem(col + lax.rem(k, COLS), COLS)
            remote(src.at[dr * COLS + dc], dst.at[me], pair, dr, dc).start()
            return carry

        lax.fori_loop(1, DEVS, send, 0)
        dst[me] = src[me]
        return remote(src.at[0 : DEVS - 1], dst.at[0 : DEVS - 1], pair, up_r, col)

    forward = exchange(sbuf, rbuf, 4)

    remote(gsend.at[0 : ROWS - 1], grecv.at[0 : ROWS - 1], 3, up_r, col).wait()
    i0 = lax.broadcasted_iota(jnp.int32, (256, 256), 0)
    i1 = lax.broadcasted_iota(jnp.int32, (256, 256), 1)
    own = (i1 & 15) == (i0 >> 4)
    same = (i0 >> 4) == (i1 & 15)
    green[...] = jnp.zeros_like(green)

    def permute_green(k2y, carry):
        pick = jnp.where(same & ((i1 >> 4) == k2y), 1.0, 0.0).astype(BF16)
        for par in range(2):
            start = pl.multiple_of(lax.rem(k2y, 2) * 16, 16)
            block = grecv[k2y // 2, par, pl.ds(start, 16), :] * (1.0 / 16777216.0)
            tiled = jnp.concatenate([block] * 16, axis=0)
            top, rest = halves(jnp.where(own, tiled, 0.0))
            green[par] += dot_nn(top, pick) + dot_nn(rest, pick)
        return carry

    lax.fori_loop(0, 16, permute_green, 0)
    lax.fori_loop(0, 2 * CHUNKS, build_slopes, 0)

    forward.wait()

    fc, fs = (fc0[...], fc1[...]), (fs0[...], fs1[...])
    gc, gs = (gc0[...], gc1[...]), (gs0[...], gs1[...])
    lc, ls = (lc0[...], lc1[...]), (ls0[...], ls1[...])
    for par in range(2):
        at = 4 * par
        xr_ = halves(jnp.concatenate([rbuf[:, at, :], rbuf[:, at + 1, :]], axis=0))
        xi_ = halves(jnp.concatenate([rbuf[:, at + 2, :], rbuf[:, at + 3, :]], axis=0))
        ur = triple(dot_nn, fc, xr_) + triple(dot_nn, fs, xi_)
        ui = triple(dot_nn, fc, xi_) - triple(dot_nn, fs, xr_)
        tc, ts = twc[...], tws[...]
        vr = halves(ur * tc + ui * ts)
        vi = halves(ui * tc - ur * ts)
        g = green[par]
        er = halves(g * (triple(dot_nn, vr, lc) + triple(dot_nn, vi, ls)))
        ei = halves(g * (triple(dot_nn, vi, lc) - triple(dot_nn, vr, ls)))
        br = triple(dot_nt, er, lc) - triple(dot_nt, ei, ls)
        bi = triple(dot_nt, ei, lc) + triple(dot_nt, er, ls)
        hr = halves(br * tc - bi * ts)
        hi = halves(bi * tc + br * ts)
        tr = triple(dot_nn, gc, hr) - triple(dot_nn, gs, hi)
        ti = triple(dot_nn, gc, hi) + triple(dot_nn, gs, hr)
        for xh in range(2):
            tbuf[:, at + xh, :] = tr[128 * xh : 128 * xh + 128]
            tbuf[:, at + 2 + xh, :] = ti[128 * xh : 128 * xh + 128]

    backward = exchange(tbuf, qbuf, 5)
    backward.wait()

    for xh in range(2):
        qr = jnp.concatenate([qbuf[:, xh, :], qbuf[:, 4 + xh, :]], axis=0)
        qi = jnp.concatenate([qbuf[:, 2 + xh, :], qbuf[:, 6 + xh, :]], axis=0)
        qr, qi = halves(qr.T), halves(qi.T)
        lo = slice(256 * xh, 256 * xh + 256)
        pot[0, lo, :] = triple(dot_nn, qr, zc) - triple(dot_nn, qi, zs)
        pot[1, lo, :] = triple(dot_nn, qi, zc) + triple(dot_nn, qr, zs)

    for s in range(2):
        view = pot.at[s].reshape(32, 16, 256)
        for k in range(5):
            ys[s, 32 * k : 32 * k + 32] = view[:, 11 + k, :]
        for k in range(5):
            hal[s, 8 * k : 8 * k + 8] = view[27 + k, 8:16]
    edge = pot.at[:, 432:512, :]
    back_halo = [
        remote(ys, yb, 6, row, up_c),
        remote(edge, xb, 7, up_r, col),
        remote(hal.at[:, 0:CH], cb, 8, up_r, up_c),
    ]
    for copy in back_halo:
        copy.start()

    for s in range(2):
        top, rest = halves(pot[s])
        fint[s, :, 0:256] = top
        fint[s, :, 256:512] = rest

    for copy in back_halo:
        copy.wait()
    for s in range(2):
        for at, ref, n in ((0, yb, YH), (YH, xb, XH), (YH + XH, cb, CH)):
            top, rest = halves(ref[s])
            fhal[s, at : at + n, 0:256] = top
            fhal[s, at : at + n, 256:512] = rest

    def sample(ref, s, hi_ref, lo_ref, lanes):
        a = ref[s, :, 0:256], ref[s, :, 256:512]
        return triple(dot_nn, a, (hi_ref[s, :, lanes], lo_ref[s, :, lanes]))

    def gather(i, carry):
        s = i // GCHUNKS
        lanes = pl.ds(pl.multiple_of(lax.rem(i, GCHUNKS) * GCHUNK, GCHUNK), GCHUNK)
        plain = sample(fint, s, z_hi, z_lo, lanes)
        slope = sample(fint, s, sz_hi, sz_lo, lanes)
        a1 = a2 = a3 = jnp.zeros((16, GCHUNK), F32)
        for x in range(32):
            wx, sx = x_scr[s, x : x + 1, lanes], sx_scr[s, x : x + 1, lanes]
            part = plain[16 * x : 16 * x + 16]
            a1 = a1 + part * sx
            a2 = a2 + part * wx
            a3 = a3 + slope[16 * x : 16 * x + 16] * wx
        plain = sample(fhal, s, z_hi, z_lo, lanes)
        slope = sample(fhal, s, sz_hi, sz_lo, lanes)
        b1 = b2 = b3 = jnp.zeros((32, GCHUNK), F32)
        e1 = e2 = e3 = jnp.zeros((8, GCHUNK), F32)
        for k in range(5):
            wy, sy = y_scr[s, 19 + k : 20 + k, lanes], sy_scr[s, 19 + k : 20 + k, lanes]
            wx, sx = x_scr[s, 35 + k : 36 + k, lanes], sx_scr[s, 35 + k : 36 + k, lanes]
            part = plain[32 * k : 32 * k + 32]
            b1 = b1 + part * wy
            b2 = b2 + part * sy
            b3 = b3 + slope[32 * k : 32 * k + 32] * wy
            at = YH + 16 * k
            part = plain[at : at + 16]
            a1 = a1 + part * sx
            a2 = a2 + part * wx
            a3 = a3 + slope[at : at + 16] * wx
            at = YH + XH + 8 * k
            part = plain[at : at + 8]
            e1 = e1 + part * sx
            e2 = e2 + part * wx
            e3 = e3 + slope[at : at + 8] * wx
        wy, sy = y_scr[s, 0:16, lanes], sy_scr[s, 0:16, lanes]
        vy, ty = y_scr[s, 16:24, lanes], sy_scr[s, 16:24, lanes]
        wx, sx = x_scr[s, 0:32, lanes], sx_scr[s, 0:32, lanes]

        def total(a, m, e, n, b, q):
            parts = [a * m, e * n, b * q]
            return sum(jnp.sum(part, axis=0, keepdims=True) for part in parts)

        negative = -yq_scr[s, 24:25, lanes]
        forces[s, 0:1, lanes] = negative * total(a1, wy, e1, vy, b1, sx)
        forces[s, 1:2, lanes] = negative * total(a2, sy, e2, ty, b2, wx)
        forces[s, 2:3, lanes] = negative * total(a3, wy, e3, vy, b3, wx)
        return carry

    lax.fori_loop(0, 2 * GCHUNKS, gather, 0)


def shards(consts, cell_index, fraction, charge, atom_count, influence):
    vmem = pl.BlockSpec(memory_space=pltpu.VMEM)
    args = [cell_index, fraction, charge, atom_count, influence] + [jnp.asarray(c) for c in consts]
    v = pltpu.VMEM
    scratch = [
        v((2, 2, 6, 3, ATOMS), F32), v((2, 40, ATOMS), F32), v((2, 24, ATOMS), F32),
        v((2, 25, ATOMS), F32), v((2, 256, ATOMS), BF16), v((2, 256, ATOMS), BF16),
        v((2, 40, ATOMS), F32), v((2, 24, ATOMS), F32), v((2, 256, ATOMS), BF16),
        v((2, 256, ATOMS), BF16), v((512, CHUNK), BF16), v((512, CHUNK), BF16),
        v((2, HALO, 256), F32), v((2, YH, 256), F32), v((2, XH, 256), F32), v((2, CH, 256), F32),
        v((2, 512, 256), F32), v((ROWS, 2, 32, 256), F32), v((ROWS, 2, 32, 256), F32),
        v((2, 256, 256), F32), v((DEVS, 8, 256), F32), v((DEVS, 8, 256), F32),
        v((DEVS, 8, 256), F32), v((DEVS, 8, 256), F32), v((2, 512, 256), F32),
        v((2, YH, 256), F32), v((2, YH, 256), F32), v((2, XH, 256), F32), v((2, CH, 256), F32),
        v((2, 512, 512), BF16), v((2, HALO, 512), BF16),
        pltpu.SemaphoreType.DMA((18,)),
    ]
    return pl.pallas_call(
        kernel,
        out_shape=jax.ShapeDtypeStruct((2, 3, ATOMS), F32),
        in_specs=[vmem] * len(args),
        out_specs=vmem,
        scratch_shapes=scratch,
        compiler_params=pltpu.CompilerParams(
            collective_id=0, has_side_effects=True, vmem_limit_bytes=66_000_000
        ),
    )(*args)


def solution(mesh):
    placed = (
        P(None, None, ("row", "col")),
        P(None, None, ("row", "col")),
        P(None, ("row", "col")),
        P(None, ("row", "col")),
        P("row", "col", None),
    )
    return jax.shard_map(
        functools.partial(shards, tables()), mesh=mesh, in_specs=placed,
        out_specs=P(None, None, ("row", "col")), check_vma=False,
    )
```

```python
import functools

import jax
import jax.numpy as jnp
import numpy as np
from jax import lax
from jax.experimental import pallas as pl
from jax.experimental.pallas import tpu as pltpu
from jax.sharding import PartitionSpec as P

F32 = jnp.float32
BF16 = jnp.bfloat16
MESH = pl.DeviceIdType.MESH

K = 256
ROWS = 8
COLS = 16
DEVS = ROWS * COLS
ATOMS = 2048
CHUNK = 512
CHUNKS = ATOMS // CHUNK
GCHUNK = 256
GCHUNKS = ATOMS // GCHUNK

YH, XH, CH = 160, 80, 48
HALO = YH + XH + CH
OFFSETS = sorted(
    (d for d in np.ndindex(4, 4, 4, 2) if d != (0, 0, 0, 0)),
    key=lambda d: (-sum(min(k, 4 - k) for k in d[:3]), d[3], d[0] + 2 * d[1] + 3 * d[2]),
)


def halves(x):
    top = x.astype(BF16)
    return top, (x - top.astype(F32)).astype(BF16)


def np_halves(x):
    x = np.asarray(x, np.float32)
    top = x.astype(jnp.bfloat16)
    return [top, (x - top.astype(np.float32)).astype(jnp.bfloat16)]


def tables():
    d = np.arange(DEVS)
    waves = np.concatenate([16 * (d % COLS) + 2 * (d // COLS) + p for p in range(2)])
    turn = 2.0 * np.pi / K
    angle = (waves[:, None] * np.arange(K)[None, :] % K) * turn
    out = np_halves(np.cos(angle)) + np_halves(np.sin(angle))
    spot = np.arange(256)
    rx, cc = 2 * (spot % 128 // 16) + spot // 128, spot % 16
    angle = ((rx[:, None] * rx[None, :] + cc[:, None] * cc[None, :]) % 16) * (16 * turn)
    out += np_halves(np.cos(angle)) + np_halves(np.sin(angle))
    xl, yl = spot // 16, spot % 16
    angle = ((xl[:, None] * xl[None, :] + yl[:, None] * yl[None, :]) % 16) * (16 * turn)
    out += np_halves(np.cos(angle)) + np_halves(np.sin(angle))
    angle = ((rx[:, None] * xl[None, :] + cc[:, None] * yl[None, :]) % K) * turn
    twiddles = np.stack([np.cos(angle), np.sin(angle)]).astype(np.float32)
    return np.stack(out), twiddles


def spline_values(f):
    nothing = jnp.zeros_like(f)
    levels = [f, 1.0 - f]
    slopes = levels
    for degree in range(3, 7):
        padded = levels + [nothing]
        following = []
        for o in range(degree):
            value = (f + float(o)) * padded[o]
            if o > 0:
                value = value + (float(degree - o) - f) * padded[o - 1]
            following.append(value * (1.0 / (degree - 1)))
        if degree == 6:
            slopes = [padded[0]] + [padded[o] - padded[o - 1] for o in range(1, 6)]
        levels = following
    return levels, slopes


def dot_nn(a, b):
    return lax.dot_general(a, b, (((1,), (0,)), ((), ())), preferred_element_type=F32)


def dot_nt(a, b):
    return lax.dot_general(a, b, (((1,), (1,)), ((), ())), preferred_element_type=F32)


def triple_nn(a, b):
    left = jnp.concatenate([a[0], a[1], a[0]], axis=1)
    return dot_nn(left, jnp.concatenate([b[0], b[0], b[1]], axis=0))


def triple_nt(a, b):
    left = jnp.concatenate([a[0], a[1], a[0]], axis=1)
    return dot_nt(left, jnp.concatenate([b[0], b[0], b[1]], axis=1))


def dense(gap, rows):
    total = jnp.where(gap == 0, rows[0], 0.0)
    for j in range(1, 6):
        total = jnp.where(gap == j, rows[j], total)
    return total


def kernel(
    cell, frac, charge, count, infl_hbm, tab_hbm, twid_hbm,
    forces,
    infl, tab, twid, w_scr, x_scr, y_scr, yq_scr, z_hi, z_lo, sx_scr, sy_scr, sz_hi, sz_lo,
    p_hi, p_lo, hal, yr, xr, cr, mesh, gsend, grecv, green, wb, fb, gb, lb,
    sbuf, rbuf, tbuf, qbuf, pot, ys, yb, xb, cb, fint, fhal, part, swap,
    sems, local, gate,
):
    row = lax.axis_index("row")
    col = lax.axis_index("col")
    me = row * COLS + col
    up_r, dn_r = lax.rem(row + 1, ROWS), lax.rem(row + ROWS - 1, ROWS)
    up_c, dn_c = lax.rem(col + 1, COLS), lax.rem(col + COLS - 1, COLS)
    core = lax.rem(col, 2)
    px = lax.rem(lax.div(col, 2), 2) * 2 + lax.rem(row, 2)
    py, pz = lax.div(col, 4), lax.div(row, 2)

    xs = [lax.rem(px + d, 4) for d in range(4)]
    x_row, x_col = [lax.rem(x, 2) for x in xs], [lax.div(x, 2) * 2 for x in xs]
    y_col = [lax.rem(py + d, 4) * 4 for d in range(4)]
    z_row = [lax.rem(pz + d, 4) * 2 for d in range(4)]
    cores = core, 1 - core

    def device(dx, dy, dz, dc):
        return z_row[dz] + x_row[dx], y_col[dy] + x_col[dx] + cores[dc]

    loads = [
        pltpu.make_async_copy(infl_hbm, infl, local.at[0]),
        pltpu.make_async_copy(tab_hbm, tab, local.at[1]),
        pltpu.make_async_copy(twid_hbm, twid, local.at[2]),
    ]
    for copy in loads:
        copy.start()

    barrier = pltpu.get_barrier_semaphore()

    def greet_column(k, carry):
        to = row, lax.rem(col + k, COLS)
        pl.semaphore_signal(barrier, inc=1, device_id=to, device_id_type=MESH)
        return carry

    def greet_row(k, carry):
        to = lax.rem(row + k, ROWS), col
        pl.semaphore_signal(barrier, inc=1, device_id=to, device_id_type=MESH)
        return carry

    def vouch(k, carry):
        to = lax.rem(row + k, ROWS), col
        pl.semaphore_signal(gate, inc=1, device_id=to, device_id_type=MESH)
        return carry

    lax.fori_loop(1, ROWS, greet_row, 0)
    lax.fori_loop(1, COLS, greet_column, 0)

    def remote(src, dst, send, recv, to):
        return pltpu.make_async_remote_copy(
            src_ref=src, dst_ref=dst, send_sem=sems.at[send], recv_sem=sems.at[recv],
            device_id=to, device_id_type=MESH,
        )

    slot = lax.broadcasted_iota(jnp.int32, (1, ATOMS), 1)
    values, slopes = spline_values(jnp.concatenate([frac[0], frac[1], frac[2]], axis=0))
    for j in range(6):
        w_scr[0, j] = values[j]
        w_scr[1, j] = slopes[j]
    for s in range(2):
        yq_scr[s, 24:25] = jnp.where(slot < count[0:1, s : s + 1], charge[s : s + 1], 0.0)

    loads[0].wait()
    for k in range(16):
        gsend[k // 2, k % 2] = infl[:, k, :]
    pl.semaphore_wait(barrier, ROWS + COLS - 2)
    lax.fori_loop(1, ROWS, vouch, 0)

    def send_green(k, carry):
        there = lax.rem(row + k, ROWS)
        remote(gsend.at[there], grecv.at[row], 0, 1, (there, col)).start()
        return carry

    lax.fori_loop(1, ROWS, send_green, 0)
    grecv[row] = gsend[row]

    def spans(i):
        s = lax.div(i, CHUNKS)
        return s, pl.ds(pl.multiple_of(lax.rem(i, CHUNKS) * CHUNK, CHUNK), CHUNK)

    def positions(n, near):
        spot = lax.broadcasted_iota(jnp.int32, (n, CHUNK), 0)
        return jnp.where(spot < near, spot, spot - n)

    def rows_of(s, kind, dim, lanes):
        return [w_scr[kind, j, pl.ds(2 * dim + s, 1), lanes] for j in range(6)]

    def gaps(s, lanes):
        return (
            (cell[0, pl.ds(s, 1), lanes] - row * 32) - positions(40, 32),
            (cell[1, pl.ds(s, 1), lanes] - col * 16) - positions(24, 16),
            (cell[2, pl.ds(s, 1), lanes] - positions(256, 256)) & 255,
        )

    def build(i, carry):
        s, lanes = spans(i)
        gx, gy, gz = gaps(s, lanes)
        x_scr[s, :, lanes] = dense(gx, rows_of(s, 0, 0, lanes))
        y = dense(gy, rows_of(s, 0, 1, lanes))
        y_scr[s, :, lanes] = y
        yq_scr[s, 0:24, lanes] = y * yq_scr[s, 24:25, lanes]
        top, rest = halves(dense(gz, rows_of(s, 0, 2, lanes)))
        z_hi[s, :, lanes] = top
        z_lo[s, :, lanes] = rest
        return carry

    def build_slopes(i, carry):
        s, lanes = spans(i)
        gx, gy, gz = gaps(s, lanes)
        sx_scr[s, :, lanes] = dense(gx, rows_of(s, 1, 0, lanes))
        sy_scr[s, :, lanes] = dense(gy, rows_of(s, 1, 1, lanes))
        top, rest = halves(dense(gz, rows_of(s, 1, 2, lanes)))
        sz_hi[s, :, lanes] = top
        sz_lo[s, :, lanes] = rest
        return carry

    lax.fori_loop(0, 2 * CHUNKS, build, 0)

    def put(at, value):
        top, rest = halves(value)
        p_hi[at : at + value.shape[0], :] = top
        p_lo[at : at + value.shape[0], :] = rest

    def accumulate(ref, s, lanes, n):
        a = p_hi[0:n, :], p_lo[0:n, :]
        b = z_hi[s, :, lanes], z_lo[s, :, lanes]
        ref[s] += triple_nt(a, b)

    def halo_chunk(i, carry):
        s, lanes = spans(i)
        for k in range(5):
            put(32 * k, x_scr[s, 0:32, lanes] * yq_scr[s, 19 + k : 20 + k, lanes])
        for k in range(5):
            put(YH + 16 * k, yq_scr[s, 0:16, lanes] * x_scr[s, 35 + k : 36 + k, lanes])
        edge = yq_scr[s, 16:24, lanes]
        for k in range(3):
            first = edge * x_scr[s, 35 + 2 * k : 36 + 2 * k, lanes]
            if k < 2:
                second = edge * x_scr[s, 36 + 2 * k : 37 + 2 * k, lanes]
            else:
                second = jnp.zeros_like(first)
            put(YH + XH + 16 * k, jnp.concatenate([first, second], axis=0))
        accumulate(hal, s, lanes, HALO)
        return carry

    hal[...] = jnp.zeros_like(hal)
    edges = []
    for s in range(2):
        lax.fori_loop(s * CHUNKS, (s + 1) * CHUNKS, halo_chunk, 0)
        if s == 0:
            pl.semaphore_wait(gate, ROWS - 1)
        at = 2 + 6 * s
        edges += [
            remote(hal.at[s, 0:YH], yr.at[s], at, at + 1, (row, dn_c)),
            remote(hal.at[s, YH : YH + XH], xr.at[s], at + 2, at + 3, (dn_r, col)),
            remote(hal.at[s, YH + XH : HALO], cr.at[s], at + 4, at + 5, (dn_r, dn_c)),
        ]
        for copy in edges[3 * s :]:
            copy.start()

    lax.fori_loop(0, 2 * CHUNKS, build_slopes, 0)

    def inner_chunk(i, carry):
        s, lanes = spans(i)
        for x in range(32):
            put(16 * x, yq_scr[s, 0:16, lanes] * x_scr[s, x : x + 1, lanes])
        accumulate(mesh, s, lanes, 512)
        return carry

    mesh[...] = jnp.zeros_like(mesh)
    lax.fori_loop(0, 2 * CHUNKS, inner_chunk, 0)

    for copy in loads[1:]:
        copy.wait()
    for h in range(2):
        zc, zs, fc, fs, lc, ls = [tab[2 * k + h] for k in range(6)]
        for par in range(2):
            at = slice(128 * par, 128 * par + 128)
            wb[h, par, 0:128, 0:256] = zc[at]
            wb[h, par, 0:128, 256:512] = zs[at]
            wb[h, par, 128:256, 0:256] = -zs[at]
            wb[h, par, 128:256, 256:512] = zc[at]
        for ref, c, s in ((fb, fc, fs), (gb, fc, -fs), (lb, lc, -ls)):
            ref[h, 0:256, 0:256] = c
            ref[h, 0:256, 256:512] = s
            ref[h, 256:512, 0:256] = -s
            ref[h, 256:512, 256:512] = c

    remote(gsend.at[0 : ROWS - 1], grecv.at[0 : ROWS - 1], 0, 1, (up_r, col)).wait()
    lane = lax.broadcasted_iota(jnp.int32, (16, 256), 1)

    def trade(par, bits, load, store):
        for rest in range(4):
            base = [(a << bits[0]) + (b << bits[1]) + (rest << (2 if bits[0] == 0 else 0))
                    for b in range(2) for a in range(2)]
            blocks = [load(k) for k in base]
            for i, bit in enumerate(bits):
                step = 1 << bit
                low = (lane & step) == 0
                for k in range(4):
                    if k & (1 << i):
                        continue
                    a, b = blocks[k], blocks[k | (1 << i)]
                    blocks[k] = jnp.where(low, a, pltpu.roll(b, step, 1))
                    blocks[k | (1 << i)] = jnp.where(low, pltpu.roll(a, 256 - step, 1), b)
            for k, block in zip(base, blocks):
                store(k, block)

    def first_load(par, k):
        return grecv[k // 2, par, 16 * (k % 2) : 16 * (k % 2) + 16, :] * (1.0 / 16777216.0)

    def first_store(par, k, block):
        swap[par, 16 * k : 16 * k + 16, :] = block

    def last_store(par, k, block):
        at = 128 * (k % 2) + 16 * (k // 2)
        green[par, at : at + 16, :] = block

    for par in range(2):
        trade(par, (0, 1), functools.partial(first_load, par), functools.partial(first_store, par))
        trade(par, (2, 3), lambda k: swap[par, 16 * k : 16 * k + 16, :],
              functools.partial(last_store, par))

    for copy in edges:
        copy.wait()
    for s in range(2):
        view = mesh.at[s].reshape(32, 16, 256)
        for k in range(5):
            view[:, 11 + k, :] += yr[s, 32 * k : 32 * k + 32]
        for k in range(5):
            view[27 + k] += xr[s, 16 * k : 16 * k + 16]
            view[27 + k, 8:16] += cr[s, 8 * k : 8 * k + 8]

    class Exchange:
        def __init__(self, src, dst, par, first):
            self.src, self.dst, self.first = src.at[par], dst.at[par], first

        def start(self):
            for offset in OFFSETS:
                to = device(*offset)
                src = self.src.at[to[0] * COLS + to[1]]
                remote(src, self.dst.at[me], self.first, self.first + 1, to).start()
            self.dst[me] = self.src[me]

        def wait(self):
            every = slice(0, DEVS - 1)
            remote(
                self.src.at[every], self.dst.at[every], self.first, self.first + 1, (up_r, col)
            ).wait()

    tops = [halves(jnp.concatenate([mesh[0, q, :], mesh[1, q, :]], axis=1))
            for q in (slice(0, 256), slice(256, 512))]
    forward = [Exchange(sbuf, rbuf, par, 14 + 2 * par) for par in range(2)]
    for par in range(2):
        for xh in range(2):
            a = triple_nt((wb[0, par], wb[1, par]), tops[xh])
            for reim in range(2):
                for lh in range(2):
                    sbuf[par, :, 4 * reim + 2 * xh + lh, :] = a[
                        128 * reim : 128 * reim + 128, 128 * lh : 128 * lh + 128
                    ]
        forward[par].start()

    fbig, gbig, lbig = (fb[0], fb[1]), (gb[0], gb[1]), (lb[0], lb[1])
    tc, ts = twid[0], twid[1]

    def stacked(buf, par):
        parts = [
            jnp.concatenate([buf[par, :, 2 * j, :], buf[par, :, 2 * j + 1, :]], axis=1)
            for j in range(4)
        ]
        return jnp.concatenate(parts, axis=0)

    backward = [Exchange(tbuf, qbuf, par, 18 + 2 * par) for par in range(2)]
    for par in range(2):
        forward[par].wait()
        u = triple_nn(fbig, halves(stacked(rbuf, par)))
        ur, ui = u[0:256], u[256:512]
        v = jnp.concatenate([ur * tc + ui * ts, ui * tc - ur * ts], axis=1)
        g = jnp.concatenate([green[par], green[par]], axis=1)
        e = g * triple_nn(halves(v), lbig)
        b = triple_nt(halves(e), lbig)
        br, bi = b[:, 0:256], b[:, 256:512]
        h = jnp.concatenate([br * tc - bi * ts, bi * tc + br * ts], axis=0)
        t = triple_nn(gbig, halves(h))
        for j in range(4):
            for lh in range(2):
                tbuf[par, :, 2 * j + lh, :] = t[
                    128 * j : 128 * j + 128, 128 * lh : 128 * lh + 128
                ]
        backward[par].start()

    for par in range(2):
        backward[par].wait()
        q = stacked(qbuf, par)
        w = wb[0, par], wb[1, par]
        for xh in range(2):
            picked = jnp.concatenate(
                [q[128 * xh : 128 * xh + 128], q[256 + 128 * xh : 384 + 128 * xh]], axis=0
            )
            a = triple_nn(halves(picked.T), w)
            lo = slice(256 * xh, 256 * xh + 256)
            for s in range(2):
                value = a[:, 256 * s : 256 * s + 256]
                pot[s, lo, :] = value if par == 0 else pot[s, lo, :] + value

    for s in range(2):
        view = pot.at[s].reshape(32, 16, 256)
        for k in range(5):
            ys[s, 32 * k : 32 * k + 32] = view[:, 11 + k, :]
        for k in range(5):
            hal[s, 8 * k : 8 * k + 8] = view[27 + k, 8:16]
    back_halo = [
        remote(ys, yb, 22, 23, (row, up_c)),
        remote(pot.at[:, 432:512, :], xb, 24, 25, (up_r, col)),
        remote(hal.at[:, 0:CH], cb, 26, 27, (up_r, up_c)),
    ]
    for copy in back_halo:
        copy.start()

    def spread_out(ref, s, at, value):
        top, rest = halves(value)
        n = value.shape[0]
        ref[s, at : at + n, 0:256] = top
        ref[s, at : at + n, 256:512] = rest
        ref[s, at : at + n, 512:768] = top

    def sample(ref, s, lanes):
        top = jnp.concatenate([z_hi[s, :, lanes], sz_hi[s, :, lanes]], axis=1)
        rest = jnp.concatenate([z_lo[s, :, lanes], sz_lo[s, :, lanes]], axis=1)
        both = dot_nn(ref[s], jnp.concatenate([top, top, rest], axis=0))
        return both[:, 0:GCHUNK], both[:, GCHUNK : 2 * GCHUNK]

    def window(i):
        s = lax.div(i, GCHUNKS)
        return s, pl.ds(pl.multiple_of(lax.rem(i, GCHUNKS) * GCHUNK, GCHUNK), GCHUNK)

    def down(value):
        return jnp.sum(value, axis=0, keepdims=True)

    def gather_inner(i, carry):
        s, lanes = window(i)
        plain, slope = sample(fint, s, lanes)
        a1 = a2 = a3 = jnp.zeros((16, GCHUNK), F32)
        for x in range(32):
            wx, sx = x_scr[s, x : x + 1, lanes], sx_scr[s, x : x + 1, lanes]
            piece = plain[16 * x : 16 * x + 16]
            a1 = a1 + piece * sx
            a2 = a2 + piece * wx
            a3 = a3 + slope[16 * x : 16 * x + 16] * wx
        wy, sy = y_scr[s, 0:16, lanes], sy_scr[s, 0:16, lanes]
        part[s, 0:1, lanes] = down(a1 * wy)
        part[s, 1:2, lanes] = down(a2 * sy)
        part[s, 2:3, lanes] = down(a3 * wy)
        return carry

    def gather_halo(i, carry):
        s, lanes = window(i)
        plain, slope = sample(fhal, s, lanes)
        a1 = a2 = a3 = jnp.zeros((16, GCHUNK), F32)
        b1 = b2 = b3 = jnp.zeros((32, GCHUNK), F32)
        e1 = e2 = e3 = jnp.zeros((8, GCHUNK), F32)
        for k in range(5):
            wy, sy = y_scr[s, 19 + k : 20 + k, lanes], sy_scr[s, 19 + k : 20 + k, lanes]
            wx, sx = x_scr[s, 35 + k : 36 + k, lanes], sx_scr[s, 35 + k : 36 + k, lanes]
            piece = plain[32 * k : 32 * k + 32]
            b1 = b1 + piece * wy
            b2 = b2 + piece * sy
            b3 = b3 + slope[32 * k : 32 * k + 32] * wy
            at = YH + 16 * k
            piece = plain[at : at + 16]
            a1 = a1 + piece * sx
            a2 = a2 + piece * wx
            a3 = a3 + slope[at : at + 16] * wx
            at = YH + XH + 8 * k
            piece = plain[at : at + 8]
            e1 = e1 + piece * sx
            e2 = e2 + piece * wx
            e3 = e3 + slope[at : at + 8] * wx
        wy, sy = y_scr[s, 0:16, lanes], sy_scr[s, 0:16, lanes]
        vy, ty = y_scr[s, 16:24, lanes], sy_scr[s, 16:24, lanes]
        wx, sx = x_scr[s, 0:32, lanes], sx_scr[s, 0:32, lanes]

        def finish(d, a, m, e, n, b, q):
            total = part[s, d : d + 1, lanes] + down(a * m) + down(e * n) + down(b * q)
            forces[d, pl.ds(s, 1), lanes] = -yq_scr[s, 24:25, lanes] * total

        finish(0, a1, wy, e1, vy, b1, sx)
        finish(1, a2, sy, e2, ty, b2, wx)
        finish(2, a3, wy, e3, vy, b3, wx)
        return carry

    for s in range(2):
        spread_out(fint, s, 0, pot[s])
    lax.fori_loop(0, 2 * GCHUNKS, gather_inner, 0)

    for copy in back_halo:
        copy.wait()
    for s in range(2):
        for at, ref in ((0, yb), (YH, xb), (YH + XH, cb)):
            spread_out(fhal, s, at, ref[s])

    lax.fori_loop(0, 2 * GCHUNKS, gather_halo, 0)


def shards(consts, cell_index, fraction, charge, atom_count, influence):
    vmem = pl.BlockSpec(memory_space=pltpu.VMEM)
    anywhere = pl.BlockSpec(memory_space=pl.ANY)
    args = [
        jnp.transpose(cell_index, (1, 0, 2)), jnp.transpose(fraction, (1, 0, 2)), charge,
        jnp.transpose(atom_count), influence, jnp.asarray(consts[0]), jnp.asarray(consts[1]),
    ]
    v = pltpu.VMEM
    scratch = [
        v((32, 16, 256), F32), v((12, 256, 256), BF16), v((2, 256, 256), F32),
        v((2, 6, 6, ATOMS), F32), v((2, 40, ATOMS), F32), v((2, 24, ATOMS), F32),
        v((2, 25, ATOMS), F32), v((2, 256, ATOMS), BF16), v((2, 256, ATOMS), BF16),
        v((2, 40, ATOMS), F32), v((2, 24, ATOMS), F32), v((2, 256, ATOMS), BF16),
        v((2, 256, ATOMS), BF16), v((512, CHUNK), BF16), v((512, CHUNK), BF16),
        v((2, HALO, 256), F32), v((2, YH, 256), F32), v((2, XH, 256), F32), v((2, CH, 256), F32),
        v((2, 512, 256), F32),
        v((ROWS, 2, 32, 256), F32), v((ROWS, 2, 32, 256), F32), v((2, 256, 256), F32),
        v((2, 2, 256, 512), BF16), v((2, 512, 512), BF16), v((2, 512, 512), BF16),
        v((2, 512, 512), BF16),
        v((2, DEVS, 8, 128), F32), v((2, DEVS, 8, 128), F32), v((2, DEVS, 8, 128), F32),
        v((2, DEVS, 8, 128), F32), v((2, 512, 256), F32),
        v((2, YH, 256), F32), v((2, YH, 256), F32), v((2, XH, 256), F32), v((2, CH, 256), F32),
        v((2, 512, 768), BF16), v((2, HALO, 768), BF16), v((2, 3, ATOMS), F32),
        v((2, 256, 256), F32),
        pltpu.SemaphoreType.DMA((28,)), pltpu.SemaphoreType.DMA((3,)), pltpu.SemaphoreType.REGULAR,
    ]
    out = pl.pallas_call(
        kernel,
        out_shape=jax.ShapeDtypeStruct((3, 2, ATOMS), F32),
        in_specs=[vmem] * 4 + [anywhere] * 3,
        out_specs=vmem,
        scratch_shapes=scratch,
        compiler_params=pltpu.CompilerParams(
            collective_id=0, has_side_effects=True, vmem_limit_bytes=66_000_000
        ),
    )(*args)
    return jnp.transpose(out, (1, 0, 2))


def solution(mesh):
    placed = (
        P(None, None, ("row", "col")),
        P(None, None, ("row", "col")),
        P(None, ("row", "col")),
        P(None, ("row", "col")),
        P("row", "col", None),
    )
    return jax.shard_map(
        functools.partial(shards, tables()), mesh=mesh, in_specs=placed,
        out_specs=P(None, None, ("row", "col")), check_vma=False,
    )
```

```python
import functools

import jax
import jax.numpy as jnp
import numpy as np
from jax import lax
from jax.experimental import pallas as pl
from jax.experimental.pallas import tpu as pltpu
from jax.sharding import PartitionSpec as P

F32 = jnp.float32
BF16 = jnp.bfloat16
MESH = pl.DeviceIdType.MESH

K = 256
ROWS = 8
COLS = 16
DEVS = ROWS * COLS
ATOMS = 2048
CHUNK = 512
CHUNKS = ATOMS // CHUNK
GCHUNK = 256
GCHUNKS = ATOMS // GCHUNK

YH, XH, CH = 160, 80, 48
HALO = YH + XH + CH
MESH_ROWS = 592


def far_first():
    offsets = [d for d in np.ndindex(4, 4, 4, 2) if d != (0, 0, 0, 0)]
    offsets.sort(key=lambda d: (-sum(min(k, 4 - k) for k in d[:3]), d[3], d[0] + 2 * d[1] + 3 * d[2]))
    lanes = {}
    for d in offsets:
        lanes.setdefault(d[0] or 10 + d[1] if d[0] or d[1] else 20 + d[2], []).append(d)
    out = []
    while any(lanes.values()):
        out += [lane.pop(0) for lane in lanes.values() if lane]
    return out


OFFSETS = far_first()


def halves(x):
    top = x.astype(BF16)
    return top, (x - top.astype(F32)).astype(BF16)


def np_halves(x):
    x = np.asarray(x, np.float32)
    top = x.astype(jnp.bfloat16)
    return [top, (x - top.astype(np.float32)).astype(jnp.bfloat16)]


def tables():
    d = np.arange(DEVS)
    waves = 16 * (d % COLS) + 2 * (d // COLS) + (d % COLS >= COLS // 2)
    turn = 2.0 * np.pi / K
    angle = (waves[:, None] * np.arange(K)[None, :] % K) * turn
    sines = -np.sin(angle)
    sines[0] = 1.0 - 2.0 * (np.arange(K) % 2)
    out = np_halves(np.concatenate([np.cos(angle), sines]))
    spot = np.arange(256)
    rx, cc = 2 * (spot % 128 // 16) + spot // 128, spot % 16
    angle = ((rx[:, None] * rx[None, :] + cc[:, None] * cc[None, :]) % 16) * (16 * turn)
    out += np_halves(np.cos(angle)) + np_halves(np.sin(angle))
    xl, yl = spot // 16, spot % 16
    angle = ((xl[:, None] * xl[None, :] + yl[:, None] * yl[None, :]) % 16) * (16 * turn)
    out += np_halves(np.cos(angle)) + np_halves(np.sin(angle))
    angle = ((rx[:, None] * xl[None, :] + cc[:, None] * yl[None, :]) % K) * turn
    twiddles = np.stack([np.cos(angle), np.sin(angle)]).astype(np.float32)
    return np.stack(out), twiddles


def spline_values(f):
    nothing = jnp.zeros_like(f)
    levels = [f, 1.0 - f]
    slopes = levels
    for degree in range(3, 7):
        padded = levels + [nothing]
        following = []
        for o in range(degree):
            value = (f + float(o)) * padded[o]
            if o > 0:
                value = value + (float(degree - o) - f) * padded[o - 1]
            following.append(value * (1.0 / (degree - 1)))
        if degree == 6:
            slopes = [padded[0]] + [padded[o] - padded[o - 1] for o in range(1, 6)]
        levels = following
    return levels, slopes


def dot_nn(a, b):
    return lax.dot_general(a, b, (((1,), (0,)), ((), ())), preferred_element_type=F32)


def dot_nt(a, b):
    return lax.dot_general(a, b, (((1,), (1,)), ((), ())), preferred_element_type=F32)


def triple_nn(a, b):
    left = jnp.concatenate([a[0], a[1], a[0]], axis=1)
    return dot_nn(left, jnp.concatenate([b[0], b[0], b[1]], axis=0))


def triple_nt(a, b):
    left = jnp.concatenate([a[0], a[1], a[0]], axis=1)
    return dot_nt(left, jnp.concatenate([b[0], b[0], b[1]], axis=1))


def dense(gap, rows):
    total = jnp.where(gap == 0, rows[0], 0.0)
    for j in range(1, 6):
        total = jnp.where(gap == j, rows[j], total)
    return total


def tiles_of(anchor, rows, size):
    gap = anchor - lax.broadcasted_iota(jnp.int32, (size, anchor.shape[1]), 0)
    return dense(gap & (size - 1), rows), gap >> (3 if size == 8 else 4)


def kernel(
    cell, frac, charge, count, infl_hbm, tab_hbm, twid_hbm,
    forces,
    infl, tab, twid, w_scr, x_scr, y_scr, yq_scr, z_hi, z_lo, sx_scr, sy_scr, sz_hi, sz_lo,
    p_hi, p_lo, ncell, nfrac, qs, nq, nw_scr, nx_scr, nyq_scr, nz_hi, nz_lo, nacc, xr, mesh, gsend, grecv, glast, green, fb, gb, lb, escr,
    sbuf, rbuf, tbuf, qbuf, pot, ys, corner, yb, xb, cb, fint, fhal, part, swap, gone,
    sems, local, gate,
):
    row = lax.axis_index("row")
    col = lax.axis_index("col")
    me = row * COLS + col
    up_r, dn_r = lax.rem(row + 1, ROWS), lax.rem(row + ROWS - 1, ROWS)
    up_c, dn_c = lax.rem(col + 1, COLS), lax.rem(col + COLS - 1, COLS)
    core = lax.rem(col, 2)
    px = lax.rem(lax.div(col, 2), 2) * 2 + lax.rem(row, 2)
    py, pz = lax.div(col, 4), lax.div(row, 2)

    xs = [lax.rem(px + d, 4) for d in range(4)]
    x_row, x_col = [lax.rem(x, 2) for x in xs], [lax.div(x, 2) * 2 for x in xs]
    y_col = [lax.rem(py + d, 4) * 4 for d in range(4)]
    z_row = [lax.rem(pz + d, 4) * 2 for d in range(4)]
    cores = core, 1 - core

    def device(dx, dy, dz, dc):
        return z_row[dz] + x_row[dx], y_col[dy] + x_col[dx] + cores[dc]

    loads = [
        pltpu.make_async_copy(infl_hbm, infl, local.at[0]),
        pltpu.make_async_copy(tab_hbm, tab, local.at[1]),
        pltpu.make_async_copy(twid_hbm, twid, local.at[2]),
    ]
    for copy in loads:
        copy.start()

    barrier = pltpu.get_barrier_semaphore()

    def greet_column(k, carry):
        to = row, lax.rem(col + k, COLS)
        pl.semaphore_signal(barrier, inc=1, device_id=to, device_id_type=MESH)
        return carry

    def greet_row(k, carry):
        to = lax.rem(row + k, ROWS), col
        pl.semaphore_signal(barrier, inc=1, device_id=to, device_id_type=MESH)
        return carry

    def vouch(k, carry):
        to = lax.rem(row + k, ROWS), col
        pl.semaphore_signal(gate, inc=1, device_id=to, device_id_type=MESH)
        return carry

    lax.fori_loop(1, ROWS, greet_row, 0)
    lax.fori_loop(1, COLS, greet_column, 0)

    def remote(src, dst, send, recv, to):
        return pltpu.make_async_remote_copy(
            src_ref=src, dst_ref=dst, send_sem=sems.at[send], recv_sem=sems.at[recv],
            device_id=to, device_id_type=MESH,
        )

    slot = lax.broadcasted_iota(jnp.int32, (1, ATOMS), 1)
    values, slopes = spline_values(jnp.concatenate([frac[0], frac[1], frac[2]], axis=0))
    for j in range(6):
        w_scr[0, j] = values[j]
        w_scr[1, j] = slopes[j]
    for s in range(2):
        masked = jnp.where(slot < count[0:1, s : s + 1], charge[s : s + 1], 0.0)
        yq_scr[s, 24:25] = masked
        qs[s : s + 1] = masked

    loads[0].wait()
    late = jnp.full((32, 256), col >= COLS // 2)
    for k in range(ROWS):
        gsend[k] = jnp.where(late, infl[:, 2 * k + 1, :], infl[:, 2 * k, :])
    pl.semaphore_wait(barrier, ROWS + COLS - 2)
    lax.fori_loop(1, ROWS, vouch, 0)
    atoms = [
        remote(src, dst, 2 + 2 * k, 3 + 2 * k, (row, dn_c))
        for k, (src, dst) in enumerate(((cell, ncell), (frac, nfrac), (qs, nq)))
    ]
    for copy in atoms:
        copy.start()

    def send_green(k, carry):
        there = lax.rem(row + k, ROWS)
        remote(gsend.at[there], grecv.at[row], 0, 1, (there, col)).start()
        return carry

    lax.fori_loop(1, ROWS, send_green, 0)
    grecv[row] = gsend[row]

    def spans(i):
        s = lax.div(i, CHUNKS)
        return s, pl.ds(pl.multiple_of(lax.rem(i, CHUNKS) * CHUNK, CHUNK), CHUNK)

    def pick(kind):
        return lambda s, dim, lanes: [
            w_scr[kind, j, 2 * dim + s : 2 * dim + s + 1, lanes] for j in range(6)
        ]

    def dense_x(anchor, rows, xo, s, lanes):
        value, tile = tiles_of(anchor, rows, 8)
        for b, at in ((0, 0), (1, 8), (2, 16), (3, 24), (-1, 32)):
            xo[s, at : at + 8, lanes] = jnp.where(tile == b, value, 0.0)

    def dense_z(anchor, rows, hi_ref, lo_ref, s, lanes):
        value, tile = tiles_of(anchor, rows, 16)
        top, rest = halves(value)
        tile = (tile & 15).astype(F32).astype(BF16)
        none = jnp.zeros_like(top)
        for b in range(16):
            here = tile == jnp.asarray(float(b), BF16)
            hi_ref[s, 16 * b : 16 * b + 16, lanes] = jnp.where(here, top, none)
            lo_ref[s, 16 * b : 16 * b + 16, lanes] = jnp.where(here, rest, none)

    def dense_all(i, s, kind, xo, yo, hi_ref, lo_ref):
        rows_of = pick(kind)
        for k in range(CHUNK // 128):
            lanes = pl.ds(pl.multiple_of(i * CHUNK + 128 * k, 128), 128)
            dense_x(cell[0, s : s + 1, lanes] - row * 32, rows_of(s, 0, lanes), xo, s, lanes)
            anchor = cell[1, s : s + 1, lanes] - col * 16
            value, tile = tiles_of(anchor, rows_of(s, 1, lanes), 8)
            for b, at in ((0, 0), (1, 8), (-1, 16)):
                y = jnp.where(tile == b, value, 0.0)
                yo[s, at : at + 8, lanes] = y
                if kind == 0:
                    yq_scr[s, at : at + 8, lanes] = y * yq_scr[s, 24:25, lanes]
            dense_z(cell[2, s : s + 1, lanes], rows_of(s, 2, lanes), hi_ref, lo_ref, s, lanes)

    def build_next(s):
        def body(i, carry):
            for k in range(CHUNK // 128):
                lanes = pl.ds(pl.multiple_of(i * CHUNK + 128 * k, 128), 128)
                rows_of = [
                    [nw_scr[j, 2 * d + s : 2 * d + s + 1, lanes] for j in range(6)]
                    for d in range(3)
                ]
                dense_x(ncell[0, s : s + 1, lanes] - row * 32, rows_of[0], nx_scr, s, lanes)
                anchor = ncell[1, s : s + 1, lanes] - up_c * 16
                value, tile = tiles_of(anchor, rows_of[1], 8)
                value = jnp.where(tile == -1, value, 0.0) * nq[s : s + 1, lanes]
                nyq_scr[s, :, lanes] = value
                dense_z(ncell[2, s : s + 1, lanes], rows_of[2], nz_hi, nz_lo, s, lanes)
            return carry

        lax.fori_loop(0, CHUNKS, body, 0)

    def build(s):
        def body(i, carry):
            dense_all(i, s, 0, x_scr, y_scr, z_hi, z_lo)
            return carry

        lax.fori_loop(0, CHUNKS, body, 0)

    def build_slopes(i, carry):
        for s in range(2):
            dense_all(i, s, 1, sx_scr, sy_scr, sz_hi, sz_lo)
        return carry

    build(0)

    def put(slot, at, value):
        top, rest = halves(value)
        p_hi[slot, at : at + value.shape[0], :] = top
        p_lo[slot, at : at + value.shape[0], :] = rest

    def pairs(fill, ref, zs, low, high):
        def body(i, carry):
            for slot in range(2):
                fill(slot, *spans(2 * i + slot))
            for slot in range(2):
                s, lanes = spans(2 * i + slot)
                a = p_hi[slot, low:high, :], p_lo[slot, low:high, :]
                b = zs[0][s, :, lanes], zs[1][s, :, lanes]
                ref[s, low:high, :] += triple_nt(a, b)
            return carry

        return body

    def fill_next(slot, s, lanes):
        for k in range(5):
            put(slot, 32 * k, nx_scr[s, 0:32, lanes] * nyq_scr[s, 3 + k : 4 + k, lanes])
        edge = nyq_scr[s, :, lanes]
        for k in range(3):
            first = edge * nx_scr[s, 35 + 2 * k : 36 + 2 * k, lanes]
            if k < 2:
                second = edge * nx_scr[s, 36 + 2 * k : 37 + 2 * k, lanes]
            else:
                second = jnp.zeros_like(first)
            put(slot, YH + 16 * k, jnp.concatenate([first, second], axis=0))

    def fill_inner(slot, s, lanes):
        for x in range(32):
            put(slot, 16 * x, yq_scr[s, 0:16, lanes] * x_scr[s, x : x + 1, lanes])

    def fill_edge(slot, s, lanes):
        for k in range(5):
            put(slot, 512 + 16 * k, yq_scr[s, 0:16, lanes] * x_scr[s, 35 + k : 36 + k, lanes])

    def fill_both(slot, s, lanes):
        fill_inner(slot, s, lanes)
        fill_edge(slot, s, lanes)

    nacc[...] = jnp.zeros_like(nacc)
    mesh[...] = jnp.zeros_like(mesh)
    edges = []

    def half(s):
        return s * CHUNKS // 2, (s + 1) * CHUNKS // 2

    def spread_own(s, fill, low, high):
        lax.fori_loop(*half(s), pairs(fill, mesh, (z_hi, z_lo), low, high), 0)

    def spread_next(s):
        lax.fori_loop(*half(s), pairs(fill_next, nacc, (nz_hi, nz_lo), 0, YH + CH), 0)

    def send_edge(s):
        view = mesh.at[s].reshape(MESH_ROWS // 16, 16, 256)
        for k in range(5):
            view[32 + k, 8:16] += nacc[s, YH + 8 * k : YH + 8 * k + 8]
        edges.append(remote(mesh.at[s, 512:MESH_ROWS], xr.at[s], 8 + 2 * s, 9 + 2 * s, (dn_r, col)))
        edges[s].start()

    spread_own(0, fill_both, 0, MESH_ROWS)
    for copy in atoms:
        copy.wait()
    values, _ = spline_values(jnp.concatenate([nfrac[0], nfrac[1], nfrac[2]], axis=0))
    for j in range(6):
        nw_scr[j] = values[j]
    build_next(0)
    spread_next(0)
    send_edge(0)

    pl.semaphore_wait(gate, ROWS - 1)
    first = me == 0

    @pl.when(col == COLS // 2)
    def _():
        gone[...] = infl[:, 0, :]
        remote(gone, glast.at[row], 12, 13, (0, 0)).start()

    build(1)
    build_next(1)
    spread_own(1, fill_edge, 512, MESH_ROWS)
    spread_next(1)
    send_edge(1)

    class Exchange:
        def __init__(self, src, dst, par, first):
            self.src, self.dst, self.first = src.at[par], dst.at[par], first

        def start(self):
            for offset in OFFSETS:
                to = device(*offset)
                src = self.src.at[to[0] * COLS + to[1]]
                remote(src, self.dst.at[me], self.first, self.first + 1, to).start()
            self.dst[me] = self.src[me]

        def wait(self):
            every = slice(0, DEVS - 1)
            remote(
                self.src.at[every], self.dst.at[every], self.first, self.first + 1, (up_r, col)
            ).wait()

    forward = [Exchange(sbuf, rbuf, s, 14 + 2 * s) for s in range(2)]
    backward = [Exchange(tbuf, qbuf, s, 18 + 2 * s) for s in range(2)]

    def send_forward(s):
        edges[s].wait()
        view = mesh.at[s].reshape(MESH_ROWS // 16, 16, 256)
        for k in range(5):
            view[0:32, 11 + k, :] += nacc[s, 32 * k : 32 * k + 32]
        for k in range(5):
            view[27 + k] += xr[s, 16 * k : 16 * k + 16]
        a = triple_nt((tab[0], tab[1]), halves(mesh[s, 0:512]))
        for reim in range(2):
            for q in range(4):
                sbuf[s, :, 4 * reim + q, :] = a[
                    128 * reim : 128 * reim + 128, 128 * q : 128 * q + 128
                ]
        forward[s].start()

    for copy in loads[1:]:
        copy.wait()

    send_forward(0)
    spread_own(1, fill_inner, 0, 512)

    for h in range(2):
        fc, fs, lc, ls = [tab[2 + 2 * k + h] for k in range(4)]
        for ref, c, q in ((fb, fc, fs), (gb, fc, -fs), (lb, lc, -ls)):
            ref[h, 0:256, 0:256] = c
            ref[h, 0:256, 256:512] = q
            ref[h, 256:512, 0:256] = -q
            ref[h, 256:512, 256:512] = c
    some = slice(0, ROWS - 1)
    remote(gsend.at[some], grecv.at[some], 0, 1, (up_r, col)).wait()
    lane = lax.broadcasted_iota(jnp.int32, (16, 256), 1)

    def trade(bits, load, store):
        for rest in range(4):
            base = [(a << bits[0]) + (b << bits[1]) + (rest << (2 if bits[0] == 0 else 0))
                    for b in range(2) for a in range(2)]
            blocks = [load(k) for k in base]
            for i, bit in enumerate(bits):
                step = 1 << bit
                low = (lane & step) == 0
                for k in range(4):
                    if k & (1 << i):
                        continue
                    a, b = blocks[k], blocks[k | (1 << i)]
                    blocks[k] = jnp.where(low, a, pltpu.roll(b, step, 1))
                    blocks[k | (1 << i)] = jnp.where(low, pltpu.roll(a, 256 - step, 1), b)
            for k, block in zip(base, blocks):
                store(k, block)

    def in_mode_order(ref, plane, scale):
        def load(k):
            return ref[k // 2, 16 * (k % 2) : 16 * (k % 2) + 16, :] * scale

        def keep(k, block):
            swap[16 * k : 16 * k + 16, :] = block

        def put_in_place(k, block):
            at = 128 * (k % 2) + 16 * (k // 2)
            green[plane, at : at + 16, :] = block

        trade((0, 1), load, keep)
        trade((2, 3), lambda k: swap[16 * k : 16 * k + 16, :], put_in_place)

    unit = 1.0 / float(K) ** 3
    lax.fori_loop(0, CHUNKS, build_slopes, 0)
    in_mode_order(grecv, 0, jnp.where(first, unit, 2.0 * unit))

    @pl.when(first)
    def _():
        remote(glast, glast, 12, 13, (1, 0)).wait_recv()
        in_mode_order(glast, 1, unit)

    @pl.when(col == COLS // 2)
    def _():
        remote(gone, glast.at[0], 12, 13, (0, 0)).wait_send()

    send_forward(1)

    tc, ts = twid[0], twid[1]

    def stacked(buf, par):
        parts = [
            jnp.concatenate([buf[par, :, 2 * j, :], buf[par, :, 2 * j + 1, :]], axis=1)
            for j in range(4)
        ]
        return jnp.concatenate(parts, axis=0)

    def modes(u):
        ur, ui = u[0:256], u[256:512]
        v = jnp.concatenate([ur * tc + ui * ts, ui * tc - ur * ts], axis=1)
        return triple_nn(halves(v), (lb[0], lb[1]))

    def turn(s, carry):
        Exchange(sbuf, rbuf, s, 14 + 2 * s).wait()

        @pl.when(me != 0)
        def _():
            u = triple_nn((fb[0], fb[1]), halves(stacked(rbuf, s)))
            escr[...] = jnp.concatenate([green[0], green[0]], axis=1) * modes(u)

        @pl.when(me == 0)
        def _():
            x = halves(stacked(rbuf, s))
            left = fb[0, :, 0:256], fb[1, :, 0:256]
            a = modes(triple_nn(left, (x[0][0:256], x[1][0:256])))
            b = modes(triple_nn(left, (x[0][256:512], x[1][256:512])))
            escr[:, 0:256] = green[0] * a[:, 0:256] - green[1] * b[:, 256:512]
            escr[:, 256:512] = green[0] * a[:, 256:512] + green[1] * b[:, 0:256]

        b = triple_nt(halves(escr[...]), (lb[0], lb[1]))
        br, bi = b[:, 0:256], b[:, 256:512]
        h = jnp.concatenate([br * tc - bi * ts, bi * tc + br * ts], axis=0)
        t = triple_nn((gb[0], gb[1]), halves(h))
        for j in range(4):
            for lh in range(2):
                tbuf[s, :, 2 * j + lh, :] = t[
                    128 * j : 128 * j + 128, 128 * lh : 128 * lh + 128
                ]
        Exchange(tbuf, qbuf, s, 18 + 2 * s).start()
        return carry

    lax.fori_loop(0, 2, turn, 0)

    back = []

    def take_back(s):
        backward[s].wait()
        q = stacked(qbuf, s)
        for xh in range(2):
            picked = jnp.concatenate(
                [q[128 * xh : 128 * xh + 128], q[256 + 128 * xh : 384 + 128 * xh]], axis=0
            )
            pot[s, 256 * xh : 256 * xh + 256, :] = triple_nn(halves(picked.T), (tab[0], tab[1]))
        view = pot.at[s].reshape(32, 16, 256)
        for k in range(5):
            ys[s, 32 * k : 32 * k + 32] = view[:, 11 + k, :]
        for k in range(5):
            corner[s, 8 * k : 8 * k + 8] = view[27 + k, 8:16]
        at = 22 + 6 * s
        back.append([
            remote(ys.at[s], yb.at[s], at, at + 1, (row, up_c)),
            remote(pot.at[s, 432:512], xb.at[s], at + 2, at + 3, (up_r, col)),
            remote(corner.at[s], cb.at[s], at + 4, at + 5, (up_r, up_c)),
        ])
        for copy in back[s]:
            copy.start()
        spread_out(fint, s, 0, pot[s])

    def take_halo(s):
        for copy in back[s]:
            copy.wait()
        for at, ref in ((0, yb), (YH, xb), (YH + XH, cb)):
            spread_out(fhal, s, at, ref[s])

    def spread_out(ref, s, at, value):
        top, rest = halves(value)
        n = value.shape[0]
        ref[s, at : at + n, 0:256] = top
        ref[s, at : at + n, 256:512] = rest
        ref[s, at : at + n, 512:768] = top

    def sample(ref, s, lanes):
        top = jnp.concatenate([z_hi[s, :, lanes], sz_hi[s, :, lanes]], axis=1)
        rest = jnp.concatenate([z_lo[s, :, lanes], sz_lo[s, :, lanes]], axis=1)
        both = dot_nn(ref[s], jnp.concatenate([top, top, rest], axis=0))
        return both[:, 0:GCHUNK], both[:, GCHUNK : 2 * GCHUNK]

    def window(i):
        s = lax.div(i, GCHUNKS)
        return s, pl.ds(pl.multiple_of(lax.rem(i, GCHUNKS) * GCHUNK, GCHUNK), GCHUNK)

    def down(value):
        return jnp.sum(value, axis=0, keepdims=True)

    def twice(body):
        return lambda i, carry: body(2 * i + 1, body(2 * i, carry))

    def gather_inner(i, carry):
        s, lanes = window(i)
        plain, slope = sample(fint, s, lanes)
        a1 = a2 = a3 = jnp.zeros((16, GCHUNK), F32)
        for x in range(32):
            wx, sx = x_scr[s, x : x + 1, lanes], sx_scr[s, x : x + 1, lanes]
            piece = plain[16 * x : 16 * x + 16]
            a1 = a1 + piece * sx
            a2 = a2 + piece * wx
            a3 = a3 + slope[16 * x : 16 * x + 16] * wx
        wy, sy = y_scr[s, 0:16, lanes], sy_scr[s, 0:16, lanes]
        part[s, 0:1, lanes] = down(a1 * wy)
        part[s, 1:2, lanes] = down(a2 * sy)
        part[s, 2:3, lanes] = down(a3 * wy)
        return carry

    def gather_halo(i, carry):
        s, lanes = window(i)
        plain, slope = sample(fhal, s, lanes)
        a1 = a2 = a3 = jnp.zeros((16, GCHUNK), F32)
        b1 = b2 = b3 = jnp.zeros((32, GCHUNK), F32)
        e1 = e2 = e3 = jnp.zeros((8, GCHUNK), F32)
        for k in range(5):
            wy, sy = y_scr[s, 19 + k : 20 + k, lanes], sy_scr[s, 19 + k : 20 + k, lanes]
            wx, sx = x_scr[s, 35 + k : 36 + k, lanes], sx_scr[s, 35 + k : 36 + k, lanes]
            piece = plain[32 * k : 32 * k + 32]
            b1 = b1 + piece * wy
            b2 = b2 + piece * sy
            b3 = b3 + slope[32 * k : 32 * k + 32] * wy
            at = YH + 16 * k
            piece = plain[at : at + 16]
            a1 = a1 + piece * sx
            a2 = a2 + piece * wx
            a3 = a3 + slope[at : at + 16] * wx
            at = YH + XH + 8 * k
            piece = plain[at : at + 8]
            e1 = e1 + piece * sx
            e2 = e2 + piece * wx
            e3 = e3 + slope[at : at + 8] * wx
        wy, sy = y_scr[s, 0:16, lanes], sy_scr[s, 0:16, lanes]
        vy, ty = y_scr[s, 16:24, lanes], sy_scr[s, 16:24, lanes]
        wx, sx = x_scr[s, 0:32, lanes], sx_scr[s, 0:32, lanes]

        def finish(d, a, m, e, n, b, q):
            total = part[s, d : d + 1, lanes] + down(a * m) + down(e * n) + down(b * q)
            forces[d, pl.ds(s, 1), lanes] = -yq_scr[s, 24:25, lanes] * total

        finish(0, a1, wy, e1, vy, b1, sx)
        finish(1, a2, sy, e2, ty, b2, wx)
        finish(2, a3, wy, e3, vy, b3, wx)
        return carry

    def gather(body, s):
        lax.fori_loop(s * GCHUNKS // 2, (s + 1) * GCHUNKS // 2, twice(body), 0)

    take_back(0)
    gather(gather_inner, 0)
    take_back(1)
    gather(gather_inner, 1)
    take_halo(0)
    gather(gather_halo, 0)
    take_halo(1)
    gather(gather_halo, 1)


def shards(consts, cell_index, fraction, charge, atom_count, influence):
    vmem = pl.BlockSpec(memory_space=pltpu.VMEM)
    anywhere = pl.BlockSpec(memory_space=pl.ANY)
    args = [
        jnp.transpose(cell_index, (1, 0, 2)), jnp.transpose(fraction, (1, 0, 2)), charge,
        jnp.transpose(atom_count), influence, jnp.asarray(consts[0]), jnp.asarray(consts[1]),
    ]
    v = pltpu.VMEM
    scratch = [
        v((32, 16, 256), F32), v((10, 256, 256), BF16), v((2, 256, 256), F32),
        v((2, 6, 6, ATOMS), F32), v((2, 40, ATOMS), F32), v((2, 24, ATOMS), F32),
        v((2, 25, ATOMS), F32), v((2, 256, ATOMS), BF16), v((2, 256, ATOMS), BF16),
        v((2, 40, ATOMS), F32), v((2, 24, ATOMS), F32), v((2, 256, ATOMS), BF16),
        v((2, 256, ATOMS), BF16), v((2, MESH_ROWS, CHUNK), BF16), v((2, MESH_ROWS, CHUNK), BF16),
        v((3, 2, ATOMS), jnp.int32), v((3, 2, ATOMS), F32), v((2, ATOMS), F32), v((2, ATOMS), F32),
        v((6, 6, ATOMS), F32), v((2, 40, ATOMS), F32), v((2, 8, ATOMS), F32),
        v((2, 256, ATOMS), BF16), v((2, 256, ATOMS), BF16),
        v((2, YH + CH, 256), F32), v((2, XH, 256), F32), v((2, MESH_ROWS, 256), F32),
        v((ROWS, 32, 256), F32), v((ROWS, 32, 256), F32), v((ROWS, 32, 256), F32),
        v((2, 256, 256), F32), v((2, 512, 512), BF16), v((2, 512, 512), BF16),
        v((2, 512, 512), BF16), v((256, 512), F32),
        v((2, DEVS, 8, 128), F32), v((2, DEVS, 8, 128), F32), v((2, DEVS, 8, 128), F32),
        v((2, DEVS, 8, 128), F32), v((2, 512, 256), F32),
        v((2, YH, 256), F32), v((2, 40, 256), F32),
        v((2, YH, 256), F32), v((2, XH, 256), F32), v((2, 40, 256), F32),
        v((2, 512, 768), BF16), v((2, HALO, 768), BF16), v((2, 3, ATOMS), F32),
        v((256, 256), F32), v((32, 256), F32),
        pltpu.SemaphoreType.DMA((34,)), pltpu.SemaphoreType.DMA((3,)), pltpu.SemaphoreType.REGULAR,
    ]
    out = pl.pallas_call(
        kernel,
        out_shape=jax.ShapeDtypeStruct((3, 2, ATOMS), F32),
        in_specs=[vmem] * 4 + [anywhere] * 3,
        out_specs=vmem,
        scratch_shapes=scratch,
        compiler_params=pltpu.CompilerParams(
            collective_id=0, has_side_effects=True, vmem_limit_bytes=66_000_000
        ),
    )(*args)
    return jnp.transpose(out, (1, 0, 2))


def solution(mesh):
    placed = (
        P(None, None, ("row", "col")),
        P(None, None, ("row", "col")),
        P(None, ("row", "col")),
        P(None, ("row", "col")),
        P("row", "col", None),
    )
    return jax.shard_map(
        functools.partial(shards, tables()), mesh=mesh, in_specs=placed,
        out_specs=P(None, None, ("row", "col")), check_vma=False,
    )
```

```python
import functools

import jax
import jax.numpy as jnp
import numpy as np
from jax import lax
from jax.experimental import pallas as pl
from jax.experimental.pallas import tpu as pltpu
from jax.sharding import PartitionSpec as P

F32 = jnp.float32
BF16 = jnp.bfloat16
MESH = pl.DeviceIdType.MESH

K = 256
ROWS = 8
COLS = 16
DEVS = ROWS * COLS
ATOMS = 2048
CHUNK = 512
CHUNKS = ATOMS // CHUNK
GCHUNK = 256
GCHUNKS = ATOMS // GCHUNK

YH, XH, CH = 160, 80, 48
HALO = YH + XH + CH
MESH_ROWS = 592


def far_first():
    offsets = [d for d in np.ndindex(4, 4, 4, 2) if d != (0, 0, 0, 0)]
    offsets.sort(key=lambda d: (-sum(min(k, 4 - k) for k in d[:3]), d[3], d[0] + 2 * d[1] + 3 * d[2]))
    lanes = {}
    for d in offsets:
        lanes.setdefault(d[0] or 10 + d[1] if d[0] or d[1] else 20 + d[2], []).append(d)
    out = []
    while any(lanes.values()):
        out += [lane.pop(0) for lane in lanes.values() if lane]
    return out


OFFSETS = far_first()


def halves(x):
    top = x.astype(BF16)
    return top, (x - top.astype(F32)).astype(BF16)


def np_halves(x):
    x = np.asarray(x, np.float32)
    top = x.astype(jnp.bfloat16)
    return [top, (x - top.astype(np.float32)).astype(jnp.bfloat16)]


def tables():
    d = np.arange(DEVS)
    waves = 16 * (d % COLS) + 2 * (d // COLS) + (d % COLS >= COLS // 2)
    turn = 2.0 * np.pi / K
    angle = (waves[:, None] * np.arange(K)[None, :] % K) * turn
    sines = -np.sin(angle)
    sines[0] = 1.0 - 2.0 * (np.arange(K) % 2)
    out = np_halves(np.concatenate([np.cos(angle), sines]))
    spot = np.arange(256)
    rx, cc = 2 * (spot % 128 // 16) + spot // 128, spot % 16
    angle = ((rx[:, None] * rx[None, :] + cc[:, None] * cc[None, :]) % 16) * (16 * turn)
    out += np_halves(np.cos(angle)) + np_halves(np.sin(angle))
    xl, yl = spot // 16, spot % 16
    angle = ((xl[:, None] * xl[None, :] + yl[:, None] * yl[None, :]) % 16) * (16 * turn)
    out += np_halves(np.cos(angle)) + np_halves(np.sin(angle))
    angle = ((rx[:, None] * xl[None, :] + cc[:, None] * yl[None, :]) % K) * turn
    twiddles = np.stack([np.cos(angle), np.sin(angle)]).astype(np.float32)
    return np.stack(out), twiddles


def spline_values(f):
    nothing = jnp.zeros_like(f)
    levels = [f, 1.0 - f]
    slopes = levels
    for degree in range(3, 7):
        padded = levels + [nothing]
        following = []
        for o in range(degree):
            value = (f + float(o)) * padded[o]
            if o > 0:
                value = value + (float(degree - o) - f) * padded[o - 1]
            following.append(value * (1.0 / (degree - 1)))
        if degree == 6:
            slopes = [padded[0]] + [padded[o] - padded[o - 1] for o in range(1, 6)]
        levels = following
    return levels, slopes


def dot_nn(a, b):
    return lax.dot_general(a, b, (((1,), (0,)), ((), ())), preferred_element_type=F32)


def dot_nt(a, b):
    return lax.dot_general(a, b, (((1,), (1,)), ((), ())), preferred_element_type=F32)


def triple_nn(a, b):
    left = jnp.concatenate([a[0], a[1], a[0]], axis=1)
    return dot_nn(left, jnp.concatenate([b[0], b[0], b[1]], axis=0))


def triple_nt(a, b):
    left = jnp.concatenate([a[0], a[1], a[0]], axis=1)
    return dot_nt(left, jnp.concatenate([b[0], b[0], b[1]], axis=1))


def dense(gap, rows):
    total = jnp.where(gap == 0, rows[0], 0.0)
    for j in range(1, 6):
        total = jnp.where(gap == j, rows[j], total)
    return total


def tiles_of(anchor, rows, size):
    gap = anchor - lax.broadcasted_iota(jnp.int32, (size, anchor.shape[1]), 0)
    return dense(gap & (size - 1), rows), gap >> (3 if size == 8 else 4)


def kernel(
    cell_hbm, frac_hbm, charge_hbm, count_hbm, infl_hbm, tab_hbm, twid_hbm,
    forces,
    cell, frac, charge, count, infl, tab, twid, w_scr, x_scr, y_scr, yq_scr, z_hi, z_lo, sx_scr, sy_scr, sz_hi, sz_lo,
    p_hi, p_lo, ncell, nfrac, qs, nq, nw_scr, nx_scr, nyq_scr, nz_hi, nz_lo, nacc, xr, mesh, gsend, grecv, glast, green, fb, gb, lb, escr,
    sbuf, rbuf, tbuf, qbuf, pot, ys, corner, yb, xb, cb, fint, fhal, part, swap, gone,
    sems, local, gate,
):
    row = lax.axis_index("row")
    col = lax.axis_index("col")
    me = row * COLS + col
    up_r, dn_r = lax.rem(row + 1, ROWS), lax.rem(row + ROWS - 1, ROWS)
    up_c, dn_c = lax.rem(col + 1, COLS), lax.rem(col + COLS - 1, COLS)
    core = lax.rem(col, 2)
    px = lax.rem(lax.div(col, 2), 2) * 2 + lax.rem(row, 2)
    py, pz = lax.div(col, 4), lax.div(row, 2)

    xs = [lax.rem(px + d, 4) for d in range(4)]
    x_row, x_col = [lax.rem(x, 2) for x in xs], [lax.div(x, 2) * 2 for x in xs]
    y_col = [lax.rem(py + d, 4) * 4 for d in range(4)]
    z_row = [lax.rem(pz + d, 4) * 2 for d in range(4)]
    cores = core, 1 - core

    def device(dx, dy, dz, dc):
        return z_row[dz] + x_row[dx], y_col[dy] + x_col[dx] + cores[dc]

    loads = [
        pltpu.make_async_copy(infl_hbm, infl, local.at[0]),
        pltpu.make_async_copy(tab_hbm, tab, local.at[1]),
        pltpu.make_async_copy(twid_hbm, twid, local.at[2]),
    ]
    inputs = [
        pltpu.make_async_copy(src, dst, local.at[3 + k])
        for k, (src, dst) in enumerate((
            (cell_hbm, cell), (frac_hbm, frac), (charge_hbm, charge), (count_hbm, count)
        ))
    ]
    for copy in inputs + loads:
        copy.start()

    barrier = pltpu.get_barrier_semaphore()

    def greet_column(k, carry):
        to = row, lax.rem(col + k, COLS)
        pl.semaphore_signal(barrier, inc=1, device_id=to, device_id_type=MESH)
        return carry

    def greet_row(k, carry):
        to = lax.rem(row + k, ROWS), col
        pl.semaphore_signal(barrier, inc=1, device_id=to, device_id_type=MESH)
        return carry

    def vouch(k, carry):
        to = lax.rem(row + k, ROWS), col
        pl.semaphore_signal(gate, inc=1, device_id=to, device_id_type=MESH)
        return carry

    lax.fori_loop(1, ROWS, greet_row, 0)
    lax.fori_loop(1, COLS, greet_column, 0)

    def remote(src, dst, send, recv, to):
        return pltpu.make_async_remote_copy(
            src_ref=src, dst_ref=dst, send_sem=sems.at[send], recv_sem=sems.at[recv],
            device_id=to, device_id_type=MESH,
        )

    for copy in inputs:
        copy.wait()
    slot = lax.broadcasted_iota(jnp.int32, (1, ATOMS), 1)
    values, slopes = spline_values(jnp.concatenate([frac[0], frac[1], frac[2]], axis=0))
    for j in range(6):
        w_scr[0, j] = values[j]
        w_scr[1, j] = slopes[j]
    for s in range(2):
        masked = jnp.where(slot < count[0:1, s : s + 1], charge[s : s + 1], 0.0)
        yq_scr[s, 24:25] = masked
        qs[s : s + 1] = masked

    loads[0].wait()
    for odd in range(2):

        @pl.when(lax.div(col, COLS // 2) == odd)
        def _():
            for k in range(ROWS):
                gsend[k] = infl[:, 2 * k + odd, :]

    pl.semaphore_wait(barrier, ROWS + COLS - 2)
    lax.fori_loop(1, ROWS, vouch, 0)
    atoms = [
        remote(src, dst, 2 + 2 * k, 3 + 2 * k, (row, dn_c))
        for k, (src, dst) in enumerate(((cell, ncell), (frac, nfrac), (qs, nq)))
    ]
    for copy in atoms:
        copy.start()

    def send_green(k, carry):
        there = lax.rem(row + k, ROWS)
        remote(gsend.at[there], grecv.at[row], 0, 1, (there, col)).start()
        return carry

    lax.fori_loop(1, ROWS, send_green, 0)
    grecv[row] = gsend[row]

    def spans(i):
        s = lax.div(i, CHUNKS)
        return s, pl.ds(pl.multiple_of(lax.rem(i, CHUNKS) * CHUNK, CHUNK), CHUNK)

    def pick(kind):
        return lambda s, dim, lanes: [
            w_scr[kind, j, 2 * dim + s : 2 * dim + s + 1, lanes] for j in range(6)
        ]

    def dense_x(anchor, rows, xo, s, lanes):
        value, tile = tiles_of(anchor, rows, 8)
        for b, at in ((0, 0), (1, 8), (2, 16), (3, 24), (-1, 32)):
            xo[s, at : at + 8, lanes] = jnp.where(tile == b, value, 0.0)

    def dense_z(anchor, rows, hi_ref, lo_ref, s, lanes):
        value, tile = tiles_of(anchor, rows, 16)
        top, rest = halves(value)
        tile = (tile & 15).astype(F32).astype(BF16)
        none = jnp.zeros_like(top)
        for b in range(16):
            here = tile == jnp.asarray(float(b), BF16)
            hi_ref[s, 16 * b : 16 * b + 16, lanes] = jnp.where(here, top, none)
            lo_ref[s, 16 * b : 16 * b + 16, lanes] = jnp.where(here, rest, none)

    def dense_all(i, s, kind, xo, yo, hi_ref, lo_ref):
        rows_of = pick(kind)
        for k in range(CHUNK // 128):
            lanes = pl.ds(pl.multiple_of(i * CHUNK + 128 * k, 128), 128)
            dense_x(cell[0, s : s + 1, lanes] - row * 32, rows_of(s, 0, lanes), xo, s, lanes)
            anchor = cell[1, s : s + 1, lanes] - col * 16
            value, tile = tiles_of(anchor, rows_of(s, 1, lanes), 8)
            for b, at in ((0, 0), (1, 8), (-1, 16)):
                y = jnp.where(tile == b, value, 0.0)
                yo[s, at : at + 8, lanes] = y
                if kind == 0:
                    yq_scr[s, at : at + 8, lanes] = y * yq_scr[s, 24:25, lanes]
            dense_z(cell[2, s : s + 1, lanes], rows_of(s, 2, lanes), hi_ref, lo_ref, s, lanes)

    def build_next(s):
        def body(i, carry):
            for k in range(CHUNK // 128):
                lanes = pl.ds(pl.multiple_of(i * CHUNK + 128 * k, 128), 128)
                rows_of = [
                    [nw_scr[j, 2 * d + s : 2 * d + s + 1, lanes] for j in range(6)]
                    for d in range(3)
                ]
                dense_x(ncell[0, s : s + 1, lanes] - row * 32, rows_of[0], nx_scr, s, lanes)
                anchor = ncell[1, s : s + 1, lanes] - up_c * 16
                value, tile = tiles_of(anchor, rows_of[1], 8)
                value = jnp.where(tile == -1, value, 0.0) * nq[s : s + 1, lanes]
                nyq_scr[s, :, lanes] = value
                dense_z(ncell[2, s : s + 1, lanes], rows_of[2], nz_hi, nz_lo, s, lanes)
            return carry

        lax.fori_loop(0, CHUNKS, body, 0)

    def build(s):
        def body(i, carry):
            dense_all(i, s, 0, x_scr, y_scr, z_hi, z_lo)
            return carry

        lax.fori_loop(0, CHUNKS, body, 0)

    def build_slopes(i, carry):
        for s in range(2):
            dense_all(i, s, 1, sx_scr, sy_scr, sz_hi, sz_lo)
        return carry

    build(0)

    def put(slot, at, value):
        top, rest = halves(value)
        p_hi[slot, at : at + value.shape[0], :] = top
        p_lo[slot, at : at + value.shape[0], :] = rest

    def pairs(fill, ref, zs, low, high):
        def body(i, carry):
            for slot in range(2):
                fill(slot, *spans(2 * i + slot))
            for slot in range(2):
                s, lanes = spans(2 * i + slot)
                a = p_hi[slot, low:high, :], p_lo[slot, low:high, :]
                b = zs[0][s, :, lanes], zs[1][s, :, lanes]
                ref[s, low:high, :] += triple_nt(a, b)
            return carry

        return body

    def fill_next(slot, s, lanes):
        for k in range(5):
            put(slot, 32 * k, nx_scr[s, 0:32, lanes] * nyq_scr[s, 3 + k : 4 + k, lanes])
        edge = nyq_scr[s, :, lanes]
        for k in range(3):
            first = edge * nx_scr[s, 35 + 2 * k : 36 + 2 * k, lanes]
            if k < 2:
                second = edge * nx_scr[s, 36 + 2 * k : 37 + 2 * k, lanes]
            else:
                second = jnp.zeros_like(first)
            put(slot, YH + 16 * k, jnp.concatenate([first, second], axis=0))

    def fill_inner(slot, s, lanes):
        for x in range(32):
            put(slot, 16 * x, yq_scr[s, 0:16, lanes] * x_scr[s, x : x + 1, lanes])

    def fill_edge(slot, s, lanes):
        for k in range(5):
            put(slot, 512 + 16 * k, yq_scr[s, 0:16, lanes] * x_scr[s, 35 + k : 36 + k, lanes])

    def fill_both(slot, s, lanes):
        fill_inner(slot, s, lanes)
        fill_edge(slot, s, lanes)

    nacc[...] = jnp.zeros_like(nacc)
    mesh[...] = jnp.zeros_like(mesh)
    edges = []

    def half(s):
        return s * CHUNKS // 2, (s + 1) * CHUNKS // 2

    def spread_own(s, fill, low, high):
        lax.fori_loop(*half(s), pairs(fill, mesh, (z_hi, z_lo), low, high), 0)

    def spread_next(s):
        lax.fori_loop(*half(s), pairs(fill_next, nacc, (nz_hi, nz_lo), 0, YH + CH), 0)

    def send_edge(s):
        view = mesh.at[s].reshape(MESH_ROWS // 16, 16, 256)
        for k in range(5):
            view[32 + k, 8:16] += nacc[s, YH + 8 * k : YH + 8 * k + 8]
        edges.append(remote(mesh.at[s, 512:MESH_ROWS], xr.at[s], 8 + 2 * s, 9 + 2 * s, (dn_r, col)))
        edges[s].start()

    spread_own(0, fill_both, 0, MESH_ROWS)
    for copy in atoms:
        copy.wait()
    values, _ = spline_values(jnp.concatenate([nfrac[0], nfrac[1], nfrac[2]], axis=0))
    for j in range(6):
        nw_scr[j] = values[j]
    build_next(0)
    spread_next(0)
    send_edge(0)

    pl.semaphore_wait(gate, ROWS - 1)
    first = me == 0

    @pl.when(col == COLS // 2)
    def _():
        gone[...] = infl[:, 0, :]
        remote(gone, glast.at[row], 12, 13, (0, 0)).start()

    build(1)
    build_next(1)
    spread_own(1, fill_edge, 512, MESH_ROWS)
    spread_next(1)
    send_edge(1)

    class Exchange:
        def __init__(self, src, dst, par, first):
            self.src, self.dst, self.first = src.at[par], dst.at[par], first

        def start(self):
            for offset in OFFSETS:
                to = device(*offset)
                src = self.src.at[to[0] * COLS + to[1]]
                remote(src, self.dst.at[me], self.first, self.first + 1, to).start()
            self.dst[me] = self.src[me]

        def wait(self):
            every = slice(0, DEVS - 1)
            remote(
                self.src.at[every], self.dst.at[every], self.first, self.first + 1, (up_r, col)
            ).wait()

    forward = [Exchange(sbuf, rbuf, s, 14 + 2 * s) for s in range(2)]
    backward = [Exchange(tbuf, qbuf, s, 18 + 2 * s) for s in range(2)]

    def send_forward(s):
        edges[s].wait()
        view = mesh.at[s].reshape(MESH_ROWS // 16, 16, 256)
        for k in range(5):
            view[0:32, 11 + k, :] += nacc[s, 32 * k : 32 * k + 32]
        for k in range(5):
            view[27 + k] += xr[s, 16 * k : 16 * k + 16]
        a = triple_nt((tab[0], tab[1]), halves(mesh[s, 0:512]))
        for reim in range(2):
            for q in range(4):
                sbuf[s, :, 4 * reim + q, :] = a[
                    128 * reim : 128 * reim + 128, 128 * q : 128 * q + 128
                ]
        forward[s].start()

    for copy in loads[1:]:
        copy.wait()

    send_forward(0)
    spread_own(1, fill_inner, 0, 512)

    for h in range(2):
        fc, fs, lc, ls = [tab[2 + 2 * k + h] for k in range(4)]
        for ref, c, q in ((fb, fc, fs), (gb, fc, -fs), (lb, lc, -ls)):
            ref[h, 0:256, 0:256] = c
            ref[h, 0:256, 256:512] = q
            ref[h, 256:512, 0:256] = -q
            ref[h, 256:512, 256:512] = c
    some = slice(0, ROWS - 1)
    remote(gsend.at[some], grecv.at[some], 0, 1, (up_r, col)).wait()
    lane = lax.broadcasted_iota(jnp.int32, (16, 256), 1)

    def trade(bits, load, store):
        for rest in range(4):
            base = [(a << bits[0]) + (b << bits[1]) + (rest << (2 if bits[0] == 0 else 0))
                    for b in range(2) for a in range(2)]
            blocks = [load(k) for k in base]
            for i, bit in enumerate(bits):
                step = 1 << bit
                low = (lane & step) == 0
                for k in range(4):
                    if k & (1 << i):
                        continue
                    a, b = blocks[k], blocks[k | (1 << i)]
                    blocks[k] = jnp.where(low, a, pltpu.roll(b, step, 1))
                    blocks[k | (1 << i)] = jnp.where(low, pltpu.roll(a, 256 - step, 1), b)
            for k, block in zip(base, blocks):
                store(k, block)

    def in_mode_order(ref, plane, scale):
        def load(k):
            return ref[k // 2, 16 * (k % 2) : 16 * (k % 2) + 16, :] * scale

        def keep(k, block):
            swap[16 * k : 16 * k + 16, :] = block

        def put_in_place(k, block):
            at = 128 * (k % 2) + 16 * (k // 2)
            green[plane, at : at + 16, :] = block

        trade((0, 1), load, keep)
        trade((2, 3), lambda k: swap[16 * k : 16 * k + 16, :], put_in_place)

    unit = 1.0 / float(K) ** 3
    lax.fori_loop(0, CHUNKS, build_slopes, 0)
    in_mode_order(grecv, 0, jnp.where(first, unit, 2.0 * unit))

    @pl.when(first)
    def _():
        remote(glast, glast, 12, 13, (1, 0)).wait_recv()
        in_mode_order(glast, 1, unit)

    @pl.when(col == COLS // 2)
    def _():
        remote(gone, glast.at[0], 12, 13, (0, 0)).wait_send()

    send_forward(1)

    tc, ts = twid[0], twid[1]

    def stacked(buf, par):
        parts = [
            jnp.concatenate([buf[par, :, 2 * j, :], buf[par, :, 2 * j + 1, :]], axis=1)
            for j in range(4)
        ]
        return jnp.concatenate(parts, axis=0)

    def modes(u):
        ur, ui = u[0:256], u[256:512]
        v = jnp.concatenate([ur * tc + ui * ts, ui * tc - ur * ts], axis=1)
        return triple_nn(halves(v), (lb[0], lb[1]))

    def turn(s, carry):
        Exchange(sbuf, rbuf, s, 14 + 2 * s).wait()

        @pl.when(me != 0)
        def _():
            u = triple_nn((fb[0], fb[1]), halves(stacked(rbuf, s)))
            escr[...] = jnp.concatenate([green[0], green[0]], axis=1) * modes(u)

        @pl.when(me == 0)
        def _():
            x = halves(stacked(rbuf, s))
            left = fb[0, :, 0:256], fb[1, :, 0:256]
            a = modes(triple_nn(left, (x[0][0:256], x[1][0:256])))
            b = modes(triple_nn(left, (x[0][256:512], x[1][256:512])))
            escr[:, 0:256] = green[0] * a[:, 0:256] - green[1] * b[:, 256:512]
            escr[:, 256:512] = green[0] * a[:, 256:512] + green[1] * b[:, 0:256]

        b = triple_nt(halves(escr[...]), (lb[0], lb[1]))
        br, bi = b[:, 0:256], b[:, 256:512]
        h = jnp.concatenate([br * tc - bi * ts, bi * tc + br * ts], axis=0)
        t = triple_nn((gb[0], gb[1]), halves(h))
        for j in range(4):
            for lh in range(2):
                tbuf[s, :, 2 * j + lh, :] = t[
                    128 * j : 128 * j + 128, 128 * lh : 128 * lh + 128
                ]
        Exchange(tbuf, qbuf, s, 18 + 2 * s).start()
        return carry

    lax.fori_loop(0, 2, turn, 0)

    back = []

    def take_back(s):
        backward[s].wait()
        q = stacked(qbuf, s)
        for xh in range(2):
            picked = jnp.concatenate(
                [q[128 * xh : 128 * xh + 128], q[256 + 128 * xh : 384 + 128 * xh]], axis=0
            )
            pot[s, 256 * xh : 256 * xh + 256, :] = triple_nn(halves(picked.T), (tab[0], tab[1]))
        view = pot.at[s].reshape(32, 16, 256)
        for k in range(5):
            ys[s, 32 * k : 32 * k + 32] = view[:, 11 + k, :]
        for k in range(5):
            corner[s, 8 * k : 8 * k + 8] = view[27 + k, 8:16]
        at = 22 + 6 * s
        back.append([
            remote(ys.at[s], yb.at[s], at, at + 1, (row, up_c)),
            remote(pot.at[s, 432:512], xb.at[s], at + 2, at + 3, (up_r, col)),
            remote(corner.at[s], cb.at[s], at + 4, at + 5, (up_r, up_c)),
        ])
        for copy in back[s]:
            copy.start()
        spread_out(fint, s, 0, pot[s])

    def take_halo(s):
        for copy in back[s]:
            copy.wait()
        for at, ref in ((0, yb), (YH, xb), (YH + XH, cb)):
            spread_out(fhal, s, at, ref[s])

    def spread_out(ref, s, at, value):
        top, rest = halves(value)
        n = value.shape[0]
        ref[s, at : at + n, 0:256] = top
        ref[s, at : at + n, 256:512] = rest
        ref[s, at : at + n, 512:768] = top

    def sample(ref, s, lanes):
        top = jnp.concatenate([z_hi[s, :, lanes], sz_hi[s, :, lanes]], axis=1)
        rest = jnp.concatenate([z_lo[s, :, lanes], sz_lo[s, :, lanes]], axis=1)
        both = dot_nn(ref[s], jnp.concatenate([top, top, rest], axis=0))
        return both[:, 0:GCHUNK], both[:, GCHUNK : 2 * GCHUNK]

    def window(i):
        s = lax.div(i, GCHUNKS)
        return s, pl.ds(pl.multiple_of(lax.rem(i, GCHUNKS) * GCHUNK, GCHUNK), GCHUNK)

    def down(value):
        return jnp.sum(value, axis=0, keepdims=True)

    def four(body):
        def several(i, carry):
            for k in range(4):
                carry = body(4 * i + k, carry)
            return carry

        return several

    def gather_inner(i, carry):
        s, lanes = window(i)
        plain, slope = sample(fint, s, lanes)
        a1 = a2 = a3 = jnp.zeros((16, GCHUNK), F32)
        for x in range(32):
            wx, sx = x_scr[s, x : x + 1, lanes], sx_scr[s, x : x + 1, lanes]
            piece = plain[16 * x : 16 * x + 16]
            a1 = a1 + piece * sx
            a2 = a2 + piece * wx
            a3 = a3 + slope[16 * x : 16 * x + 16] * wx
        wy, sy = y_scr[s, 0:16, lanes], sy_scr[s, 0:16, lanes]
        part[s, 0:1, lanes] = down(a1 * wy)
        part[s, 1:2, lanes] = down(a2 * sy)
        part[s, 2:3, lanes] = down(a3 * wy)
        return carry

    def gather_halo(i, carry):
        s, lanes = window(i)
        plain, slope = sample(fhal, s, lanes)
        a1 = a2 = a3 = jnp.zeros((16, GCHUNK), F32)
        b1 = b2 = b3 = jnp.zeros((32, GCHUNK), F32)
        e1 = e2 = e3 = jnp.zeros((8, GCHUNK), F32)
        for k in range(5):
            wy, sy = y_scr[s, 19 + k : 20 + k, lanes], sy_scr[s, 19 + k : 20 + k, lanes]
            wx, sx = x_scr[s, 35 + k : 36 + k, lanes], sx_scr[s, 35 + k : 36 + k, lanes]
            piece = plain[32 * k : 32 * k + 32]
            b1 = b1 + piece * wy
            b2 = b2 + piece * sy
            b3 = b3 + slope[32 * k : 32 * k + 32] * wy
            at = YH + 16 * k
            piece = plain[at : at + 16]
            a1 = a1 + piece * sx
            a2 = a2 + piece * wx
            a3 = a3 + slope[at : at + 16] * wx
            at = YH + XH + 8 * k
            piece = plain[at : at + 8]
            e1 = e1 + piece * sx
            e2 = e2 + piece * wx
            e3 = e3 + slope[at : at + 8] * wx
        wy, sy = y_scr[s, 0:16, lanes], sy_scr[s, 0:16, lanes]
        vy, ty = y_scr[s, 16:24, lanes], sy_scr[s, 16:24, lanes]
        wx, sx = x_scr[s, 0:32, lanes], sx_scr[s, 0:32, lanes]

        def finish(d, a, m, e, n, b, q):
            total = part[s, d : d + 1, lanes] + down(a * m) + down(e * n) + down(b * q)
            forces[d, pl.ds(s, 1), lanes] = -yq_scr[s, 24:25, lanes] * total

        finish(0, a1, wy, e1, vy, b1, sx)
        finish(1, a2, sy, e2, ty, b2, wx)
        finish(2, a3, wy, e3, vy, b3, wx)
        return carry

    def gather(body, s):
        lax.fori_loop(s * GCHUNKS // 4, (s + 1) * GCHUNKS // 4, four(body), 0)

    take_back(0)
    gather(gather_inner, 0)
    take_back(1)
    gather(gather_inner, 1)
    take_halo(0)
    gather(gather_halo, 0)
    take_halo(1)
    gather(gather_halo, 1)


def shards(consts, cell_index, fraction, charge, atom_count, influence):
    vmem = pl.BlockSpec(memory_space=pltpu.VMEM)
    anywhere = pl.BlockSpec(memory_space=pl.ANY)
    args = [
        jnp.transpose(cell_index, (1, 0, 2)), jnp.transpose(fraction, (1, 0, 2)), charge,
        jnp.transpose(atom_count), influence, jnp.asarray(consts[0]), jnp.asarray(consts[1]),
    ]
    v = pltpu.VMEM
    scratch = [
        v((3, 2, ATOMS), jnp.int32), v((3, 2, ATOMS), F32), v((2, ATOMS), F32),
        v((1, 2), jnp.int32), v((32, 16, 256), F32), v((10, 256, 256), BF16), v((2, 256, 256), F32),
        v((2, 6, 6, ATOMS), F32), v((2, 40, ATOMS), F32), v((2, 24, ATOMS), F32),
        v((2, 25, ATOMS), F32), v((2, 256, ATOMS), BF16), v((2, 256, ATOMS), BF16),
        v((2, 40, ATOMS), F32), v((2, 24, ATOMS), F32), v((2, 256, ATOMS), BF16),
        v((2, 256, ATOMS), BF16), v((2, MESH_ROWS, CHUNK), BF16), v((2, MESH_ROWS, CHUNK), BF16),
        v((3, 2, ATOMS), jnp.int32), v((3, 2, ATOMS), F32), v((2, ATOMS), F32), v((2, ATOMS), F32),
        v((6, 6, ATOMS), F32), v((2, 40, ATOMS), F32), v((2, 8, ATOMS), F32),
        v((2, 256, ATOMS), BF16), v((2, 256, ATOMS), BF16),
        v((2, YH + CH, 256), F32), v((2, XH, 256), F32), v((2, MESH_ROWS, 256), F32),
        v((ROWS, 32, 256), F32), v((ROWS, 32, 256), F32), v((ROWS, 32, 256), F32),
        v((2, 256, 256), F32), v((2, 512, 512), BF16), v((2, 512, 512), BF16),
        v((2, 512, 512), BF16), v((256, 512), F32),
        v((2, DEVS, 8, 128), F32), v((2, DEVS, 8, 128), F32), v((2, DEVS, 8, 128), F32),
        v((2, DEVS, 8, 128), F32), v((2, 512, 256), F32),
        v((2, YH, 256), F32), v((2, 40, 256), F32),
        v((2, YH, 256), F32), v((2, XH, 256), F32), v((2, 40, 256), F32),
        v((2, 512, 768), BF16), v((2, HALO, 768), BF16), v((2, 3, ATOMS), F32),
        v((256, 256), F32), v((32, 256), F32),
        pltpu.SemaphoreType.DMA((34,)), pltpu.SemaphoreType.DMA((7,)), pltpu.SemaphoreType.REGULAR,
    ]
    out = pl.pallas_call(
        kernel,
        out_shape=pltpu.VMEM((3, 2, ATOMS), F32),
        in_specs=[anywhere] * 7,
        out_specs=vmem,
        scratch_shapes=scratch,
        compiler_params=pltpu.CompilerParams(
            collective_id=0, has_side_effects=True, vmem_limit_bytes=66_000_000
        ),
    )(*args)
    return jnp.transpose(out, (1, 0, 2))


def solution(mesh):
    placed = (
        P(None, None, ("row", "col")),
        P(None, None, ("row", "col")),
        P(None, ("row", "col")),
        P(None, ("row", "col")),
        P("row", "col", None),
    )
    return jax.shard_map(
        functools.partial(shards, tables()), mesh=mesh, in_specs=placed,
        out_specs=P(None, None, ("row", "col")), check_vma=False,
    )
```

```python
import functools

import jax
import jax.numpy as jnp
import numpy as np
from jax import lax
from jax.experimental import pallas as pl
from jax.experimental.pallas import tpu as pltpu
from jax.sharding import PartitionSpec as P

F32 = jnp.float32
BF16 = jnp.bfloat16
MESH = pl.DeviceIdType.MESH

K = 256
ROWS = 8
COLS = 16
DEVS = ROWS * COLS
ATOMS = 2048
CHUNK = 512
CHUNKS = ATOMS // CHUNK
GCHUNK = 256
GCHUNKS = ATOMS // GCHUNK

YH, XH, CH = 160, 80, 48
HALO = YH + XH + CH
MESH_ROWS = 592


def far_first():
    offsets = [d for d in np.ndindex(4, 4, 4, 2) if d != (0, 0, 0, 0)]
    offsets.sort(key=lambda d: (-sum(min(k, 4 - k) for k in d[:3]), d[3], d[0] + 2 * d[1] + 3 * d[2]))
    lanes = {}
    for d in offsets:
        lanes.setdefault(d[0] or 10 + d[1] if d[0] or d[1] else 20 + d[2], []).append(d)
    out = []
    while any(lanes.values()):
        out += [lane.pop(0) for lane in lanes.values() if lane]
    return out


OFFSETS = far_first()


def halves(x):
    top = x.astype(BF16)
    return top, (x - top.astype(F32)).astype(BF16)


def np_halves(x):
    x = np.asarray(x, np.float32)
    top = x.astype(jnp.bfloat16)
    return [top, (x - top.astype(np.float32)).astype(jnp.bfloat16)]


def tables():
    d = np.arange(DEVS)
    waves = 16 * (d % COLS) + 2 * (d // COLS) + (d % COLS >= COLS // 2)
    turn = 2.0 * np.pi / K
    angle = (waves[:, None] * np.arange(K)[None, :] % K) * turn
    sines = -np.sin(angle)
    sines[0] = 1.0 - 2.0 * (np.arange(K) % 2)
    out = np_halves(np.concatenate([np.cos(angle), sines]))
    spot = np.arange(256)
    rx, cc = 2 * (spot % 128 // 16) + spot // 128, spot % 16
    angle = ((rx[:, None] * rx[None, :] + cc[:, None] * cc[None, :]) % 16) * (16 * turn)
    out += np_halves(np.cos(angle)) + np_halves(np.sin(angle))
    xl, yl = spot // 16, spot % 16
    angle = ((xl[:, None] * xl[None, :] + yl[:, None] * yl[None, :]) % 16) * (16 * turn)
    out += np_halves(np.cos(angle)) + np_halves(np.sin(angle))
    angle = ((rx[:, None] * xl[None, :] + cc[:, None] * yl[None, :]) % K) * turn
    twiddles = np.stack([np.cos(angle), np.sin(angle)]).astype(np.float32)
    return np.stack(out), twiddles


def spline_values(f):
    nothing = jnp.zeros_like(f)
    levels = [f, 1.0 - f]
    slopes = levels
    for degree in range(3, 7):
        padded = levels + [nothing]
        following = []
        for o in range(degree):
            value = (f + float(o)) * padded[o]
            if o > 0:
                value = value + (float(degree - o) - f) * padded[o - 1]
            following.append(value * (1.0 / (degree - 1)))
        if degree == 6:
            slopes = [padded[0]] + [padded[o] - padded[o - 1] for o in range(1, 6)]
        levels = following
    return levels, slopes


def dot_nn(a, b):
    return lax.dot_general(a, b, (((1,), (0,)), ((), ())), preferred_element_type=F32)


def dot_nt(a, b):
    return lax.dot_general(a, b, (((1,), (1,)), ((), ())), preferred_element_type=F32)


def triple_nn(a, b):
    left = jnp.concatenate([a[0], a[1], a[0]], axis=1)
    return dot_nn(left, jnp.concatenate([b[0], b[0], b[1]], axis=0))


def three_nn(a, b):
    return dot_nn(a[0], b[0]) + dot_nn(a[1], b[0]) + dot_nn(a[0], b[1])


def tall_nn(a, b):
    n = a[0].shape[0] // 2
    return jnp.concatenate(
        [three_nn((a[0][q], a[1][q]), b) for q in (slice(0, n), slice(n, 2 * n))], axis=0
    )


def triple_nt(a, b):
    left = jnp.concatenate([a[0], a[1], a[0]], axis=1)
    return dot_nt(left, jnp.concatenate([b[0], b[0], b[1]], axis=1))


def dense(gap, rows):
    total = jnp.where(gap == 0, rows[0], 0.0)
    for j in range(1, 6):
        total = jnp.where(gap == j, rows[j], total)
    return total


def tiles_of(anchor, rows, size):
    gap = anchor - lax.broadcasted_iota(jnp.int32, (size, anchor.shape[1]), 0)
    return dense(gap & (size - 1), rows), gap >> (3 if size == 8 else 4)


def kernel(
    cell_hbm, frac_hbm, charge_hbm, count_hbm, infl_hbm, tab_hbm, twid_hbm,
    forces,
    cell, frac, charge, count, infl, tab, twid, w_scr, x_scr, y_scr, yq_scr, z_hi, z_lo, sx_scr, sy_scr, sz_hi, sz_lo,
    p_hi, p_lo, ncell, nfrac, qs, nq, nw_scr, nx_scr, nyq_scr, nz_hi, nz_lo, nacc, xr, mesh, gsend, grecv, glast, green, fb, gb, lb, escr,
    sbuf, rbuf, tbuf, qbuf, pot, ys, corner, yb, xb, cb, fint, fhal, part, swap, gone,
    sems, local, gate,
):
    row = lax.axis_index("row")
    col = lax.axis_index("col")
    me = row * COLS + col
    up_r, dn_r = lax.rem(row + 1, ROWS), lax.rem(row + ROWS - 1, ROWS)
    up_c, dn_c = lax.rem(col + 1, COLS), lax.rem(col + COLS - 1, COLS)
    core = lax.rem(col, 2)
    px = lax.rem(lax.div(col, 2), 2) * 2 + lax.rem(row, 2)
    py, pz = lax.div(col, 4), lax.div(row, 2)

    xs = [lax.rem(px + d, 4) for d in range(4)]
    x_row, x_col = [lax.rem(x, 2) for x in xs], [lax.div(x, 2) * 2 for x in xs]
    y_col = [lax.rem(py + d, 4) * 4 for d in range(4)]
    z_row = [lax.rem(pz + d, 4) * 2 for d in range(4)]
    cores = core, 1 - core

    def device(dx, dy, dz, dc):
        return z_row[dz] + x_row[dx], y_col[dy] + x_col[dx] + cores[dc]

    loads = [
        pltpu.make_async_copy(infl_hbm, infl, local.at[0]),
        pltpu.make_async_copy(tab_hbm, tab, local.at[1]),
        pltpu.make_async_copy(twid_hbm, twid, local.at[2]),
    ]
    inputs = [
        pltpu.make_async_copy(src, dst, local.at[3 + k])
        for k, (src, dst) in enumerate((
            (cell_hbm, cell), (frac_hbm, frac), (charge_hbm, charge), (count_hbm, count)
        ))
    ]
    for copy in inputs + loads:
        copy.start()

    barrier = pltpu.get_barrier_semaphore()

    def greet_column(k, carry):
        to = row, lax.rem(col + k, COLS)
        pl.semaphore_signal(barrier, inc=1, device_id=to, device_id_type=MESH)
        return carry

    def greet_row(k, carry):
        to = lax.rem(row + k, ROWS), col
        pl.semaphore_signal(barrier, inc=1, device_id=to, device_id_type=MESH)
        return carry

    def vouch(k, carry):
        to = lax.rem(row + k, ROWS), col
        pl.semaphore_signal(gate, inc=1, device_id=to, device_id_type=MESH)
        return carry

    lax.fori_loop(1, ROWS, greet_row, 0)
    lax.fori_loop(1, COLS, greet_column, 0)

    def remote(src, dst, send, recv, to):
        return pltpu.make_async_remote_copy(
            src_ref=src, dst_ref=dst, send_sem=sems.at[send], recv_sem=sems.at[recv],
            device_id=to, device_id_type=MESH,
        )

    for copy in inputs:
        copy.wait()
    slot = lax.broadcasted_iota(jnp.int32, (1, ATOMS), 1)
    values, slopes = spline_values(jnp.concatenate([frac[0], frac[1], frac[2]], axis=0))
    for j in range(6):
        w_scr[0, j] = values[j]
        w_scr[1, j] = slopes[j]
    for s in range(2):
        masked = jnp.where(slot < count[0:1, s : s + 1], charge[s : s + 1], 0.0)
        yq_scr[s, 24:25] = masked
        qs[s : s + 1] = masked

    loads[0].wait()
    for odd in range(2):

        @pl.when(lax.div(col, COLS // 2) == odd)
        def _():
            for k in range(ROWS):
                gsend[k] = infl[:, 2 * k + odd, :]

    pl.semaphore_wait(barrier, ROWS + COLS - 2)
    lax.fori_loop(1, ROWS, vouch, 0)
    atoms = [
        remote(src, dst, 2 + 2 * k, 3 + 2 * k, (row, dn_c))
        for k, (src, dst) in enumerate(((cell, ncell), (frac, nfrac), (qs, nq)))
    ]
    for copy in atoms:
        copy.start()

    def send_green(k, carry):
        there = lax.rem(row + k, ROWS)
        remote(gsend.at[there], grecv.at[row], 0, 1, (there, col)).start()
        return carry

    lax.fori_loop(1, ROWS, send_green, 0)
    grecv[row] = gsend[row]

    def spans(i):
        s = lax.div(i, CHUNKS)
        return s, pl.ds(pl.multiple_of(lax.rem(i, CHUNKS) * CHUNK, CHUNK), CHUNK)

    def pick(kind):
        return lambda s, dim, lanes: [
            w_scr[kind, j, 2 * dim + s : 2 * dim + s + 1, lanes] for j in range(6)
        ]

    def dense_x(anchor, rows, xo, s, lanes):
        value, tile = tiles_of(anchor, rows, 8)
        for b, at in ((0, 0), (1, 8), (2, 16), (3, 24), (-1, 32)):
            xo[s, at : at + 8, lanes] = jnp.where(tile == b, value, 0.0)

    def dense_z(anchor, rows, hi_ref, lo_ref, s, lanes):
        value, tile = tiles_of(anchor, rows, 16)
        top, rest = halves(value)
        tile = (tile & 15).astype(F32).astype(BF16)
        none = jnp.zeros_like(top)
        for b in range(16):
            here = tile == jnp.asarray(float(b), BF16)
            hi_ref[s, 16 * b : 16 * b + 16, lanes] = jnp.where(here, top, none)
            lo_ref[s, 16 * b : 16 * b + 16, lanes] = jnp.where(here, rest, none)

    def dense_all(i, s, kind, xo, yo, hi_ref, lo_ref):
        rows_of = pick(kind)
        for k in range(CHUNK // 128):
            lanes = pl.ds(pl.multiple_of(i * CHUNK + 128 * k, 128), 128)
            dense_x(cell[0, s : s + 1, lanes] - row * 32, rows_of(s, 0, lanes), xo, s, lanes)
            anchor = cell[1, s : s + 1, lanes] - col * 16
            value, tile = tiles_of(anchor, rows_of(s, 1, lanes), 8)
            for b, at in ((0, 0), (1, 8), (-1, 16)):
                y = jnp.where(tile == b, value, 0.0)
                yo[s, at : at + 8, lanes] = y
                if kind == 0:
                    yq_scr[s, at : at + 8, lanes] = y * yq_scr[s, 24:25, lanes]
            dense_z(cell[2, s : s + 1, lanes], rows_of(s, 2, lanes), hi_ref, lo_ref, s, lanes)

    def build_next(s):
        def body(i, carry):
            for k in range(CHUNK // 128):
                lanes = pl.ds(pl.multiple_of(i * CHUNK + 128 * k, 128), 128)
                rows_of = [
                    [nw_scr[j, 2 * d + s : 2 * d + s + 1, lanes] for j in range(6)]
                    for d in range(3)
                ]
                dense_x(ncell[0, s : s + 1, lanes] - row * 32, rows_of[0], nx_scr, s, lanes)
                anchor = ncell[1, s : s + 1, lanes] - up_c * 16
                value, tile = tiles_of(anchor, rows_of[1], 8)
                value = jnp.where(tile == -1, value, 0.0) * nq[s : s + 1, lanes]
                nyq_scr[s, :, lanes] = value
                dense_z(ncell[2, s : s + 1, lanes], rows_of[2], nz_hi, nz_lo, s, lanes)
            return carry

        lax.fori_loop(0, CHUNKS, body, 0)

    def build(s):
        def body(i, carry):
            dense_all(i, s, 0, x_scr, y_scr, z_hi, z_lo)
            return carry

        lax.fori_loop(0, CHUNKS, body, 0)

    def build_slopes(i, carry):
        for s in range(2):
            dense_all(i, s, 1, sx_scr, sy_scr, sz_hi, sz_lo)
        return carry

    build(0)

    def put(slot, at, value):
        top, rest = halves(value)
        p_hi[slot, at : at + value.shape[0], :] = top
        p_lo[slot, at : at + value.shape[0], :] = rest

    def pairs(fill, ref, zs, low, high):
        def body(i, carry):
            for slot in range(2):
                fill(slot, *spans(2 * i + slot))
            for slot in range(2):
                s, lanes = spans(2 * i + slot)
                a = p_hi[slot, low:high, :], p_lo[slot, low:high, :]
                b = zs[0][s, :, lanes], zs[1][s, :, lanes]
                ref[s, low:high, :] += triple_nt(a, b)
            return carry

        return body

    def fill_next(slot, s, lanes):
        for k in range(5):
            put(slot, 32 * k, nx_scr[s, 0:32, lanes] * nyq_scr[s, 3 + k : 4 + k, lanes])
        edge = nyq_scr[s, :, lanes]
        for k in range(3):
            first = edge * nx_scr[s, 35 + 2 * k : 36 + 2 * k, lanes]
            if k < 2:
                second = edge * nx_scr[s, 36 + 2 * k : 37 + 2 * k, lanes]
            else:
                second = jnp.zeros_like(first)
            put(slot, YH + 16 * k, jnp.concatenate([first, second], axis=0))

    def fill_inner(slot, s, lanes):
        for x in range(32):
            put(slot, 16 * x, yq_scr[s, 0:16, lanes] * x_scr[s, x : x + 1, lanes])

    def fill_edge(slot, s, lanes):
        for k in range(5):
            put(slot, 512 + 16 * k, yq_scr[s, 0:16, lanes] * x_scr[s, 35 + k : 36 + k, lanes])

    def fill_both(slot, s, lanes):
        fill_inner(slot, s, lanes)
        fill_edge(slot, s, lanes)

    nacc[...] = jnp.zeros_like(nacc)
    mesh[...] = jnp.zeros_like(mesh)
    edges = []

    def half(s):
        return s * CHUNKS // 2, (s + 1) * CHUNKS // 2

    def spread_own(s, fill, low, high):
        lax.fori_loop(*half(s), pairs(fill, mesh, (z_hi, z_lo), low, high), 0)

    def spread_next(s):
        lax.fori_loop(*half(s), pairs(fill_next, nacc, (nz_hi, nz_lo), 0, YH + CH), 0)

    def send_edge(s):
        view = mesh.at[s].reshape(MESH_ROWS // 16, 16, 256)
        for k in range(5):
            view[32 + k, 8:16] += nacc[s, YH + 8 * k : YH + 8 * k + 8]
        edges.append(remote(mesh.at[s, 512:MESH_ROWS], xr.at[s], 8 + 2 * s, 9 + 2 * s, (dn_r, col)))
        edges[s].start()

    spread_own(0, fill_both, 0, MESH_ROWS)
    for copy in atoms:
        copy.wait()
    values, _ = spline_values(jnp.concatenate([nfrac[0], nfrac[1], nfrac[2]], axis=0))
    for j in range(6):
        nw_scr[j] = values[j]
    build_next(0)
    spread_next(0)
    send_edge(0)

    pl.semaphore_wait(gate, ROWS - 1)
    first = me == 0

    @pl.when(col == COLS // 2)
    def _():
        gone[...] = infl[:, 0, :]
        remote(gone, glast.at[row], 12, 13, (0, 0)).start()

    build(1)
    build_next(1)
    spread_own(1, fill_edge, 512, MESH_ROWS)
    spread_next(1)
    send_edge(1)

    class Exchange:
        def __init__(self, src, dst, par, first):
            self.src, self.dst, self.first = src.at[par], dst.at[par], first

        def start(self):
            for offset in OFFSETS:
                to = device(*offset)
                src = self.src.at[to[0] * COLS + to[1]]
                remote(src, self.dst.at[me], self.first, self.first + 1, to).start()
            self.dst[me] = self.src[me]

        def wait(self):
            every = slice(0, DEVS - 1)
            remote(
                self.src.at[every], self.dst.at[every], self.first, self.first + 1, (up_r, col)
            ).wait()

    forward = [Exchange(sbuf, rbuf, s, 14 + 2 * s) for s in range(2)]
    backward = [Exchange(tbuf, qbuf, s, 18 + 2 * s) for s in range(2)]

    def send_forward(s):
        edges[s].wait()
        view = mesh.at[s].reshape(MESH_ROWS // 16, 16, 256)
        for k in range(5):
            view[0:32, 11 + k, :] += nacc[s, 32 * k : 32 * k + 32]
        for k in range(5):
            view[27 + k] += xr[s, 16 * k : 16 * k + 16]
        a = triple_nt((tab[0], tab[1]), halves(mesh[s, 0:512]))
        for reim in range(2):
            for q in range(4):
                sbuf[s, :, 4 * reim + q, :] = a[
                    128 * reim : 128 * reim + 128, 128 * q : 128 * q + 128
                ]
        forward[s].start()

    for copy in loads[1:]:
        copy.wait()

    send_forward(0)
    spread_own(1, fill_inner, 0, 512)

    for h in range(2):
        fc, fs, lc, ls = [tab[2 + 2 * k + h] for k in range(4)]
        for ref, c, q in ((fb, fc, fs), (gb, fc, -fs), (lb, lc, -ls)):
            ref[h, 0:256, 0:256] = c
            ref[h, 0:256, 256:512] = q
            ref[h, 256:512, 0:256] = -q
            ref[h, 256:512, 256:512] = c
    some = slice(0, ROWS - 1)
    remote(gsend.at[some], grecv.at[some], 0, 1, (up_r, col)).wait()
    lane = lax.broadcasted_iota(jnp.int32, (16, 256), 1)

    def trade(bits, load, store):
        for rest in range(4):
            base = [(a << bits[0]) + (b << bits[1]) + (rest << (2 if bits[0] == 0 else 0))
                    for b in range(2) for a in range(2)]
            blocks = [load(k) for k in base]
            for i, bit in enumerate(bits):
                step = 1 << bit
                low = (lane & step) == 0
                for k in range(4):
                    if k & (1 << i):
                        continue
                    a, b = blocks[k], blocks[k | (1 << i)]
                    blocks[k] = jnp.where(low, a, pltpu.roll(b, step, 1))
                    blocks[k | (1 << i)] = jnp.where(low, pltpu.roll(a, 256 - step, 1), b)
            for k, block in zip(base, blocks):
                store(k, block)

    def in_mode_order(ref, plane, scale):
        def load(k):
            return ref[k // 2, 16 * (k % 2) : 16 * (k % 2) + 16, :] * scale

        def keep(k, block):
            swap[16 * k : 16 * k + 16, :] = block

        def put_in_place(k, block):
            at = 128 * (k % 2) + 16 * (k // 2)
            green[plane, at : at + 16, :] = block

        trade((0, 1), load, keep)
        trade((2, 3), lambda k: swap[16 * k : 16 * k + 16, :], put_in_place)

    unit = 1.0 / float(K) ** 3
    lax.fori_loop(0, CHUNKS, build_slopes, 0)
    in_mode_order(grecv, 0, jnp.where(first, unit, 2.0 * unit))

    @pl.when(first)
    def _():
        remote(glast, glast, 12, 13, (1, 0)).wait_recv()
        in_mode_order(glast, 1, unit)

    @pl.when(col == COLS // 2)
    def _():
        remote(gone, glast.at[0], 12, 13, (0, 0)).wait_send()

    send_forward(1)

    tc, ts = twid[0], twid[1]

    def stacked(buf, par):
        parts = [
            jnp.concatenate([buf[par, :, 2 * j, :], buf[par, :, 2 * j + 1, :]], axis=1)
            for j in range(4)
        ]
        return jnp.concatenate(parts, axis=0)

    def modes(u):
        ur, ui = u[0:256], u[256:512]
        v = jnp.concatenate([ur * tc + ui * ts, ui * tc - ur * ts], axis=1)
        return three_nn(halves(v), (lb[0], lb[1]))

    def turn(s, carry):
        Exchange(sbuf, rbuf, s, 14 + 2 * s).wait()

        @pl.when(me != 0)
        def _():
            u = tall_nn((fb[0], fb[1]), halves(stacked(rbuf, s)))
            escr[...] = jnp.concatenate([green[0], green[0]], axis=1) * modes(u)

        @pl.when(me == 0)
        def _():
            x = halves(stacked(rbuf, s))
            left = fb[0, :, 0:256], fb[1, :, 0:256]
            a = modes(tall_nn(left, (x[0][0:256], x[1][0:256])))
            b = modes(tall_nn(left, (x[0][256:512], x[1][256:512])))
            escr[:, 0:256] = green[0] * a[:, 0:256] - green[1] * b[:, 256:512]
            escr[:, 256:512] = green[0] * a[:, 256:512] + green[1] * b[:, 0:256]

        b = triple_nt(halves(escr[...]), (lb[0], lb[1]))
        br, bi = b[:, 0:256], b[:, 256:512]
        h = jnp.concatenate([br * tc - bi * ts, bi * tc + br * ts], axis=0)
        t = tall_nn((gb[0], gb[1]), halves(h))
        for j in range(4):
            for lh in range(2):
                tbuf[s, :, 2 * j + lh, :] = t[
                    128 * j : 128 * j + 128, 128 * lh : 128 * lh + 128
                ]
        Exchange(tbuf, qbuf, s, 18 + 2 * s).start()
        return carry

    lax.fori_loop(0, 2, turn, 0)

    back = []

    def take_back(s):
        backward[s].wait()
        q = stacked(qbuf, s)
        for xh in range(2):
            picked = jnp.concatenate(
                [q[128 * xh : 128 * xh + 128], q[256 + 128 * xh : 384 + 128 * xh]], axis=0
            )
            pot[s, 256 * xh : 256 * xh + 256, :] = triple_nn(halves(picked.T), (tab[0], tab[1]))
        view = pot.at[s].reshape(32, 16, 256)
        for k in range(5):
            ys[s, 32 * k : 32 * k + 32] = view[:, 11 + k, :]
        for k in range(5):
            corner[s, 8 * k : 8 * k + 8] = view[27 + k, 8:16]
        at = 22 + 6 * s
        back.append([
            remote(ys.at[s], yb.at[s], at, at + 1, (row, up_c)),
            remote(pot.at[s, 432:512], xb.at[s], at + 2, at + 3, (up_r, col)),
            remote(corner.at[s], cb.at[s], at + 4, at + 5, (up_r, up_c)),
        ])
        for copy in back[s]:
            copy.start()
        spread_out(fint, s, 0, pot[s])

    def take_halo(s):
        for copy in back[s]:
            copy.wait()
        for at, ref in ((0, yb), (YH, xb), (YH + XH, cb)):
            spread_out(fhal, s, at, ref[s])

    def spread_out(ref, s, at, value):
        top, rest = halves(value)
        n = value.shape[0]
        ref[s, at : at + n, 0:256] = top
        ref[s, at : at + n, 256:512] = rest
        ref[s, at : at + n, 512:768] = top

    def sample(ref, s, lanes):
        top = jnp.concatenate([z_hi[s, :, lanes], sz_hi[s, :, lanes]], axis=1)
        rest = jnp.concatenate([z_lo[s, :, lanes], sz_lo[s, :, lanes]], axis=1)
        both = dot_nn(ref[s], jnp.concatenate([top, top, rest], axis=0))
        return both[:, 0:GCHUNK], both[:, GCHUNK : 2 * GCHUNK]

    def window(i):
        s = lax.div(i, GCHUNKS)
        return s, pl.ds(pl.multiple_of(lax.rem(i, GCHUNKS) * GCHUNK, GCHUNK), GCHUNK)

    def down(value):
        return jnp.sum(value, axis=0, keepdims=True)

    def four(body):
        def several(i, carry):
            for k in range(4):
                carry = body(4 * i + k, carry)
            return carry

        return several

    def gather_inner(i, carry):
        s, lanes = window(i)
        plain, slope = sample(fint, s, lanes)
        a1 = a2 = a3 = jnp.zeros((16, GCHUNK), F32)
        for x in range(32):
            wx, sx = x_scr[s, x : x + 1, lanes], sx_scr[s, x : x + 1, lanes]
            piece = plain[16 * x : 16 * x + 16]
            a1 = a1 + piece * sx
            a2 = a2 + piece * wx
            a3 = a3 + slope[16 * x : 16 * x + 16] * wx
        wy, sy = y_scr[s, 0:16, lanes], sy_scr[s, 0:16, lanes]
        part[s, 0:1, lanes] = down(a1 * wy)
        part[s, 1:2, lanes] = down(a2 * sy)
        part[s, 2:3, lanes] = down(a3 * wy)
        return carry

    def gather_halo(i, carry):
        s, lanes = window(i)
        plain, slope = sample(fhal, s, lanes)
        a1 = a2 = a3 = jnp.zeros((16, GCHUNK), F32)
        b1 = b2 = b3 = jnp.zeros((32, GCHUNK), F32)
        e1 = e2 = e3 = jnp.zeros((8, GCHUNK), F32)
        for k in range(5):
            wy, sy = y_scr[s, 19 + k : 20 + k, lanes], sy_scr[s, 19 + k : 20 + k, lanes]
            wx, sx = x_scr[s, 35 + k : 36 + k, lanes], sx_scr[s, 35 + k : 36 + k, lanes]
            piece = plain[32 * k : 32 * k + 32]
            b1 = b1 + piece * wy
            b2 = b2 + piece * sy
            b3 = b3 + slope[32 * k : 32 * k + 32] * wy
            at = YH + 16 * k
            piece = plain[at : at + 16]
            a1 = a1 + piece * sx
            a2 = a2 + piece * wx
            a3 = a3 + slope[at : at + 16] * wx
            at = YH + XH + 8 * k
            piece = plain[at : at + 8]
            e1 = e1 + piece * sx
            e2 = e2 + piece * wx
            e3 = e3 + slope[at : at + 8] * wx
        wy, sy = y_scr[s, 0:16, lanes], sy_scr[s, 0:16, lanes]
        vy, ty = y_scr[s, 16:24, lanes], sy_scr[s, 16:24, lanes]
        wx, sx = x_scr[s, 0:32, lanes], sx_scr[s, 0:32, lanes]

        def finish(d, a, m, e, n, b, q):
            total = part[s, d : d + 1, lanes] + down(a * m) + down(e * n) + down(b * q)
            forces[d, pl.ds(s, 1), lanes] = -yq_scr[s, 24:25, lanes] * total

        finish(0, a1, wy, e1, vy, b1, sx)
        finish(1, a2, sy, e2, ty, b2, wx)
        finish(2, a3, wy, e3, vy, b3, wx)
        return carry

    def gather(body, s):
        lax.fori_loop(s * GCHUNKS // 4, (s + 1) * GCHUNKS // 4, four(body), 0)

    take_back(0)
    gather(gather_inner, 0)
    take_back(1)
    gather(gather_inner, 1)
    take_halo(0)
    gather(gather_halo, 0)
    take_halo(1)
    gather(gather_halo, 1)


def shards(consts, cell_index, fraction, charge, atom_count, influence):
    vmem = pl.BlockSpec(memory_space=pltpu.VMEM)
    anywhere = pl.BlockSpec(memory_space=pl.ANY)
    args = [
        jnp.transpose(cell_index, (1, 0, 2)), jnp.transpose(fraction, (1, 0, 2)), charge,
        jnp.transpose(atom_count), influence, jnp.asarray(consts[0]), jnp.asarray(consts[1]),
    ]
    v = pltpu.VMEM
    scratch = [
        v((3, 2, ATOMS), jnp.int32), v((3, 2, ATOMS), F32), v((2, ATOMS), F32),
        v((1, 2), jnp.int32), v((32, 16, 256), F32), v((10, 256, 256), BF16), v((2, 256, 256), F32),
        v((2, 6, 6, ATOMS), F32), v((2, 40, ATOMS), F32), v((2, 24, ATOMS), F32),
        v((2, 25, ATOMS), F32), v((2, 256, ATOMS), BF16), v((2, 256, ATOMS), BF16),
        v((2, 40, ATOMS), F32), v((2, 24, ATOMS), F32), v((2, 256, ATOMS), BF16),
        v((2, 256, ATOMS), BF16), v((2, MESH_ROWS, CHUNK), BF16), v((2, MESH_ROWS, CHUNK), BF16),
        v((3, 2, ATOMS), jnp.int32), v((3, 2, ATOMS), F32), v((2, ATOMS), F32), v((2, ATOMS), F32),
        v((6, 6, ATOMS), F32), v((2, 40, ATOMS), F32), v((2, 8, ATOMS), F32),
        v((2, 256, ATOMS), BF16), v((2, 256, ATOMS), BF16),
        v((2, YH + CH, 256), F32), v((2, XH, 256), F32), v((2, MESH_ROWS, 256), F32),
        v((ROWS, 32, 256), F32), v((ROWS, 32, 256), F32), v((ROWS, 32, 256), F32),
        v((2, 256, 256), F32), v((2, 512, 512), BF16), v((2, 512, 512), BF16),
        v((2, 512, 512), BF16), v((256, 512), F32),
        v((2, DEVS, 8, 128), F32), v((2, DEVS, 8, 128), F32), v((2, DEVS, 8, 128), F32),
        v((2, DEVS, 8, 128), F32), v((2, 512, 256), F32),
        v((2, YH, 256), F32), v((2, 40, 256), F32),
        v((2, YH, 256), F32), v((2, XH, 256), F32), v((2, 40, 256), F32),
        v((2, 512, 768), BF16), v((2, HALO, 768), BF16), v((2, 3, ATOMS), F32),
        v((256, 256), F32), v((32, 256), F32),
        pltpu.SemaphoreType.DMA((34,)), pltpu.SemaphoreType.DMA((7,)), pltpu.SemaphoreType.REGULAR,
    ]
    out = pl.pallas_call(
        kernel,
        out_shape=pltpu.VMEM((3, 2, ATOMS), F32),
        in_specs=[anywhere] * 7,
        out_specs=vmem,
        scratch_shapes=scratch,
        compiler_params=pltpu.CompilerParams(
            collective_id=0, has_side_effects=True, vmem_limit_bytes=66_000_000
        ),
    )(*args)
    return jnp.transpose(out, (1, 0, 2))


def solution(mesh):
    placed = (
        P(None, None, ("row", "col")),
        P(None, None, ("row", "col")),
        P(None, ("row", "col")),
        P(None, ("row", "col")),
        P("row", "col", None),
    )
    return jax.shard_map(
        functools.partial(shards, tables()), mesh=mesh, in_specs=placed,
        out_specs=P(None, None, ("row", "col")), check_vma=False,
    )
```

```python
import functools

import jax
import jax.numpy as jnp
import numpy as np
from jax import lax
from jax.experimental import pallas as pl
from jax.experimental.pallas import tpu as pltpu
from jax.sharding import PartitionSpec as P

F32 = jnp.float32
BF16 = jnp.bfloat16
MESH = pl.DeviceIdType.MESH

K = 256
ROWS = 8
COLS = 16
DEVS = ROWS * COLS
ATOMS = 2048
CHUNK = 512
CHUNKS = ATOMS // CHUNK
GCHUNK = 256
GCHUNKS = ATOMS // GCHUNK

YH, XH, CH = 160, 80, 48
HALO = YH + XH + CH
MESH_ROWS = 592


def far_first():
    offsets = [d for d in np.ndindex(4, 4, 4, 2) if d != (0, 0, 0, 0)]
    offsets.sort(key=lambda d: (-sum(min(k, 4 - k) for k in d[:3]), d[3], d[0] + 2 * d[1] + 3 * d[2]))
    lanes = {}
    for d in offsets:
        lanes.setdefault(d[0] or 10 + d[1] if d[0] or d[1] else 20 + d[2], []).append(d)
    out = []
    while any(lanes.values()):
        out += [lane.pop(0) for lane in lanes.values() if lane]
    return out


OFFSETS = far_first()


def halves(x):
    top = x.astype(BF16)
    return top, (x - top.astype(F32)).astype(BF16)


def np_halves(x):
    x = np.asarray(x, np.float32)
    top = x.astype(jnp.bfloat16)
    return [top, (x - top.astype(np.float32)).astype(jnp.bfloat16)]


def tables():
    d = np.arange(DEVS)
    waves = 16 * (d % COLS) + 2 * (d // COLS) + (d % COLS >= COLS // 2)
    turn = 2.0 * np.pi / K
    angle = (waves[:, None] * np.arange(K)[None, :] % K) * turn
    sines = -np.sin(angle)
    sines[0] = 1.0 - 2.0 * (np.arange(K) % 2)
    out = np_halves(np.concatenate([np.cos(angle), sines]))
    spot = np.arange(256)
    rx, cc = 2 * (spot % 128 // 16) + spot // 128, spot % 16
    angle = ((rx[:, None] * rx[None, :] + cc[:, None] * cc[None, :]) % 16) * (16 * turn)
    out += np_halves(np.cos(angle)) + np_halves(np.sin(angle))
    xl, yl = spot // 16, spot % 16
    angle = ((xl[:, None] * xl[None, :] + yl[:, None] * yl[None, :]) % 16) * (16 * turn)
    out += np_halves(np.cos(angle)) + np_halves(np.sin(angle))
    angle = ((rx[:, None] * xl[None, :] + cc[:, None] * yl[None, :]) % K) * turn
    twiddles = np.stack([np.cos(angle), np.sin(angle)]).astype(np.float32)
    return np.stack(out), twiddles


def spline_values(f):
    nothing = jnp.zeros_like(f)
    levels = [f, 1.0 - f]
    slopes = levels
    for degree in range(3, 7):
        padded = levels + [nothing]
        following = []
        for o in range(degree):
            value = (f + float(o)) * padded[o]
            if o > 0:
                value = value + (float(degree - o) - f) * padded[o - 1]
            following.append(value * (1.0 / (degree - 1)))
        if degree == 6:
            slopes = [padded[0]] + [padded[o] - padded[o - 1] for o in range(1, 6)]
        levels = following
    return levels, slopes


def dot_nn(a, b):
    return lax.dot_general(a, b, (((1,), (0,)), ((), ())), preferred_element_type=F32)


def dot_nt(a, b):
    return lax.dot_general(a, b, (((1,), (1,)), ((), ())), preferred_element_type=F32)


def triple_nn(a, b):
    left = jnp.concatenate([a[0], a[1], a[0]], axis=1)
    return dot_nn(left, jnp.concatenate([b[0], b[0], b[1]], axis=0))


def three_nn(a, b):
    return dot_nn(a[0], b[0]) + dot_nn(a[1], b[0]) + dot_nn(a[0], b[1])


def tall_nn(a, b):
    n = a[0].shape[0] // 2
    return jnp.concatenate(
        [three_nn((a[0][q], a[1][q]), b) for q in (slice(0, n), slice(n, 2 * n))], axis=0
    )


def triple_nt(a, b):
    left = jnp.concatenate([a[0], a[1], a[0]], axis=1)
    return dot_nt(left, jnp.concatenate([b[0], b[0], b[1]], axis=1))


def dense(gap, rows):
    total = jnp.where(gap == 0, rows[0], 0.0)
    for j in range(1, 6):
        total = jnp.where(gap == j, rows[j], total)
    return total


def tiles_of(anchor, rows, size):
    gap = anchor - lax.broadcasted_iota(jnp.int32, (size, anchor.shape[1]), 0)
    return dense(gap & (size - 1), rows), gap >> (3 if size == 8 else 4)


def kernel(
    cell_hbm, frac_hbm, charge_hbm, count_hbm, infl_hbm, tab_hbm, twid_hbm,
    forces,
    cell, frac, charge, count, infl, tab, twid, w_scr, x_scr, y_scr, yq_scr, z_hi, z_lo, sx_scr, sy_scr, sz_hi, sz_lo,
    p_hi, p_lo, ncell, nfrac, qs, nq, nw_scr, nx_scr, nyq_scr, nz_hi, nz_lo, nacc, xr, mesh, gsend, grecv, glast, green, fb, gb, lb, escr,
    sbuf, rbuf, tbuf, qbuf, pot, ys, corner, yb, xb, cb, fint, fhal, part, swap, gone,
    sems, local, gate,
):
    row = lax.axis_index("row")
    col = lax.axis_index("col")
    me = row * COLS + col
    up_r, dn_r = lax.rem(row + 1, ROWS), lax.rem(row + ROWS - 1, ROWS)
    up_c, dn_c = lax.rem(col + 1, COLS), lax.rem(col + COLS - 1, COLS)
    core = lax.rem(col, 2)
    px = lax.rem(lax.div(col, 2), 2) * 2 + lax.rem(row, 2)
    py, pz = lax.div(col, 4), lax.div(row, 2)

    xs = [lax.rem(px + d, 4) for d in range(4)]
    x_row, x_col = [lax.rem(x, 2) for x in xs], [lax.div(x, 2) * 2 for x in xs]
    y_col = [lax.rem(py + d, 4) * 4 for d in range(4)]
    z_row = [lax.rem(pz + d, 4) * 2 for d in range(4)]
    cores = core, 1 - core

    def device(dx, dy, dz, dc):
        return z_row[dz] + x_row[dx], y_col[dy] + x_col[dx] + cores[dc]

    loads = [
        pltpu.make_async_copy(infl_hbm, infl, local.at[0]),
        pltpu.make_async_copy(tab_hbm, tab, local.at[1]),
        pltpu.make_async_copy(twid_hbm, twid, local.at[2]),
    ]
    inputs = [
        pltpu.make_async_copy(src, dst, local.at[3 + k])
        for k, (src, dst) in enumerate((
            (cell_hbm, cell), (frac_hbm, frac), (charge_hbm, charge), (count_hbm, count)
        ))
    ]
    for copy in inputs + loads:
        copy.start()

    barrier = pltpu.get_barrier_semaphore()

    def greet_column(k, carry):
        to = row, lax.rem(col + k, COLS)
        pl.semaphore_signal(barrier, inc=1, device_id=to, device_id_type=MESH)
        return carry

    def greet_row(k, carry):
        to = lax.rem(row + k, ROWS), col
        pl.semaphore_signal(barrier, inc=1, device_id=to, device_id_type=MESH)
        return carry

    def vouch(k, carry):
        to = lax.rem(row + k, ROWS), col
        pl.semaphore_signal(gate, inc=1, device_id=to, device_id_type=MESH)
        return carry

    lax.fori_loop(1, ROWS, greet_row, 0)
    lax.fori_loop(1, COLS, greet_column, 0)

    def remote(src, dst, send, recv, to):
        return pltpu.make_async_remote_copy(
            src_ref=src, dst_ref=dst, send_sem=sems.at[send], recv_sem=sems.at[recv],
            device_id=to, device_id_type=MESH,
        )

    for copy in inputs:
        copy.wait()
    slot = lax.broadcasted_iota(jnp.int32, (1, ATOMS), 1)
    values, slopes = spline_values(jnp.concatenate([frac[0], frac[1], frac[2]], axis=0))
    for j in range(6):
        w_scr[0, j] = values[j]
        w_scr[1, j] = slopes[j]
    for s in range(2):
        masked = jnp.where(slot < count[0:1, s : s + 1], charge[s : s + 1], 0.0)
        yq_scr[s, 24:25] = masked
        qs[s : s + 1] = masked

    loads[0].wait()
    for odd in range(2):

        @pl.when(lax.div(col, COLS // 2) == odd)
        def _():
            for k in range(ROWS):
                gsend[k] = infl[:, 2 * k + odd, :]

    pl.semaphore_wait(barrier, ROWS + COLS - 2)
    lax.fori_loop(1, ROWS, vouch, 0)
    atoms = [
        remote(src, dst, 2 + 2 * k, 3 + 2 * k, (row, dn_c))
        for k, (src, dst) in enumerate(((cell, ncell), (frac, nfrac), (qs, nq)))
    ]
    for copy in atoms:
        copy.start()

    def send_green(k, carry):
        there = lax.rem(row + k, ROWS)
        remote(gsend.at[there], grecv.at[row], 0, 1, (there, col)).start()
        return carry

    lax.fori_loop(1, ROWS, send_green, 0)
    grecv[row] = gsend[row]

    def spans(i):
        s = lax.div(i, CHUNKS)
        return s, pl.ds(pl.multiple_of(lax.rem(i, CHUNKS) * CHUNK, CHUNK), CHUNK)

    def pick(kind):
        return lambda s, dim, lanes: [
            w_scr[kind, j, 2 * dim + s : 2 * dim + s + 1, lanes] for j in range(6)
        ]

    def dense_x(anchor, rows, xo, s, lanes):
        value, tile = tiles_of(anchor, rows, 8)
        for b, at in ((0, 0), (1, 8), (2, 16), (3, 24), (-1, 32)):
            xo[s, at : at + 8, lanes] = jnp.where(tile == b, value, 0.0)

    def dense_z(anchor, rows, hi_ref, lo_ref, s, lanes):
        value, tile = tiles_of(anchor, rows, 16)
        top, rest = halves(value)
        tile = (tile & 15).astype(F32).astype(BF16)
        none = jnp.zeros_like(top)
        for b in range(16):
            here = tile == jnp.asarray(float(b), BF16)
            hi_ref[s, 16 * b : 16 * b + 16, lanes] = jnp.where(here, top, none)
            lo_ref[s, 16 * b : 16 * b + 16, lanes] = jnp.where(here, rest, none)

    def dense_all(i, s, kind, xo, yo, hi_ref, lo_ref):
        rows_of = pick(kind)
        for k in range(CHUNK // 128):
            lanes = pl.ds(pl.multiple_of(i * CHUNK + 128 * k, 128), 128)
            dense_x(cell[0, s : s + 1, lanes] - row * 32, rows_of(s, 0, lanes), xo, s, lanes)
            anchor = cell[1, s : s + 1, lanes] - col * 16
            value, tile = tiles_of(anchor, rows_of(s, 1, lanes), 8)
            for b, at in ((0, 0), (1, 8), (-1, 16)):
                y = jnp.where(tile == b, value, 0.0)
                yo[s, at : at + 8, lanes] = y
                if kind == 0:
                    yq_scr[s, at : at + 8, lanes] = y * yq_scr[s, 24:25, lanes]
            dense_z(cell[2, s : s + 1, lanes], rows_of(s, 2, lanes), hi_ref, lo_ref, s, lanes)

    def build_next(s):
        def body(i, carry):
            for k in range(CHUNK // 128):
                lanes = pl.ds(pl.multiple_of(i * CHUNK + 128 * k, 128), 128)
                rows_of = [
                    [nw_scr[j, 2 * d + s : 2 * d + s + 1, lanes] for j in range(6)]
                    for d in range(3)
                ]
                dense_x(ncell[0, s : s + 1, lanes] - row * 32, rows_of[0], nx_scr, s, lanes)
                anchor = ncell[1, s : s + 1, lanes] - up_c * 16
                value, tile = tiles_of(anchor, rows_of[1], 8)
                value = jnp.where(tile == -1, value, 0.0) * nq[s : s + 1, lanes]
                nyq_scr[s, :, lanes] = value
                dense_z(ncell[2, s : s + 1, lanes], rows_of[2], nz_hi, nz_lo, s, lanes)
            return carry

        lax.fori_loop(0, CHUNKS, body, 0)

    def build(s):
        def body(i, carry):
            dense_all(i, s, 0, x_scr, y_scr, z_hi, z_lo)
            return carry

        lax.fori_loop(0, CHUNKS, body, 0)

    def build_slopes(i, carry):
        for s in range(2):
            dense_all(i, s, 1, sx_scr, sy_scr, sz_hi, sz_lo)
        return carry

    build(0)

    def put(slot, at, value):
        top, rest = halves(value)
        p_hi[slot, at : at + value.shape[0], :] = top
        p_lo[slot, at : at + value.shape[0], :] = rest

    def pairs(fill, ref, zs, low, high):
        def body(i, carry):
            for slot in range(2):
                fill(slot, *spans(2 * i + slot))
            for slot in range(2):
                s, lanes = spans(2 * i + slot)
                a = p_hi[slot, low:high, :], p_lo[slot, low:high, :]
                b = zs[0][s, :, lanes], zs[1][s, :, lanes]
                ref[s, low:high, :] += triple_nt(a, b)
            return carry

        return body

    def fill_next(slot, s, lanes):
        for k in range(5):
            put(slot, 32 * k, nx_scr[s, 0:32, lanes] * nyq_scr[s, 3 + k : 4 + k, lanes])
        edge = nyq_scr[s, :, lanes]
        for k in range(3):
            first = edge * nx_scr[s, 35 + 2 * k : 36 + 2 * k, lanes]
            if k < 2:
                second = edge * nx_scr[s, 36 + 2 * k : 37 + 2 * k, lanes]
            else:
                second = jnp.zeros_like(first)
            put(slot, YH + 16 * k, jnp.concatenate([first, second], axis=0))

    def fill_inner(slot, s, lanes):
        for x in range(32):
            put(slot, 16 * x, yq_scr[s, 0:16, lanes] * x_scr[s, x : x + 1, lanes])

    def fill_edge(slot, s, lanes):
        for k in range(5):
            put(slot, 512 + 16 * k, yq_scr[s, 0:16, lanes] * x_scr[s, 35 + k : 36 + k, lanes])

    def fill_both(slot, s, lanes):
        fill_inner(slot, s, lanes)
        fill_edge(slot, s, lanes)

    nacc[...] = jnp.zeros_like(nacc)
    mesh[...] = jnp.zeros_like(mesh)
    edges = []

    def half(s):
        return s * CHUNKS // 2, (s + 1) * CHUNKS // 2

    def spread_own(s, fill, low, high):
        lax.fori_loop(*half(s), pairs(fill, mesh, (z_hi, z_lo), low, high), 0)

    def spread_next(s):
        lax.fori_loop(*half(s), pairs(fill_next, nacc, (nz_hi, nz_lo), 0, YH + CH), 0)

    def send_edge(s):
        view = mesh.at[s].reshape(MESH_ROWS // 16, 16, 256)
        for k in range(5):
            view[32 + k, 8:16] += nacc[s, YH + 8 * k : YH + 8 * k + 8]
        edges.append(remote(mesh.at[s, 512:MESH_ROWS], xr.at[s], 8 + 2 * s, 9 + 2 * s, (dn_r, col)))
        edges[s].start()

    spread_own(0, fill_both, 0, MESH_ROWS)
    build(1)
    for copy in atoms:
        copy.wait()
    values, _ = spline_values(jnp.concatenate([nfrac[0], nfrac[1], nfrac[2]], axis=0))
    for j in range(6):
        nw_scr[j] = values[j]
    build_next(0)
    spread_next(0)
    send_edge(0)

    pl.semaphore_wait(gate, ROWS - 1)
    first = me == 0

    @pl.when(col == COLS // 2)
    def _():
        gone[...] = infl[:, 0, :]
        remote(gone, glast.at[row], 12, 13, (0, 0)).start()

    build_next(1)
    spread_own(1, fill_edge, 512, MESH_ROWS)
    spread_next(1)
    send_edge(1)

    class Exchange:
        def __init__(self, src, dst, par, first):
            self.src, self.dst, self.first = src.at[par], dst.at[par], first

        def start(self):
            for offset in OFFSETS:
                to = device(*offset)
                src = self.src.at[to[0] * COLS + to[1]]
                remote(src, self.dst.at[me], self.first, self.first + 1, to).start()
            self.dst[me] = self.src[me]

        def wait(self):
            every = slice(0, DEVS - 1)
            remote(
                self.src.at[every], self.dst.at[every], self.first, self.first + 1, (up_r, col)
            ).wait()

    forward = [Exchange(sbuf, rbuf, s, 14 + 2 * s) for s in range(2)]
    backward = [Exchange(tbuf, qbuf, s, 18 + 2 * s) for s in range(2)]

    def send_forward(s):
        edges[s].wait()
        view = mesh.at[s].reshape(MESH_ROWS // 16, 16, 256)
        for k in range(5):
            view[0:32, 11 + k, :] += nacc[s, 32 * k : 32 * k + 32]
        for k in range(5):
            view[27 + k] += xr[s, 16 * k : 16 * k + 16]
        a = triple_nt((tab[0], tab[1]), halves(mesh[s, 0:512]))
        for reim in range(2):
            for q in range(4):
                sbuf[s, :, 4 * reim + q, :] = a[
                    128 * reim : 128 * reim + 128, 128 * q : 128 * q + 128
                ]
        forward[s].start()

    for copy in loads[1:]:
        copy.wait()

    send_forward(0)
    spread_own(1, fill_inner, 0, 512)

    for h in range(2):
        fc, fs, lc, ls = [tab[2 + 2 * k + h] for k in range(4)]
        for ref, c, q in ((fb, fc, fs), (gb, fc, -fs), (lb, lc, -ls)):
            ref[h, 0:256, 0:256] = c
            ref[h, 0:256, 256:512] = q
            ref[h, 256:512, 0:256] = -q
            ref[h, 256:512, 256:512] = c
    some = slice(0, ROWS - 1)
    remote(gsend.at[some], grecv.at[some], 0, 1, (up_r, col)).wait()
    lane = lax.broadcasted_iota(jnp.int32, (16, 256), 1)

    def trade(bits, load, store):
        for rest in range(4):
            base = [(a << bits[0]) + (b << bits[1]) + (rest << (2 if bits[0] == 0 else 0))
                    for b in range(2) for a in range(2)]
            blocks = [load(k) for k in base]
            for i, bit in enumerate(bits):
                step = 1 << bit
                low = (lane & step) == 0
                for k in range(4):
                    if k & (1 << i):
                        continue
                    a, b = blocks[k], blocks[k | (1 << i)]
                    blocks[k] = jnp.where(low, a, pltpu.roll(b, step, 1))
                    blocks[k | (1 << i)] = jnp.where(low, pltpu.roll(a, 256 - step, 1), b)
            for k, block in zip(base, blocks):
                store(k, block)

    def in_mode_order(ref, plane, scale):
        def load(k):
            return ref[k // 2, 16 * (k % 2) : 16 * (k % 2) + 16, :] * scale

        def keep(k, block):
            swap[16 * k : 16 * k + 16, :] = block

        def put_in_place(k, block):
            at = 128 * (k % 2) + 16 * (k // 2)
            green[plane, at : at + 16, :] = block

        trade((0, 1), load, keep)
        trade((2, 3), lambda k: swap[16 * k : 16 * k + 16, :], put_in_place)

    unit = 1.0 / float(K) ** 3
    lax.fori_loop(0, CHUNKS, build_slopes, 0)
    in_mode_order(grecv, 0, jnp.where(first, unit, 2.0 * unit))

    @pl.when(first)
    def _():
        remote(glast, glast, 12, 13, (1, 0)).wait_recv()
        in_mode_order(glast, 1, unit)

    @pl.when(col == COLS // 2)
    def _():
        remote(gone, glast.at[0], 12, 13, (0, 0)).wait_send()

    send_forward(1)

    tc, ts = twid[0], twid[1]

    def stacked(buf, par):
        parts = [
            jnp.concatenate([buf[par, :, 2 * j, :], buf[par, :, 2 * j + 1, :]], axis=1)
            for j in range(4)
        ]
        return jnp.concatenate(parts, axis=0)

    def modes(u):
        ur, ui = u[0:256], u[256:512]
        v = jnp.concatenate([ur * tc + ui * ts, ui * tc - ur * ts], axis=1)
        return three_nn(halves(v), (lb[0], lb[1]))

    def turn(s, carry):
        Exchange(sbuf, rbuf, s, 14 + 2 * s).wait()

        @pl.when(me != 0)
        def _():
            u = tall_nn((fb[0], fb[1]), halves(stacked(rbuf, s)))
            escr[...] = jnp.concatenate([green[0], green[0]], axis=1) * modes(u)

        @pl.when(me == 0)
        def _():
            x = halves(stacked(rbuf, s))
            left = fb[0, :, 0:256], fb[1, :, 0:256]
            a = modes(tall_nn(left, (x[0][0:256], x[1][0:256])))
            b = modes(tall_nn(left, (x[0][256:512], x[1][256:512])))
            escr[:, 0:256] = green[0] * a[:, 0:256] - green[1] * b[:, 256:512]
            escr[:, 256:512] = green[0] * a[:, 256:512] + green[1] * b[:, 0:256]

        b = triple_nt(halves(escr[...]), (lb[0], lb[1]))
        br, bi = b[:, 0:256], b[:, 256:512]
        h = jnp.concatenate([br * tc - bi * ts, bi * tc + br * ts], axis=0)
        t = tall_nn((gb[0], gb[1]), halves(h))
        for j in range(4):
            for lh in range(2):
                tbuf[s, :, 2 * j + lh, :] = t[
                    128 * j : 128 * j + 128, 128 * lh : 128 * lh + 128
                ]
        Exchange(tbuf, qbuf, s, 18 + 2 * s).start()
        return carry

    lax.fori_loop(0, 2, turn, 0)

    back = []

    def take_back(s):
        backward[s].wait()
        q = stacked(qbuf, s)
        for xh in range(2):
            picked = jnp.concatenate(
                [q[128 * xh : 128 * xh + 128], q[256 + 128 * xh : 384 + 128 * xh]], axis=0
            )
            pot[s, 256 * xh : 256 * xh + 256, :] = triple_nn(halves(picked.T), (tab[0], tab[1]))
        view = pot.at[s].reshape(32, 16, 256)
        for k in range(5):
            ys[s, 32 * k : 32 * k + 32] = view[:, 11 + k, :]
        for k in range(5):
            corner[s, 8 * k : 8 * k + 8] = view[27 + k, 8:16]
        at = 22 + 6 * s
        back.append([
            remote(ys.at[s], yb.at[s], at, at + 1, (row, up_c)),
            remote(pot.at[s, 432:512], xb.at[s], at + 2, at + 3, (up_r, col)),
            remote(corner.at[s], cb.at[s], at + 4, at + 5, (up_r, up_c)),
        ])
        for copy in back[s]:
            copy.start()
        spread_out(fint, s, 0, pot[s])

    def take_halo(s):
        for copy in back[s]:
            copy.wait()
        for at, ref in ((0, yb), (YH, xb), (YH + XH, cb)):
            spread_out(fhal, s, at, ref[s])

    def spread_out(ref, s, at, value):
        top, rest = halves(value)
        n = value.shape[0]
        ref[s, at : at + n, 0:256] = top
        ref[s, at : at + n, 256:512] = rest
        ref[s, at : at + n, 512:768] = top

    def sample(ref, s, lanes):
        top = jnp.concatenate([z_hi[s, :, lanes], sz_hi[s, :, lanes]], axis=1)
        rest = jnp.concatenate([z_lo[s, :, lanes], sz_lo[s, :, lanes]], axis=1)
        both = dot_nn(ref[s], jnp.concatenate([top, top, rest], axis=0))
        return both[:, 0:GCHUNK], both[:, GCHUNK : 2 * GCHUNK]

    def window(i):
        s = lax.div(i, GCHUNKS)
        return s, pl.ds(pl.multiple_of(lax.rem(i, GCHUNKS) * GCHUNK, GCHUNK), GCHUNK)

    def down(value):
        return jnp.sum(value, axis=0, keepdims=True)

    def four(body):
        def several(i, carry):
            for k in range(4):
                carry = body(4 * i + k, carry)
            return carry

        return several

    def gather_inner(i, carry):
        s, lanes = window(i)
        plain, slope = sample(fint, s, lanes)
        a1 = a2 = a3 = jnp.zeros((16, GCHUNK), F32)
        for x in range(32):
            wx, sx = x_scr[s, x : x + 1, lanes], sx_scr[s, x : x + 1, lanes]
            piece = plain[16 * x : 16 * x + 16]
            a1 = a1 + piece * sx
            a2 = a2 + piece * wx
            a3 = a3 + slope[16 * x : 16 * x + 16] * wx
        wy, sy = y_scr[s, 0:16, lanes], sy_scr[s, 0:16, lanes]
        part[s, 0:1, lanes] = down(a1 * wy)
        part[s, 1:2, lanes] = down(a2 * sy)
        part[s, 2:3, lanes] = down(a3 * wy)
        return carry

    def gather_halo(i, carry):
        s, lanes = window(i)
        plain, slope = sample(fhal, s, lanes)
        a1 = a2 = a3 = jnp.zeros((16, GCHUNK), F32)
        b1 = b2 = b3 = jnp.zeros((32, GCHUNK), F32)
        e1 = e2 = e3 = jnp.zeros((8, GCHUNK), F32)
        for k in range(5):
            wy, sy = y_scr[s, 19 + k : 20 + k, lanes], sy_scr[s, 19 + k : 20 + k, lanes]
            wx, sx = x_scr[s, 35 + k : 36 + k, lanes], sx_scr[s, 35 + k : 36 + k, lanes]
            piece = plain[32 * k : 32 * k + 32]
            b1 = b1 + piece * wy
            b2 = b2 + piece * sy
            b3 = b3 + slope[32 * k : 32 * k + 32] * wy
            at = YH + 16 * k
            piece = plain[at : at + 16]
            a1 = a1 + piece * sx
            a2 = a2 + piece * wx
            a3 = a3 + slope[at : at + 16] * wx
            at = YH + XH + 8 * k
            piece = plain[at : at + 8]
            e1 = e1 + piece * sx
            e2 = e2 + piece * wx
            e3 = e3 + slope[at : at + 8] * wx
        wy, sy = y_scr[s, 0:16, lanes], sy_scr[s, 0:16, lanes]
        vy, ty = y_scr[s, 16:24, lanes], sy_scr[s, 16:24, lanes]
        wx, sx = x_scr[s, 0:32, lanes], sx_scr[s, 0:32, lanes]

        def finish(d, a, m, e, n, b, q):
            total = part[s, d : d + 1, lanes] + down(a * m) + down(e * n) + down(b * q)
            forces[d, pl.ds(s, 1), lanes] = -yq_scr[s, 24:25, lanes] * total

        finish(0, a1, wy, e1, vy, b1, sx)
        finish(1, a2, sy, e2, ty, b2, wx)
        finish(2, a3, wy, e3, vy, b3, wx)
        return carry

    def gather(body, s):
        lax.fori_loop(s * GCHUNKS // 4, (s + 1) * GCHUNKS // 4, four(body), 0)

    take_back(0)
    gather(gather_inner, 0)
    take_back(1)
    gather(gather_inner, 1)
    take_halo(0)
    gather(gather_halo, 0)
    take_halo(1)
    gather(gather_halo, 1)


def shards(consts, cell_index, fraction, charge, atom_count, influence):
    vmem = pl.BlockSpec(memory_space=pltpu.VMEM)
    anywhere = pl.BlockSpec(memory_space=pl.ANY)
    args = [
        jnp.transpose(cell_index, (1, 0, 2)), jnp.transpose(fraction, (1, 0, 2)), charge,
        jnp.transpose(atom_count), influence, jnp.asarray(consts[0]), jnp.asarray(consts[1]),
    ]
    v = pltpu.VMEM
    scratch = [
        v((3, 2, ATOMS), jnp.int32), v((3, 2, ATOMS), F32), v((2, ATOMS), F32),
        v((1, 2), jnp.int32), v((32, 16, 256), F32), v((10, 256, 256), BF16), v((2, 256, 256), F32),
        v((2, 6, 6, ATOMS), F32), v((2, 40, ATOMS), F32), v((2, 24, ATOMS), F32),
        v((2, 25, ATOMS), F32), v((2, 256, ATOMS), BF16), v((2, 256, ATOMS), BF16),
        v((2, 40, ATOMS), F32), v((2, 24, ATOMS), F32), v((2, 256, ATOMS), BF16),
        v((2, 256, ATOMS), BF16), v((2, MESH_ROWS, CHUNK), BF16), v((2, MESH_ROWS, CHUNK), BF16),
        v((3, 2, ATOMS), jnp.int32), v((3, 2, ATOMS), F32), v((2, ATOMS), F32), v((2, ATOMS), F32),
        v((6, 6, ATOMS), F32), v((2, 40, ATOMS), F32), v((2, 8, ATOMS), F32),
        v((2, 256, ATOMS), BF16), v((2, 256, ATOMS), BF16),
        v((2, YH + CH, 256), F32), v((2, XH, 256), F32), v((2, MESH_ROWS, 256), F32),
        v((ROWS, 32, 256), F32), v((ROWS, 32, 256), F32), v((ROWS, 32, 256), F32),
        v((2, 256, 256), F32), v((2, 512, 512), BF16), v((2, 512, 512), BF16),
        v((2, 512, 512), BF16), v((256, 512), F32),
        v((2, DEVS, 8, 128), F32), v((2, DEVS, 8, 128), F32), v((2, DEVS, 8, 128), F32),
        v((2, DEVS, 8, 128), F32), v((2, 512, 256), F32),
        v((2, YH, 256), F32), v((2, 40, 256), F32),
        v((2, YH, 256), F32), v((2, XH, 256), F32), v((2, 40, 256), F32),
        v((2, 512, 768), BF16), v((2, HALO, 768), BF16), v((2, 3, ATOMS), F32),
        v((256, 256), F32), v((32, 256), F32),
        pltpu.SemaphoreType.DMA((34,)), pltpu.SemaphoreType.DMA((7,)), pltpu.SemaphoreType.REGULAR,
    ]
    out = pl.pallas_call(
        kernel,
        out_shape=pltpu.VMEM((3, 2, ATOMS), F32),
        in_specs=[anywhere] * 7,
        out_specs=vmem,
        scratch_shapes=scratch,
        compiler_params=pltpu.CompilerParams(
            collective_id=0, has_side_effects=True, vmem_limit_bytes=66_000_000
        ),
    )(*args)
    return jnp.transpose(out, (1, 0, 2))


def solution(mesh):
    placed = (
        P(None, None, ("row", "col")),
        P(None, None, ("row", "col")),
        P(None, ("row", "col")),
        P(None, ("row", "col")),
        P("row", "col", None),
    )
    return jax.shard_map(
        functools.partial(shards, tables()), mesh=mesh, in_specs=placed,
        out_specs=P(None, None, ("row", "col")), check_vma=False,
    )
```

```python
import functools

import jax
import jax.numpy as jnp
import numpy as np
from jax import lax
from jax.experimental import pallas as pl
from jax.experimental.pallas import tpu as pltpu
from jax.sharding import PartitionSpec as P

F32 = jnp.float32
BF16 = jnp.bfloat16
MESH = pl.DeviceIdType.MESH

K = 256
ROWS = 8
COLS = 16
DEVS = ROWS * COLS
ATOMS = 2048
CHUNK = 512
CHUNKS = ATOMS // CHUNK
GCHUNK = 256
GCHUNKS = ATOMS // GCHUNK

YH, XH, CH = 160, 80, 48
HALO = YH + XH + CH
MESH_ROWS = 592


def far_first():
    offsets = [d for d in np.ndindex(4, 4, 4, 2) if d != (0, 0, 0, 0)]
    offsets.sort(key=lambda d: (-sum(min(k, 4 - k) for k in d[:3]), d[3], d[0] + 2 * d[1] + 3 * d[2]))
    lanes = {}
    for d in offsets:
        lanes.setdefault(d[0] or 10 + d[1] if d[0] or d[1] else 20 + d[2], []).append(d)
    out = []
    while any(lanes.values()):
        out += [lane.pop(0) for lane in lanes.values() if lane]
    return out


OFFSETS = far_first()


def halves(x):
    top = x.astype(BF16)
    return top, (x - top.astype(F32)).astype(BF16)


def np_halves(x):
    x = np.asarray(x, np.float32)
    top = x.astype(jnp.bfloat16)
    return [top, (x - top.astype(np.float32)).astype(jnp.bfloat16)]


def tables():
    d = np.arange(DEVS)
    waves = 16 * (d % COLS) + 2 * (d // COLS) + (d % COLS >= COLS // 2)
    turn = 2.0 * np.pi / K
    angle = (waves[:, None] * np.arange(K)[None, :] % K) * turn
    sines = -np.sin(angle)
    sines[0] = 1.0 - 2.0 * (np.arange(K) % 2)
    out = np_halves(np.concatenate([np.cos(angle), sines]))
    spot = np.arange(256)
    rx, cc = 2 * (spot % 128 // 16) + spot // 128, spot % 16
    angle = ((rx[:, None] * rx[None, :] + cc[:, None] * cc[None, :]) % 16) * (16 * turn)
    out += np_halves(np.cos(angle)) + np_halves(np.sin(angle))
    xl, yl = spot // 16, spot % 16
    angle = ((xl[:, None] * xl[None, :] + yl[:, None] * yl[None, :]) % 16) * (16 * turn)
    out += np_halves(np.cos(angle)) + np_halves(np.sin(angle))
    angle = ((rx[:, None] * xl[None, :] + cc[:, None] * yl[None, :]) % K) * turn
    twiddles = np.stack([np.cos(angle), np.sin(angle)]).astype(np.float32)
    return np.stack(out), twiddles


def spline_values(f):
    nothing = jnp.zeros_like(f)
    levels = [f, 1.0 - f]
    slopes = levels
    for degree in range(3, 7):
        padded = levels + [nothing]
        following = []
        for o in range(degree):
            value = (f + float(o)) * padded[o]
            if o > 0:
                value = value + (float(degree - o) - f) * padded[o - 1]
            following.append(value * (1.0 / (degree - 1)))
        if degree == 6:
            slopes = [padded[0]] + [padded[o] - padded[o - 1] for o in range(1, 6)]
        levels = following
    return levels, slopes


def dot_nn(a, b):
    return lax.dot_general(a, b, (((1,), (0,)), ((), ())), preferred_element_type=F32)


def dot_nt(a, b):
    return lax.dot_general(a, b, (((1,), (1,)), ((), ())), preferred_element_type=F32)


def triple_nn(a, b):
    left = jnp.concatenate([a[0], a[1], a[0]], axis=1)
    return dot_nn(left, jnp.concatenate([b[0], b[0], b[1]], axis=0))


def three_nn(a, b):
    return dot_nn(a[0], b[0]) + dot_nn(a[1], b[0]) + dot_nn(a[0], b[1])


def tall_nn(a, b):
    n = a[0].shape[0] // 2
    return jnp.concatenate(
        [three_nn((a[0][q], a[1][q]), b) for q in (slice(0, n), slice(n, 2 * n))], axis=0
    )


def triple_nt(a, b):
    left = jnp.concatenate([a[0], a[1], a[0]], axis=1)
    return dot_nt(left, jnp.concatenate([b[0], b[0], b[1]], axis=1))


def dense(gap, rows):
    total = jnp.where(gap == 0, rows[0], 0.0)
    for j in range(1, 6):
        total = jnp.where(gap == j, rows[j], total)
    return total


def tiles_of(anchor, rows, size):
    gap = anchor - lax.broadcasted_iota(jnp.int32, (size, anchor.shape[1]), 0)
    return dense(gap & (size - 1), rows), gap >> (3 if size == 8 else 4)


def kernel(
    cell_hbm, frac_hbm, charge_hbm, count_hbm, infl_hbm, tab_hbm, twid_hbm,
    forces,
    cell, frac, charge, count, infl, tab, twid, w_scr, x_scr, y_scr, yq_scr, z_hi, z_lo, sx_scr, sy_scr, sz_hi, sz_lo,
    p_hi, p_lo, ncell, nfrac, qs, nq, nw_scr, nx_scr, nyq_scr, nz_hi, nz_lo, nacc, xr, mesh, gsend, grecv, glast, green, fb, gb, lb, escr,
    sbuf, rbuf, tbuf, qbuf, pot, ys, corner, yb, xb, cb, fint, fhal, part, swap, gone,
    sems, local, gate,
):
    row = lax.axis_index("row")
    col = lax.axis_index("col")
    me = row * COLS + col
    up_r, dn_r = lax.rem(row + 1, ROWS), lax.rem(row + ROWS - 1, ROWS)
    up_c, dn_c = lax.rem(col + 1, COLS), lax.rem(col + COLS - 1, COLS)
    core = lax.rem(col, 2)
    px = lax.rem(lax.div(col, 2), 2) * 2 + lax.rem(row, 2)
    py, pz = lax.div(col, 4), lax.div(row, 2)

    xs = [lax.rem(px + d, 4) for d in range(4)]
    x_row, x_col = [lax.rem(x, 2) for x in xs], [lax.div(x, 2) * 2 for x in xs]
    y_col = [lax.rem(py + d, 4) * 4 for d in range(4)]
    z_row = [lax.rem(pz + d, 4) * 2 for d in range(4)]
    cores = core, 1 - core

    def device(dx, dy, dz, dc):
        return z_row[dz] + x_row[dx], y_col[dy] + x_col[dx] + cores[dc]

    loads = [
        pltpu.make_async_copy(infl_hbm, infl, local.at[0]),
        pltpu.make_async_copy(tab_hbm, tab, local.at[1]),
        pltpu.make_async_copy(twid_hbm, twid, local.at[2]),
    ]
    inputs = [
        pltpu.make_async_copy(src, dst, local.at[3 + k])
        for k, (src, dst) in enumerate((
            (cell_hbm, cell), (frac_hbm, frac), (charge_hbm, charge), (count_hbm, count)
        ))
    ]
    for copy in inputs + loads:
        copy.start()

    barrier = pltpu.get_barrier_semaphore()

    def greet_column(k, carry):
        to = row, lax.rem(col + k, COLS)
        pl.semaphore_signal(barrier, inc=1, device_id=to, device_id_type=MESH)
        return carry

    def greet_row(k, carry):
        to = lax.rem(row + k, ROWS), col
        pl.semaphore_signal(barrier, inc=1, device_id=to, device_id_type=MESH)
        return carry

    def vouch(k, carry):
        to = lax.rem(row + k, ROWS), col
        pl.semaphore_signal(gate, inc=1, device_id=to, device_id_type=MESH)
        return carry

    lax.fori_loop(1, ROWS, greet_row, 0)
    lax.fori_loop(1, COLS, greet_column, 0)

    def remote(src, dst, send, recv, to):
        return pltpu.make_async_remote_copy(
            src_ref=src, dst_ref=dst, send_sem=sems.at[send], recv_sem=sems.at[recv],
            device_id=to, device_id_type=MESH,
        )

    for copy in inputs:
        copy.wait()
    slot = lax.broadcasted_iota(jnp.int32, (1, ATOMS), 1)
    for s in range(2):
        masked = jnp.where(slot < count[0:1, s : s + 1], charge[s : s + 1], 0.0)
        yq_scr[s, 24:25] = masked
        qs[s : s + 1] = masked

    pl.semaphore_wait(barrier, ROWS + COLS - 2)
    lax.fori_loop(1, ROWS, vouch, 0)
    atoms = [
        remote(src, dst, 2 + 2 * k, 3 + 2 * k, (row, dn_c))
        for k, (src, dst) in enumerate(((cell, ncell), (frac, nfrac), (qs, nq)))
    ]
    for copy in atoms:
        copy.start()

    loads[0].wait()
    for odd in range(2):

        @pl.when(lax.div(col, COLS // 2) == odd)
        def _():
            for k in range(ROWS):
                gsend[k] = infl[:, 2 * k + odd, :]

    def send_green(k, carry):
        there = lax.rem(row + k, ROWS)
        remote(gsend.at[there], grecv.at[row], 0, 1, (there, col)).start()
        return carry

    lax.fori_loop(1, ROWS, send_green, 0)
    grecv[row] = gsend[row]

    values, slopes = spline_values(jnp.concatenate([frac[0], frac[1], frac[2]], axis=0))
    for j in range(6):
        w_scr[0, j] = values[j]
        w_scr[1, j] = slopes[j]

    def spans(i):
        s = lax.div(i, CHUNKS)
        return s, pl.ds(pl.multiple_of(lax.rem(i, CHUNKS) * CHUNK, CHUNK), CHUNK)

    def pick(kind):
        return lambda s, dim, lanes: [
            w_scr[kind, j, 2 * dim + s : 2 * dim + s + 1, lanes] for j in range(6)
        ]

    def dense_x(anchor, rows, xo, s, lanes):
        value, tile = tiles_of(anchor, rows, 8)
        for b, at in ((0, 0), (1, 8), (2, 16), (3, 24), (-1, 32)):
            xo[s, at : at + 8, lanes] = jnp.where(tile == b, value, 0.0)

    def dense_z(anchor, rows, hi_ref, lo_ref, s, lanes):
        value, tile = tiles_of(anchor, rows, 16)
        top, rest = halves(value)
        tile = (tile & 15).astype(F32).astype(BF16)
        none = jnp.zeros_like(top)
        for b in range(16):
            here = tile == jnp.asarray(float(b), BF16)
            hi_ref[s, 16 * b : 16 * b + 16, lanes] = jnp.where(here, top, none)
            lo_ref[s, 16 * b : 16 * b + 16, lanes] = jnp.where(here, rest, none)

    def dense_all(i, s, kind, xo, yo, hi_ref, lo_ref):
        rows_of = pick(kind)
        for k in range(CHUNK // 128):
            lanes = pl.ds(pl.multiple_of(i * CHUNK + 128 * k, 128), 128)
            dense_x(cell[0, s : s + 1, lanes] - row * 32, rows_of(s, 0, lanes), xo, s, lanes)
            anchor = cell[1, s : s + 1, lanes] - col * 16
            value, tile = tiles_of(anchor, rows_of(s, 1, lanes), 8)
            for b, at in ((0, 0), (1, 8), (-1, 16)):
                y = jnp.where(tile == b, value, 0.0)
                yo[s, at : at + 8, lanes] = y
                if kind == 0:
                    yq_scr[s, at : at + 8, lanes] = y * yq_scr[s, 24:25, lanes]
            dense_z(cell[2, s : s + 1, lanes], rows_of(s, 2, lanes), hi_ref, lo_ref, s, lanes)

    def build_next(s):
        def body(i, carry):
            for k in range(CHUNK // 128):
                lanes = pl.ds(pl.multiple_of(i * CHUNK + 128 * k, 128), 128)
                rows_of = [
                    [nw_scr[j, 2 * d + s : 2 * d + s + 1, lanes] for j in range(6)]
                    for d in range(3)
                ]
                dense_x(ncell[0, s : s + 1, lanes] - row * 32, rows_of[0], nx_scr, s, lanes)
                anchor = ncell[1, s : s + 1, lanes] - up_c * 16
                value, tile = tiles_of(anchor, rows_of[1], 8)
                value = jnp.where(tile == -1, value, 0.0) * nq[s : s + 1, lanes]
                nyq_scr[s, :, lanes] = value
                dense_z(ncell[2, s : s + 1, lanes], rows_of[2], nz_hi, nz_lo, s, lanes)
            return carry

        lax.fori_loop(0, CHUNKS, body, 0)

    def build(s):
        def body(i, carry):
            dense_all(i, s, 0, x_scr, y_scr, z_hi, z_lo)
            return carry

        lax.fori_loop(0, CHUNKS, body, 0)

    def build_slopes(i, carry):
        for s in range(2):
            dense_all(i, s, 1, sx_scr, sy_scr, sz_hi, sz_lo)
        return carry

    build(0)

    def put(slot, at, value):
        top, rest = halves(value)
        p_hi[slot, at : at + value.shape[0], :] = top
        p_lo[slot, at : at + value.shape[0], :] = rest

    def pairs(fill, ref, zs, low, high):
        def body(i, carry):
            for slot in range(2):
                fill(slot, *spans(2 * i + slot))
            for slot in range(2):
                s, lanes = spans(2 * i + slot)
                a = p_hi[slot, low:high, :], p_lo[slot, low:high, :]
                b = zs[0][s, :, lanes], zs[1][s, :, lanes]
                ref[s, low:high, :] += triple_nt(a, b)
            return carry

        return body

    def fill_next(slot, s, lanes):
        for k in range(5):
            put(slot, 32 * k, nx_scr[s, 0:32, lanes] * nyq_scr[s, 3 + k : 4 + k, lanes])
        edge = nyq_scr[s, :, lanes]
        for k in range(3):
            first = edge * nx_scr[s, 35 + 2 * k : 36 + 2 * k, lanes]
            if k < 2:
                second = edge * nx_scr[s, 36 + 2 * k : 37 + 2 * k, lanes]
            else:
                second = jnp.zeros_like(first)
            put(slot, YH + 16 * k, jnp.concatenate([first, second], axis=0))

    def fill_inner(slot, s, lanes):
        for x in range(32):
            put(slot, 16 * x, yq_scr[s, 0:16, lanes] * x_scr[s, x : x + 1, lanes])

    def fill_edge(slot, s, lanes):
        for k in range(5):
            put(slot, 512 + 16 * k, yq_scr[s, 0:16, lanes] * x_scr[s, 35 + k : 36 + k, lanes])

    def fill_both(slot, s, lanes):
        fill_inner(slot, s, lanes)
        fill_edge(slot, s, lanes)

    nacc[...] = jnp.zeros_like(nacc)
    mesh[...] = jnp.zeros_like(mesh)
    edges = []

    def half(s):
        return s * CHUNKS // 2, (s + 1) * CHUNKS // 2

    def spread_own(s, fill, low, high):
        lax.fori_loop(*half(s), pairs(fill, mesh, (z_hi, z_lo), low, high), 0)

    def spread_next(s):
        lax.fori_loop(*half(s), pairs(fill_next, nacc, (nz_hi, nz_lo), 0, YH + CH), 0)

    def send_edge(s):
        view = mesh.at[s].reshape(MESH_ROWS // 16, 16, 256)
        for k in range(5):
            view[32 + k, 8:16] += nacc[s, YH + 8 * k : YH + 8 * k + 8]
        edges.append(remote(mesh.at[s, 512:MESH_ROWS], xr.at[s], 8 + 2 * s, 9 + 2 * s, (dn_r, col)))
        edges[s].start()

    spread_own(0, fill_both, 0, MESH_ROWS)
    build(1)
    for copy in atoms:
        copy.wait()
    values, _ = spline_values(jnp.concatenate([nfrac[0], nfrac[1], nfrac[2]], axis=0))
    for j in range(6):
        nw_scr[j] = values[j]
    build_next(0)
    spread_next(0)
    send_edge(0)

    pl.semaphore_wait(gate, ROWS - 1)
    first = me == 0

    @pl.when(col == COLS // 2)
    def _():
        gone[...] = infl[:, 0, :]
        remote(gone, glast.at[row], 12, 13, (0, 0)).start()

    build_next(1)
    spread_own(1, fill_edge, 512, MESH_ROWS)
    spread_next(1)
    send_edge(1)

    class Exchange:
        def __init__(self, src, dst, par, first):
            self.src, self.dst, self.first = src.at[par], dst.at[par], first

        def start(self):
            for offset in OFFSETS:
                to = device(*offset)
                src = self.src.at[to[0] * COLS + to[1]]
                remote(src, self.dst.at[me], self.first, self.first + 1, to).start()
            self.dst[me] = self.src[me]

        def wait(self):
            every = slice(0, DEVS - 1)
            remote(
                self.src.at[every], self.dst.at[every], self.first, self.first + 1, (up_r, col)
            ).wait()

    forward = [Exchange(sbuf, rbuf, s, 14 + 2 * s) for s in range(2)]
    backward = [Exchange(tbuf, qbuf, s, 18 + 2 * s) for s in range(2)]

    def send_forward(s):
        edges[s].wait()
        view = mesh.at[s].reshape(MESH_ROWS // 16, 16, 256)
        for k in range(5):
            view[0:32, 11 + k, :] += nacc[s, 32 * k : 32 * k + 32]
        for k in range(5):
            view[27 + k] += xr[s, 16 * k : 16 * k + 16]
        a = triple_nt((tab[0], tab[1]), halves(mesh[s, 0:512]))
        for reim in range(2):
            for q in range(4):
                sbuf[s, :, 4 * reim + q, :] = a[
                    128 * reim : 128 * reim + 128, 128 * q : 128 * q + 128
                ]
        forward[s].start()

    for copy in loads[1:]:
        copy.wait()

    send_forward(0)
    spread_own(1, fill_inner, 0, 512)

    for h in range(2):
        fc, fs, lc, ls = [tab[2 + 2 * k + h] for k in range(4)]
        for ref, c, q in ((fb, fc, fs), (gb, fc, -fs), (lb, lc, -ls)):
            ref[h, 0:256, 0:256] = c
            ref[h, 0:256, 256:512] = q
            ref[h, 256:512, 0:256] = -q
            ref[h, 256:512, 256:512] = c
    some = slice(0, ROWS - 1)
    remote(gsend.at[some], grecv.at[some], 0, 1, (up_r, col)).wait()
    lane = lax.broadcasted_iota(jnp.int32, (16, 256), 1)

    def trade(bits, load, store):
        for rest in range(4):
            base = [(a << bits[0]) + (b << bits[1]) + (rest << (2 if bits[0] == 0 else 0))
                    for b in range(2) for a in range(2)]
            blocks = [load(k) for k in base]
            for i, bit in enumerate(bits):
                step = 1 << bit
                low = (lane & step) == 0
                for k in range(4):
                    if k & (1 << i):
                        continue
                    a, b = blocks[k], blocks[k | (1 << i)]
                    blocks[k] = jnp.where(low, a, pltpu.roll(b, step, 1))
                    blocks[k | (1 << i)] = jnp.where(low, pltpu.roll(a, 256 - step, 1), b)
            for k, block in zip(base, blocks):
                store(k, block)

    def in_mode_order(ref, plane, scale):
        def load(k):
            return ref[k // 2, 16 * (k % 2) : 16 * (k % 2) + 16, :] * scale

        def keep(k, block):
            swap[16 * k : 16 * k + 16, :] = block

        def put_in_place(k, block):
            at = 128 * (k % 2) + 16 * (k // 2)
            green[plane, at : at + 16, :] = block

        trade((0, 1), load, keep)
        trade((2, 3), lambda k: swap[16 * k : 16 * k + 16, :], put_in_place)

    unit = 1.0 / float(K) ** 3
    lax.fori_loop(0, CHUNKS, build_slopes, 0)
    in_mode_order(grecv, 0, jnp.where(first, unit, 2.0 * unit))

    @pl.when(first)
    def _():
        remote(glast, glast, 12, 13, (1, 0)).wait_recv()
        in_mode_order(glast, 1, unit)

    @pl.when(col == COLS // 2)
    def _():
        remote(gone, glast.at[0], 12, 13, (0, 0)).wait_send()

    send_forward(1)

    tc, ts = twid[0], twid[1]

    def stacked(buf, par):
        parts = [
            jnp.concatenate([buf[par, :, 2 * j, :], buf[par, :, 2 * j + 1, :]], axis=1)
            for j in range(4)
        ]
        return jnp.concatenate(parts, axis=0)

    def modes(u):
        ur, ui = u[0:256], u[256:512]
        v = jnp.concatenate([ur * tc + ui * ts, ui * tc - ur * ts], axis=1)
        return three_nn(halves(v), (lb[0], lb[1]))

    def turn(s, carry):
        Exchange(sbuf, rbuf, s, 14 + 2 * s).wait()

        @pl.when(me != 0)
        def _():
            u = tall_nn((fb[0], fb[1]), halves(stacked(rbuf, s)))
            escr[...] = jnp.concatenate([green[0], green[0]], axis=1) * modes(u)

        @pl.when(me == 0)
        def _():
            x = halves(stacked(rbuf, s))
            left = fb[0, :, 0:256], fb[1, :, 0:256]
            a = modes(tall_nn(left, (x[0][0:256], x[1][0:256])))
            b = modes(tall_nn(left, (x[0][256:512], x[1][256:512])))
            escr[:, 0:256] = green[0] * a[:, 0:256] - green[1] * b[:, 256:512]
            escr[:, 256:512] = green[0] * a[:, 256:512] + green[1] * b[:, 0:256]

        b = triple_nt(halves(escr[...]), (lb[0], lb[1]))
        br, bi = b[:, 0:256], b[:, 256:512]
        h = jnp.concatenate([br * tc - bi * ts, bi * tc + br * ts], axis=0)
        t = tall_nn((gb[0], gb[1]), halves(h))
        for j in range(4):
            for lh in range(2):
                tbuf[s, :, 2 * j + lh, :] = t[
                    128 * j : 128 * j + 128, 128 * lh : 128 * lh + 128
                ]
        Exchange(tbuf, qbuf, s, 18 + 2 * s).start()
        return carry

    lax.fori_loop(0, 2, turn, 0)

    back = []

    def take_back(s):
        backward[s].wait()
        q = stacked(qbuf, s)
        for xh in range(2):
            picked = jnp.concatenate(
                [q[128 * xh : 128 * xh + 128], q[256 + 128 * xh : 384 + 128 * xh]], axis=0
            )
            pot[s, 256 * xh : 256 * xh + 256, :] = triple_nn(halves(picked.T), (tab[0], tab[1]))
        view = pot.at[s].reshape(32, 16, 256)
        for k in range(5):
            ys[s, 32 * k : 32 * k + 32] = view[:, 11 + k, :]
        for k in range(5):
            corner[s, 8 * k : 8 * k + 8] = view[27 + k, 8:16]
        at = 22 + 6 * s
        back.append([
            remote(ys.at[s], yb.at[s], at, at + 1, (row, up_c)),
            remote(pot.at[s, 432:512], xb.at[s], at + 2, at + 3, (up_r, col)),
            remote(corner.at[s], cb.at[s], at + 4, at + 5, (up_r, up_c)),
        ])
        for copy in back[s]:
            copy.start()
        spread_out(fint, s, 0, pot[s])

    def take_halo(s):
        for copy in back[s]:
            copy.wait()
        for at, ref in ((0, yb), (YH, xb), (YH + XH, cb)):
            spread_out(fhal, s, at, ref[s])

    def spread_out(ref, s, at, value):
        top, rest = halves(value)
        n = value.shape[0]
        ref[s, at : at + n, 0:256] = top
        ref[s, at : at + n, 256:512] = rest
        ref[s, at : at + n, 512:768] = top

    def sample(ref, s, lanes):
        top = jnp.concatenate([z_hi[s, :, lanes], sz_hi[s, :, lanes]], axis=1)
        rest = jnp.concatenate([z_lo[s, :, lanes], sz_lo[s, :, lanes]], axis=1)
        both = dot_nn(ref[s], jnp.concatenate([top, top, rest], axis=0))
        return both[:, 0:GCHUNK], both[:, GCHUNK : 2 * GCHUNK]

    def window(i):
        s = lax.div(i, GCHUNKS)
        return s, pl.ds(pl.multiple_of(lax.rem(i, GCHUNKS) * GCHUNK, GCHUNK), GCHUNK)

    def down(value):
        return jnp.sum(value, axis=0, keepdims=True)

    def four(body):
        def several(i, carry):
            for k in range(4):
                carry = body(4 * i + k, carry)
            return carry

        return several

    def gather_inner(i, carry):
        s, lanes = window(i)
        plain, slope = sample(fint, s, lanes)
        a1 = a2 = a3 = jnp.zeros((16, GCHUNK), F32)
        for x in range(32):
            wx, sx = x_scr[s, x : x + 1, lanes], sx_scr[s, x : x + 1, lanes]
            piece = plain[16 * x : 16 * x + 16]
            a1 = a1 + piece * sx
            a2 = a2 + piece * wx
            a3 = a3 + slope[16 * x : 16 * x + 16] * wx
        wy, sy = y_scr[s, 0:16, lanes], sy_scr[s, 0:16, lanes]
        part[s, 0:1, lanes] = down(a1 * wy)
        part[s, 1:2, lanes] = down(a2 * sy)
        part[s, 2:3, lanes] = down(a3 * wy)
        return carry

    def gather_halo(i, carry):
        s, lanes = window(i)
        plain, slope = sample(fhal, s, lanes)
        a1 = a2 = a3 = jnp.zeros((16, GCHUNK), F32)
        b1 = b2 = b3 = jnp.zeros((32, GCHUNK), F32)
        e1 = e2 = e3 = jnp.zeros((8, GCHUNK), F32)
        for k in range(5):
            wy, sy = y_scr[s, 19 + k : 20 + k, lanes], sy_scr[s, 19 + k : 20 + k, lanes]
            wx, sx = x_scr[s, 35 + k : 36 + k, lanes], sx_scr[s, 35 + k : 36 + k, lanes]
            piece = plain[32 * k : 32 * k + 32]
            b1 = b1 + piece * wy
            b2 = b2 + piece * sy
            b3 = b3 + slope[32 * k : 32 * k + 32] * wy
            at = YH + 16 * k
            piece = plain[at : at + 16]
            a1 = a1 + piece * sx
            a2 = a2 + piece * wx
            a3 = a3 + slope[at : at + 16] * wx
            at = YH + XH + 8 * k
            piece = plain[at : at + 8]
            e1 = e1 + piece * sx
            e2 = e2 + piece * wx
            e3 = e3 + slope[at : at + 8] * wx
        wy, sy = y_scr[s, 0:16, lanes], sy_scr[s, 0:16, lanes]
        vy, ty = y_scr[s, 16:24, lanes], sy_scr[s, 16:24, lanes]
        wx, sx = x_scr[s, 0:32, lanes], sx_scr[s, 0:32, lanes]

        def finish(d, a, m, e, n, b, q):
            total = part[s, d : d + 1, lanes] + down(a * m) + down(e * n) + down(b * q)
            forces[d, pl.ds(s, 1), lanes] = -yq_scr[s, 24:25, lanes] * total

        finish(0, a1, wy, e1, vy, b1, sx)
        finish(1, a2, sy, e2, ty, b2, wx)
        finish(2, a3, wy, e3, vy, b3, wx)
        return carry

    def gather(body, s):
        lax.fori_loop(s * GCHUNKS // 4, (s + 1) * GCHUNKS // 4, four(body), 0)

    take_back(0)
    gather(gather_inner, 0)
    take_back(1)
    gather(gather_inner, 1)
    take_halo(0)
    gather(gather_halo, 0)
    take_halo(1)
    gather(gather_halo, 1)


def shards(consts, cell_index, fraction, charge, atom_count, influence):
    vmem = pl.BlockSpec(memory_space=pltpu.VMEM)
    anywhere = pl.BlockSpec(memory_space=pl.ANY)
    args = [
        jnp.transpose(cell_index, (1, 0, 2)), jnp.transpose(fraction, (1, 0, 2)), charge,
        jnp.transpose(atom_count), influence, jnp.asarray(consts[0]), jnp.asarray(consts[1]),
    ]
    v = pltpu.VMEM
    scratch = [
        v((3, 2, ATOMS), jnp.int32), v((3, 2, ATOMS), F32), v((2, ATOMS), F32),
        v((1, 2), jnp.int32), v((32, 16, 256), F32), v((10, 256, 256), BF16), v((2, 256, 256), F32),
        v((2, 6, 6, ATOMS), F32), v((2, 40, ATOMS), F32), v((2, 24, ATOMS), F32),
        v((2, 25, ATOMS), F32), v((2, 256, ATOMS), BF16), v((2, 256, ATOMS), BF16),
        v((2, 40, ATOMS), F32), v((2, 24, ATOMS), F32), v((2, 256, ATOMS), BF16),
        v((2, 256, ATOMS), BF16), v((2, MESH_ROWS, CHUNK), BF16), v((2, MESH_ROWS, CHUNK), BF16),
        v((3, 2, ATOMS), jnp.int32), v((3, 2, ATOMS), F32), v((2, ATOMS), F32), v((2, ATOMS), F32),
        v((6, 6, ATOMS), F32), v((2, 40, ATOMS), F32), v((2, 8, ATOMS), F32),
        v((2, 256, ATOMS), BF16), v((2, 256, ATOMS), BF16),
        v((2, YH + CH, 256), F32), v((2, XH, 256), F32), v((2, MESH_ROWS, 256), F32),
        v((ROWS, 32, 256), F32), v((ROWS, 32, 256), F32), v((ROWS, 32, 256), F32),
        v((2, 256, 256), F32), v((2, 512, 512), BF16), v((2, 512, 512), BF16),
        v((2, 512, 512), BF16), v((256, 512), F32),
        v((2, DEVS, 8, 128), F32), v((2, DEVS, 8, 128), F32), v((2, DEVS, 8, 128), F32),
        v((2, DEVS, 8, 128), F32), v((2, 512, 256), F32),
        v((2, YH, 256), F32), v((2, 40, 256), F32),
        v((2, YH, 256), F32), v((2, XH, 256), F32), v((2, 40, 256), F32),
        v((2, 512, 768), BF16), v((2, HALO, 768), BF16), v((2, 3, ATOMS), F32),
        v((256, 256), F32), v((32, 256), F32),
        pltpu.SemaphoreType.DMA((34,)), pltpu.SemaphoreType.DMA((7,)), pltpu.SemaphoreType.REGULAR,
    ]
    out = pl.pallas_call(
        kernel,
        out_shape=pltpu.VMEM((3, 2, ATOMS), F32),
        in_specs=[anywhere] * 7,
        out_specs=vmem,
        scratch_shapes=scratch,
        compiler_params=pltpu.CompilerParams(
            collective_id=0, has_side_effects=True, vmem_limit_bytes=66_000_000
        ),
    )(*args)
    return jnp.transpose(out, (1, 0, 2))


def solution(mesh):
    placed = (
        P(None, None, ("row", "col")),
        P(None, None, ("row", "col")),
        P(None, ("row", "col")),
        P(None, ("row", "col")),
        P("row", "col", None),
    )
    return jax.shard_map(
        functools.partial(shards, tables()), mesh=mesh, in_specs=placed,
        out_specs=P(None, None, ("row", "col")), check_vma=False,
    )
```
